32 devices in a mesh: dp: 4 (over y, z), fsdp: 8 (over x, core).
Axes of the slice: x: 4, y: 2, z: 2, core: 2. Of those that a mesh axis runs over, the one named last changes fastest.
The devices are a block of a 4x4x8 slice.
Arguments:
- tokens: bfloat16 [32, 128, 1024], P(('dp', 'fsdp')), parts along dimension 0
- lengths: int32 [32], P(('dp', 'fsdp')), parts along dimension 0
- attn_gain: bfloat16 [2, 1024], P(None, 'fsdp')
- w_q: bfloat16 [2, 1024, 1024], P(None, None, 'fsdp')
- w_k: bfloat16 [2, 1024, 1024], P(None, None, 'fsdp')
- w_v: bfloat16 [2, 1024, 1024], P(None, None, 'fsdp')
- w_o: bfloat16 [2, 1024, 1024], P(None, 'fsdp')
- rel_bias: bfloat16 [2, 32, 16], P(None, None, 'fsdp')
- ffn_gain: bfloat16 [2, 1024], P(None, 'fsdp')
- w_in0: bfloat16 [2, 1024, 2816], P(None, None, 'fsdp')
- w_in1: bfloat16 [2, 1024, 2816], P(None, None, 'fsdp')
- w_out: bfloat16 [2, 2816, 1024], P(None, 'fsdp')
- final_gain: bfloat16 [1024], P('fsdp')
Outputs:
- output: bfloat16 [32, 128, 1024], P(('dp', 'fsdp')), parts along dimension 0
There are 4 independent parts. The reference program is written for one: setup_inputs(seed, part) draws one part's arguments, and reference() takes and returns one part's arrays. A program takes and returns all parts, laid end to end along the dimension named above; an argument that names none is the same for every part.
All inputs are finite; a program needn't handle non-finite values.
Results may differ from the reference program's by a relative error of at most 0.0106357.
Values are sent between devices in bfloat16 or wider.
A program may use at most 768 MiB of HBM per device.

```python
import jax
import jax.numpy as jnp
from jax import lax

NUM_PROMPTS = 8
SEQ_LEN = 128
D_MODEL = 1024
NUM_HEADS = 16
HEAD_DIM = 64
FF_DIM = 2816
NUM_LAYERS = 2
NUM_BUCKETS = 32
INNER_DIM = NUM_HEADS * HEAD_DIM
NORM_EPS = 1e-6


def bucket_table(seq_len):
    positions = jnp.arange(seq_len, dtype=jnp.int32)
    rel_pos = positions[None, :] - positions[:, None]
    half_buckets = NUM_BUCKETS // 2
    max_exact = half_buckets // 2
    distance = jnp.abs(rel_pos)
    log_steps = jnp.arange(1, half_buckets - max_exact, dtype=jnp.int32)
    thresholds = max_exact * max_exact * 2 ** log_steps
    log_bucket = max_exact + jnp.sum((distance * distance)[:, :, None] >= thresholds, axis=-1, dtype=jnp.int32)
    return jnp.where(rel_pos > 0, half_buckets, 0) + jnp.where(distance < max_exact, distance, log_bucket)


def rms_norm(hidden, gain):
    mean_sq = jnp.mean(hidden * hidden, axis=-1, keepdims=True)
    return (hidden * lax.rsqrt(mean_sq + NORM_EPS) * gain.astype(jnp.float32)).astype(jnp.bfloat16)


def setup_inputs(seed: int = 0, part: int = 0) -> dict:
    root_key = jax.random.key(seed)
    part_key = jax.random.fold_in(root_key, part)
    tok_key, len_key, slot_key = jax.random.split(part_key, 3)
    weight_keys = jax.random.split(root_key, 12)
    tokens = jax.random.normal(tok_key, (NUM_PROMPTS, SEQ_LEN, D_MODEL), jnp.float32).astype(jnp.bfloat16)
    lengths = jax.random.randint(len_key, (NUM_PROMPTS,), SEQ_LEN // 4, SEQ_LEN + 1, dtype=jnp.int32)
    full_slot = jax.random.randint(slot_key, (), 0, NUM_PROMPTS, dtype=jnp.int32)
    slots = jnp.arange(NUM_PROMPTS, dtype=jnp.int32)
    lengths = jnp.where(slots == full_slot, SEQ_LEN, lengths)
    lengths = jnp.where(slots == (full_slot + 1) % NUM_PROMPTS, SEQ_LEN // 4, lengths)

    def normal_draw(index, shape, scale):
        return (jax.random.normal(weight_keys[index], shape, jnp.float32) * scale).astype(jnp.bfloat16)

    def gain_draw(index, shape):
        return (1.0 + 0.4 * jax.random.normal(weight_keys[index], shape, jnp.float32)).astype(jnp.bfloat16)

    qk_scale = D_MODEL ** -0.5 * HEAD_DIM ** -0.25
    return {
        "tokens": tokens,
        "lengths": lengths,
        "attn_gain": gain_draw(0, (NUM_LAYERS, D_MODEL)),
        "w_q": normal_draw(1, (NUM_LAYERS, D_MODEL, INNER_DIM), qk_scale),
        "w_k": normal_draw(2, (NUM_LAYERS, D_MODEL, INNER_DIM), qk_scale),
        "w_v": normal_draw(3, (NUM_LAYERS, D_MODEL, INNER_DIM), D_MODEL ** -0.5),
        "w_o": normal_draw(4, (NUM_LAYERS, INNER_DIM, D_MODEL), 3.0 * INNER_DIM ** -0.5),
        "rel_bias": normal_draw(5, (NUM_LAYERS, NUM_BUCKETS, NUM_HEADS), 2.0),
        "ffn_gain": gain_draw(6, (NUM_LAYERS, D_MODEL)),
        "w_in0": normal_draw(7, (NUM_LAYERS, D_MODEL, FF_DIM), D_MODEL ** -0.5),
        "w_in1": normal_draw(8, (NUM_LAYERS, D_MODEL, FF_DIM), D_MODEL ** -0.5),
        "w_out": normal_draw(9, (NUM_LAYERS, FF_DIM, D_MODEL), FF_DIM ** -0.5),
        "final_gain": gain_draw(10, (D_MODEL,)),
    }


def reference(tokens, lengths, attn_gain, w_q, w_k, w_v, w_o, rel_bias, ffn_gain, w_in0, w_in1, w_out, final_gain):
    buckets = bucket_table(SEQ_LEN)
    positions = jnp.arange(SEQ_LEN, dtype=jnp.int32)
    stacked = (attn_gain, w_q, w_k, w_v, w_o, rel_bias, ffn_gain, w_in0, w_in1, w_out)

    def one_prompt(prompt_pair):
        prompt_tokens, prompt_len = prompt_pair
        key_ok = positions < prompt_len

        def layer_step(hidden, layer_weights):
            gain_attn, wq_layer, wk_layer, wv_layer, wo_layer, table_layer, gain_ffn, wi0_layer, wi1_layer, wout_layer = layer_weights
            normed = rms_norm(hidden, gain_attn)

            def project(weight):
                projected = jnp.dot(normed, weight, preferred_element_type=jnp.float32).astype(jnp.bfloat16)
                return projected.reshape(SEQ_LEN, NUM_HEADS, HEAD_DIM).astype(jnp.float32)

            queries = project(wq_layer)
            keys_proj = project(wk_layer)
            values = project(wv_layer)
            pos_bias = jnp.take(table_layer.T, buckets, axis=1).astype(jnp.float32)
            scores = jnp.einsum("qhd,khd->hqk", queries, keys_proj) + pos_bias
            scores = jnp.where(key_ok[None, None, :], scores, -1e30)
            attn_probs = jax.nn.softmax(scores, axis=-1).astype(jnp.bfloat16).astype(jnp.float32)
            context = jnp.einsum("hqk,khd->qhd", attn_probs, values).astype(jnp.bfloat16).reshape(SEQ_LEN, INNER_DIM)
            hidden = hidden + jnp.dot(context, wo_layer, preferred_element_type=jnp.float32)
            normed_ffn = rms_norm(hidden, gain_ffn)
            gate_act = jnp.dot(normed_ffn, wi0_layer, preferred_element_type=jnp.float32)
            lin_act = jnp.dot(normed_ffn, wi1_layer, preferred_element_type=jnp.float32)
            mixed_act = (jax.nn.gelu(gate_act, approximate=True) * lin_act).astype(jnp.bfloat16)
            hidden = hidden + jnp.dot(mixed_act, wout_layer, preferred_element_type=jnp.float32)
            return hidden, None

        hidden_end = lax.scan(layer_step, prompt_tokens.astype(jnp.float32), stacked)[0]
        normed_out = rms_norm(hidden_end, final_gain)
        return jnp.where(key_ok[:, None], normed_out, jnp.zeros_like(normed_out))

    return lax.map(one_prompt, (tokens, lengths))
```

```python
import functools

import jax
import jax.numpy as jnp
from jax import lax
from jax.experimental import pallas as pl
from jax.experimental.pallas import tpu as pltpu
from jax.sharding import PartitionSpec as P

HEAD_DIM = 64
NUM_BUCKETS = 32
NORM_EPS = 1e-6
LANES = 128
MASKED = -1e30
MESH = pl.DeviceIdType.MESH
BF16 = jnp.bfloat16
F32 = jnp.float32

ROW_ATTN, ROW_FFN, ROW_FINAL, ROW_BIAS, ROW_LEN, SMALL_ROWS = 0, 2, 4, 5, 9, 16

OWN, RT, LT, OP = 0, 1, 2, 3
TO_RIGHT = {OWN: LT, RT: OWN, LT: OP, OP: RT}
TO_LEFT = {OWN: RT, RT: OP, LT: OWN, OP: LT}


def bucket_of(rel_pos):
    half_buckets = NUM_BUCKETS // 2
    max_exact = half_buckets // 2
    distance = jnp.abs(rel_pos)
    log_bucket = jnp.full_like(distance, max_exact)
    for step in range(1, half_buckets - max_exact):
        log_bucket += jnp.where(distance * distance >= max_exact * max_exact * 2**step, 1, 0)
    return jnp.where(rel_pos > 0, half_buckets, 0) + jnp.where(distance < max_exact, distance, log_bucket)


def dot(a, b):
    return jnp.dot(a, b, preferred_element_type=F32)


def kernel(n, smalls, tok, wq, wk, wv, wo, win0, win1, wout, out,
           sm_all, gainb, lenb, biasb, tokb, nb, mb, wqkvb, wob, winb, woutb, qb, kb, vb, cb, c1b, hb, pb,
           relay_a, relay_b, recv_l, recv_r, send_sem, recv_sem, load_sem):
    seq, d_model = tok.shape[1], tok.shape[2]
    layers = wq.shape[0]
    half, rows_half = d_model // 2, seq // 2
    share = wq.shape[2]
    chip_cols = 2 * share

    me = lax.axis_index("fsdp")
    right, left = lax.rem(me + 2, n), lax.rem(me + n - 2, n)
    opposite = lax.rem(me + n // 2, n)
    partner = me + 1 - 2 * lax.rem(me, 2)
    counts = {"remote": 0, "local": 0}
    sent, done = [], set()

    def remote(src, dst, device):
        index = counts["remote"]
        counts["remote"] += 1
        copy = pltpu.make_async_remote_copy(
            src_ref=src, dst_ref=dst, send_sem=send_sem.at[index], recv_sem=recv_sem.at[index],
            device_id={"fsdp": device}, device_id_type=MESH)
        sent.append(copy)
        return copy

    def load(src, dst):
        index = counts["local"]
        counts["local"] += 1
        copy = pltpu.make_async_copy(src, dst, load_sem.at[index])
        copy.start()
        return copy

    def rows(slot, count=1):
        return pl.ds(slot * seq, count * seq)

    def part(ref, slot, r, c):
        row = pl.ds(slot * seq, seq) if r is None else pl.ds(slot * seq + r * rows_half, rows_half)
        col = slice(None) if c is None else pl.ds(c * half, half)
        return ref.at[row, col]

    tok_load = load(tok.at[0], tokb.at[rows(OWN), :])
    qkv_loads = []
    for layer in range(layers):
        qkv_loads.append([load(w.at[layer], wqkvb.at[layer, :, pl.ds(i * chip_cols, share)])
                          for i, w in enumerate((wq, wk, wv))])
        if layer == 0:
            wo_loads = [load(wo.at[k], wob.at[k, OWN, pl.ds(0, share), :]) for k in range(layers)]
            in_loads = []
            out_loads = []
        in_loads.append([load(w.at[layer], winb.at[layer, i, 0]) for i, w in enumerate((win0, win1))])
        out_loads.append(load(wout.at[layer], woutb.at[layer, 0]))

    barrier = pltpu.get_barrier_semaphore()
    for k in range(1, n):
        pl.semaphore_signal(barrier, inc=1, device_id={"fsdp": lax.rem(me + k, n)}, device_id_type=MESH)
    pl.semaphore_wait(barrier, n - 1)

    def block_sends(src, dst):
        to_right = [remote(src(c), dst(LT, c), right) for c in range(2)]
        to_left = [remote(src(c), dst(RT, c), left) for c in range(2)]
        return to_right, to_left

    def block_forwards(dst):
        return remote(dst(LT, 0), dst(OP, 0), right), remote(dst(RT, 1), dst(OP, 1), left)

    small_sends = [remote(smalls, sm_all.at[me], lax.rem(me + k, n)) for k in range(1, n)]
    tok_src = lambda c: tok.at[0, :, pl.ds(c * half, half)]
    tok_dst = lambda slot, c: part(tokb, slot, None, c)
    tok_r, tok_l = block_sends(tok_src, tok_dst)
    qkv_push = [[remote(w.at[layer], wqkvb.at[layer, :, pl.ds(i * chip_cols + share, share)], partner)
                 for i, w in enumerate((wq, wk, wv))] for layer in range(layers)]
    in_push = [[remote(w.at[layer], winb.at[layer, i, 1], partner) for i, w in enumerate((win0, win1))]
               for layer in range(layers)]
    out_push = [remote(wout.at[layer], woutb.at[layer, 1], partner) for layer in range(layers)]
    wo_push = [remote(wo.at[layer], wob.at[layer, OWN, pl.ds(share, share), :], partner) for layer in range(layers)]

    for copy in small_sends:
        copy.start()
    tok_r[0].start()
    tok_l[1].start()
    tok_r[1].start()
    tok_l[0].start()
    for copy in qkv_push[0]:
        copy.start()
    wo_push[0].start()

    sm_all[me] = smalls[...]
    for copy in small_sends:
        copy.wait_recv()
    for k in range(n):
        gainb[:, k * LANES:(k + 1) * LANES] = sm_all[k, 0:8, :]
    for slot, device in ((OWN, me), (RT, right), (LT, left), (OP, opposite)):
        lenb[slot] = jnp.broadcast_to(sm_all[device, ROW_LEN:ROW_LEN + 1, :], (8, LANES))

    def norm_rows(load_row, gain_row, dst, start, count):
        step = 32

        def body(i, carry):
            r = pl.multiple_of(start + i * step, step)
            x = load_row(r, step)
            mean_sq = jnp.mean(x * x, axis=-1, keepdims=True)
            normed = x * lax.rsqrt(mean_sq + NORM_EPS) * gainb[gain_row:gain_row + 1, :]
            dst[pl.ds(r, step), :] = normed.astype(BF16)
            return carry

        lax.fori_loop(0, count // step, body, 0)

    def token_row(r, step):
        return tokb[pl.ds(r, step), :].astype(F32)

    def hidden_row(r, step):
        return hb[pl.ds(r, step), :]

    lane_low = lax.rem(lax.broadcasted_iota(jnp.int32, (1, chip_cols), 1), 2 * HEAD_DIM) < HEAD_DIM

    def project(layer, src, slot, count):
        x = src[rows(slot, count), :]
        q = dot(x, wqkvb[layer, :, 0:chip_cols])
        qb[rows(slot, count), :] = q.astype(BF16)
        for i, ref in ((1, kb), (2, vb)):
            y = dot(x, wqkvb[layer, :, i * chip_cols:(i + 1) * chip_cols])
            ref[0, rows(slot, count), :] = jnp.where(lane_low, y, 0.0).astype(BF16)
            ref[1, rows(slot, count), :] = jnp.where(lane_low, 0.0, y).astype(BF16)

    key_index = lax.broadcasted_iota(jnp.int32, (1, seq), 1).astype(F32)

    def attend(layer, slot, count):
        def body(i, carry):
            s = slot + i
            row = pl.ds(pl.multiple_of(s * seq, seq), seq)
            key_ok = key_index < lenb[s, 0:1, :]
            for pair in range(chip_cols // LANES):
                col = pl.ds(pair * LANES, LANES)
                keys = jnp.concatenate([kb[0, row, col], kb[1, row, col]], axis=0)
                scores = lax.dot_general(qb[row, col], keys, (((1,), (1,)), ((), ())), preferred_element_type=F32)
                scores = scores + biasb[layer, pair]
                probs = []
                for h in range(2):
                    x = jnp.where(key_ok, scores[:, h * seq:(h + 1) * seq], MASKED)
                    e = jnp.exp(x - jnp.max(x, axis=-1, keepdims=True))
                    probs.append((e / jnp.sum(e, axis=-1, keepdims=True)).astype(BF16))
                values = jnp.concatenate([vb[0, row, col], vb[1, row, col]], axis=0)
                cb[0, row, col] = dot(jnp.concatenate(probs, axis=1), values).astype(BF16)
            return carry

        lax.fori_loop(0, count, body, 0)

    def build_bias():
        rel = lax.broadcasted_iota(jnp.int32, (LANES, 2 * seq), 1)
        rel = jnp.where(rel < seq, rel, rel - 2 * seq)
        one_hot = jnp.where(bucket_of(rel) == lax.broadcasted_iota(jnp.int32, (LANES, 2 * seq), 0), 1.0, 0.0)
        one_hot = one_hot.astype(BF16)
        for pair, device in ((0, me), (1, partner)):
            table = dot(sm_all[device].astype(BF16), one_hot)
            for layer in range(layers):
                for h in range(2):
                    row = ROW_BIAS + 2 * layer + h
                    line = jnp.broadcast_to(table[row:row + 1, :], (seq, 2 * seq))
                    shifted = pltpu.roll(line, 0, 1, stride=1, stride_axis=0)
                    biasb[layer, pair, :, h * seq:(h + 1) * seq] = shifted[:, 0:seq]

    tok_load.wait()
    norm_rows(token_row, ROW_ATTN, nb, OWN * seq, seq)
    build_bias()
    for copy in qkv_loads[0]:
        copy.wait()
    for copy in qkv_push[0]:
        copy.wait_recv()
    project(0, nb, OWN, 1)
    attend(0, OWN, 1)

    tok_fr, tok_fl = block_forwards(tok_dst)
    tok_r[0].wait_recv()
    tok_fr.start()
    tok_l[1].wait_recv()
    tok_fl.start()

    def c_part(src, slot, pair):
        return cb.at[src, rows(slot), pl.ds(pair * LANES, LANES)]

    c_r, c_l = {}, {}

    def send_context(slot):
        c_r[slot] = [remote(c_part(0, slot, p), c_part(LT, TO_RIGHT[slot], p), right) for p in range(2)]
        c_l[slot] = [remote(c_part(0, slot, p), c_part(RT, TO_LEFT[slot], p), left) for p in range(2)]
        c_r[slot][0].start()
        c_l[slot][1].start()
        c_r[slot][1].start()
        c_l[slot][0].start()

    send_context(OWN)

    def wo_copies(layer):
        src = lambda c: wo.at[layer, :, pl.ds(c * half, half)]
        dst = lambda slot, c: wob.at[layer, slot, pl.ds(0, share), pl.ds(c * half, half)]
        to_right, to_left = block_sends(src, dst)
        fr, fl = block_forwards(dst)
        push = {s: remote(wob.at[layer, s, pl.ds(0, share), :], wob.at[layer, s, pl.ds(share, share), :], partner)
                for s in (RT, LT, OP)}
        return to_right, to_left, fr, fl, push

    wo_r, wo_l, wo_fr, wo_fl, wo_share = zip(*[wo_copies(layer) for layer in range(layers)])

    def start_wo(layer):
        wo_r[layer][0].start()
        wo_l[layer][1].start()
        wo_r[layer][1].start()
        wo_l[layer][0].start()

    def forward_wo(layer):
        wo_r[layer][0].wait_recv()
        wo_fr[layer].start()
        wo_l[layer][1].wait_recv()
        wo_fl[layer].start()

    def share_wo_near(layer):
        wo_r[layer][1].wait_recv()
        wo_share[layer][LT].start()
        wo_l[layer][0].wait_recv()
        wo_share[layer][RT].start()

    def share_wo_far(layer):
        wo_fr[layer].wait_recv()
        wo_fl[layer].wait_recv()
        wo_share[layer][OP].start()

    start_wo(0)
    for copy in in_push[0]:
        copy.start()
    out_push[0].start()

    tok_r[1].wait_recv()
    tok_l[0].wait_recv()
    norm_rows(token_row, ROW_ATTN, nb, RT * seq, 2 * seq)
    project(0, nb, RT, 2)
    attend(0, RT, 2)
    send_context(RT)
    send_context(LT)

    tok_fr.wait_recv()
    tok_fl.wait_recv()
    norm_rows(token_row, ROW_ATTN, nb, OP * seq, seq)
    project(0, nb, OP, 1)
    attend(0, OP, 1)
    forward_wo(0)
    send_context(OP)

    def add_context(layer, src, slot, count, first):
        for j in range(0, d_model, chip_cols):
            col = pl.ds(j, chip_cols)
            y = dot(cb[src, rows(slot, count), :], wob[layer, src, :, col])
            if first:
                hb[rows(slot, count), col] = tokb[rows(slot, count), col].astype(F32) + y
            else:
                hb[rows(slot, count), col] += y

    c_fr, c_fl = {}, {}

    def forward_context(slot):
        near, far = TO_RIGHT[slot], TO_RIGHT[TO_RIGHT[slot]]
        c_fr[slot] = remote(c_part(LT, near, 0), c_part(OP, far, 0), right)
        c_r[slot][0].wait_recv()
        c_fr[slot].start()
        near, far = TO_LEFT[slot], TO_LEFT[TO_LEFT[slot]]
        c_fl[slot] = remote(c_part(RT, near, 1), c_part(OP, far, 1), left)
        c_l[slot][1].wait_recv()
        c_fl[slot].start()

    forward_context(OWN)
    wo_loads[0].wait()
    wo_push[0].wait_recv()
    add_context(0, OWN, OWN, 4, True)
    share_wo_near(0)
    forward_context(RT)
    forward_context(LT)
    share_wo_far(0)
    forward_context(OP)
    for slot in (OWN, RT, LT, OP):
        c_r[slot][1].wait_recv()
        c_l[slot][0].wait_recv()
    for slot in (RT, LT, OP):
        wo_share[0][slot].wait_recv()
    start_wo(1)
    add_context(0, LT, OWN, 4, False)
    add_context(0, RT, OWN, 4, False)
    for copy in in_loads[0]:
        copy.wait()
    out_loads[0].wait()
    for copy in in_push[0]:
        copy.wait_recv()
    out_push[0].wait_recv()

    def feed_forward(layer, slot, count):
        x = mb[layer, rows(slot, count), :]
        mixed = []
        for i in range(2):
            gate = dot(x, winb[layer, 0, i])
            lin = dot(x, winb[layer, 1, i])
            mixed.append((jax.nn.gelu(gate, approximate=True) * lin).astype(BF16))
        for j in range(0, d_model, chip_cols):
            col = pl.ds(j, chip_cols)
            pb[layer, rows(slot, count), col] = (
                dot(mixed[0], woutb[layer, 0, :, col]) + dot(mixed[1], woutb[layer, 1, :, col]))

    def scatter_copies(layer):
        p, ra, rb = pb.at[layer], relay_a.at[layer], relay_b.at[layer]
        rl, rr = recv_l.at[layer], recv_r.at[layer]
        row = lambda r: pl.ds(r * rows_half, rows_half)
        copies = {}
        for r in range(2):
            copies["op_r", r] = remote(part(p, OP, r, 0), ra.at[row(r), :], right)
            copies["op_l", r] = remote(part(p, OP, r, 1), rb.at[row(r), :], left)
            copies["plain_r", r] = remote(part(p, RT, r, 1), part(rl, 0, r, 1), right)
            copies["plain_l", r] = remote(part(p, LT, r, 0), part(rr, 0, r, 0), left)
            copies["sum_r", r] = remote(part(p, RT, r, 0), part(rl, 0, r, 0), right)
            copies["sum_l", r] = remote(part(p, LT, r, 1), part(rr, 0, r, 1), left)
        return copies

    def pass_on(layer, copies, r):
        a = pl.ds(RT * seq + r * rows_half, rows_half)
        b = pl.ds(LT * seq + r * rows_half, rows_half)
        row = pl.ds(r * rows_half, rows_half)
        copies["op_r", r].wait_recv()
        pb[layer, a, 0:half] += relay_a[layer, row, :]
        copies["sum_r", r].start()
        copies["op_l", r].wait_recv()
        pb[layer, b, half:d_model] += relay_b[layer, row, :]
        copies["sum_l", r].start()

    def collect(layer, copies, r):
        for name in ("plain_r", "plain_l", "sum_r", "sum_l"):
            copies[name, r].wait_recv()
        row = pl.ds(r * rows_half, rows_half)
        hb[row, :] = hb[row, :] + ((pb[layer, row, :] + recv_l[layer, row, :]) + recv_r[layer, row, :])

    rs = scatter_copies(0)
    for slot in (OWN, RT, LT, OP):
        c_fr[slot].wait_recv()
        c_fl[slot].wait_recv()
    add_context(0, OP, OP, 1, False)
    norm_rows(hidden_row, ROW_FFN, mb.at[0], OP * seq, seq)
    feed_forward(0, OP, 1)
    for r in range(2):
        rs["op_r", r].start()
        rs["op_l", r].start()
    add_context(0, OP, OWN, 3, False)
    norm_rows(hidden_row, ROW_FFN, mb.at[0], OWN * seq, 3 * seq)
    feed_forward(0, RT, 2)
    rs["plain_r", 0].start()
    rs["plain_l", 0].start()
    feed_forward(0, OWN, 1)
    pass_on(0, rs, 0)
    rs["plain_r", 1].start()
    rs["plain_l", 1].start()
    pass_on(0, rs, 1)
    for copy in qkv_push[1]:
        copy.start()
    wo_push[1].start()
    for copy in in_push[1]:
        copy.start()
    out_push[1].start()

    def gather_copies(ref, r):
        to_right = [remote(part(ref, OWN, r, c), part(ref, LT, r, c), right) for c in range(2)]
        to_left = [remote(part(ref, OWN, r, c), part(ref, RT, r, c), left) for c in range(2)]
        fr = remote(part(ref, LT, r, 0), part(ref, OP, r, 0), right)
        fl = remote(part(ref, RT, r, 1), part(ref, OP, r, 1), left)
        return to_right, to_left, fr, fl

    n_gather = [gather_copies(mb.at[2], r) for r in range(2)]
    for r in range(2):
        collect(0, rs, r)
        norm_rows(hidden_row, 1, mb.at[2], r * rows_half, rows_half)
        to_right, to_left, _, _ = n_gather[r]
        to_right[0].start()
        to_left[1].start()
        to_right[1].start()
        to_left[0].start()

    def forward_gather(gather):
        to_right, to_left, fr, fl = gather
        to_right[0].wait_recv()
        fr.start()
        to_left[1].wait_recv()
        fl.start()

    forward_gather(n_gather[0])
    for copy in qkv_loads[1]:
        copy.wait()
    for copy in qkv_push[1]:
        copy.wait_recv()
    for copies in c_r, c_l:
        for slot in (OWN, RT, LT, OP):
            for copy in copies[slot]:
                copy.wait_send()
                done.add(id(copy))
    project(1, mb.at[2], OWN, 1)
    attend(1, OWN, 1)
    forward_gather(n_gather[1])
    forward_wo(1)
    share_wo_near(1)
    for r in range(2):
        n_gather[r][0][1].wait_recv()
        n_gather[r][1][0].wait_recv()
    project(1, mb.at[2], RT, 2)
    attend(1, RT, 2)
    ctx_r = remote(cb.at[0, rows(RT), :], c1b.at[LT], right)
    ctx_l = remote(cb.at[0, rows(LT), :], c1b.at[RT], left)
    ctx_o = remote(cb.at[0, rows(OP), :], c1b.at[OP], opposite)
    ctx_r.start()
    ctx_l.start()
    for r in range(2):
        n_gather[r][2].wait_recv()
        n_gather[r][3].wait_recv()
    project(1, mb.at[2], OP, 1)
    attend(1, OP, 1)
    ctx_o.start()
    share_wo_far(1)
    wo_loads[1].wait()
    wo_push[1].wait_recv()

    def add_second(src, context):
        for j in range(0, d_model, chip_cols):
            col = pl.ds(j, chip_cols)
            hb[rows(OWN), col] += dot(context, wob[1, src, :, col])

    add_second(OWN, cb[0, rows(OWN), :])
    for slot, copy in ((LT, ctx_r), (RT, ctx_l), (OP, ctx_o)):
        wo_share[1][slot].wait_recv()
        copy.wait_recv()
        add_second(slot, c1b[slot])
    norm_rows(hidden_row, ROW_FFN + 1, mb.at[1], OWN * seq, seq)
    m_gather = [gather_copies(mb.at[1], r) for r in range(2)]
    for first, second in ((0, 1), (1, 0)):
        for r in range(2):
            m_gather[r][0][first].start()
            m_gather[r][1][second].start()
    for copy in in_loads[1]:
        copy.wait()
    out_loads[1].wait()
    for copy in in_push[1]:
        copy.wait_recv()
    out_push[1].wait_recv()
    rs = scatter_copies(1)
    feed_forward(1, OWN, 1)
    for r in range(2):
        forward_gather(m_gather[r])
    for r in range(2):
        m_gather[r][0][1].wait_recv()
        m_gather[r][1][0].wait_recv()
    feed_forward(1, RT, 2)
    rs["plain_r", 0].start()
    rs["plain_l", 0].start()
    for r in range(2):
        m_gather[r][2].wait_recv()
        m_gather[r][3].wait_recv()
    feed_forward(1, OP, 1)
    for r in range(2):
        rs["op_r", r].start()
        rs["op_l", r].start()
    rs["plain_r", 1].start()
    rs["plain_l", 1].start()
    for r in range(2):
        pass_on(1, rs, r)
    for r in range(2):
        collect(1, rs, r)
        norm_rows(hidden_row, ROW_FINAL, out, r * rows_half, rows_half)
    for copy in sent:
        if id(copy) not in done:
            copy.wait_send()


def encode(n, smalls, tokens, w_q, w_k, w_v, w_o, w_in0, w_in1, w_out):
    _, seq, d_model = tokens.shape
    layers, _, share = w_q.shape
    ff_share = w_in0.shape[2]
    chip_cols = 2 * share
    ring = n // 2
    any_spec = pl.BlockSpec(memory_space=pl.ANY)
    vmem = pl.BlockSpec(memory_space=pltpu.VMEM)
    scratch = [
        pltpu.VMEM((n, SMALL_ROWS, LANES), F32),
        pltpu.VMEM((8, d_model), F32),
        pltpu.VMEM((ring, 8, LANES), F32),
        pltpu.VMEM((layers, 2, seq, 2 * seq), F32),
        pltpu.VMEM((ring * seq, d_model), BF16),
        pltpu.VMEM((ring * seq, d_model), BF16),
        pltpu.VMEM((layers + 1, ring * seq, d_model), BF16),
        pltpu.VMEM((layers, d_model, 3 * chip_cols), BF16),
        pltpu.VMEM((layers, ring, chip_cols, d_model), BF16),
        pltpu.VMEM((layers, 2, 2, d_model, ff_share), BF16),
        pltpu.VMEM((layers, 2, ff_share, d_model), BF16),
        pltpu.VMEM((ring * seq, chip_cols), BF16),
        pltpu.VMEM((2, ring * seq, chip_cols), BF16),
        pltpu.VMEM((2, ring * seq, chip_cols), BF16),
        pltpu.VMEM((ring, ring * seq, chip_cols), BF16),
        pltpu.VMEM((ring, seq, chip_cols), BF16),
        pltpu.VMEM((ring * seq, d_model), F32),
        pltpu.VMEM((layers, ring * seq, d_model), F32),
        pltpu.VMEM((layers, seq, d_model // 2), F32),
        pltpu.VMEM((layers, seq, d_model // 2), F32),
        pltpu.VMEM((layers, seq, d_model), F32),
        pltpu.VMEM((layers, seq, d_model), F32),
        pltpu.SemaphoreType.DMA((160,)),
        pltpu.SemaphoreType.DMA((160,)),
        pltpu.SemaphoreType.DMA((24,)),
    ]
    return pl.pallas_call(
        functools.partial(kernel, n),
        out_shape=jax.ShapeDtypeStruct((seq, d_model), BF16),
        in_specs=[vmem] + [any_spec] * 8,
        out_specs=vmem,
        scratch_shapes=scratch,
        compiler_params=pltpu.CompilerParams(
            collective_id=0, has_side_effects=True, vmem_limit_bytes=56 * 1024 * 1024),
    )(smalls, tokens, w_q, w_k, w_v, w_o, w_in0, w_in1, w_out)


def solution(mesh):
    n = mesh.shape["fsdp"]
    batch_spec = P(("dp", "fsdp"))
    col_spec = P(None, None, "fsdp")
    row_spec = P(None, "fsdp", None)
    gain_spec = P(None, "fsdp")
    in_specs = (batch_spec, batch_spec, gain_spec, col_spec, col_spec, col_spec, row_spec, col_spec, gain_spec,
                col_spec, col_spec, row_spec, P("fsdp"))

    def local_forward(tokens, lengths, attn_gain, w_q, w_k, w_v, w_o, rel_bias, ffn_gain, w_in0, w_in1, w_out, final_gain):
        seq_len = tokens.shape[1]
        layers, buckets, heads = rel_bias.shape
        bias_rows = jnp.pad(jnp.swapaxes(rel_bias, 1, 2).reshape(layers * heads, buckets), ((0, 0), (0, LANES - buckets)))
        length_row = jnp.broadcast_to(lengths.astype(F32)[:, None], (1, LANES))
        smalls = jnp.concatenate(
            [attn_gain.astype(F32), ffn_gain.astype(F32), final_gain.astype(F32)[None], bias_rows.astype(F32), length_row], axis=0)
        smalls = jnp.pad(smalls, ((0, SMALL_ROWS - smalls.shape[0]), (0, 0)))
        normed_out = encode(n, smalls, tokens, w_q, w_k, w_v, w_o, w_in0, w_in1, w_out)
        key_ok = jnp.arange(seq_len, dtype=jnp.int32)[:, None] < lengths
        return jnp.where(key_ok, normed_out, jnp.zeros_like(normed_out))[None]

    return jax.shard_map(local_forward, mesh=mesh, in_specs=in_specs, out_specs=batch_spec, check_vma=False)
```

```python
import functools

import jax
import jax.numpy as jnp
from jax import lax
from jax.experimental import pallas as pl
from jax.experimental.pallas import tpu as pltpu
from jax.sharding import PartitionSpec as P

HEAD_DIM = 64
NUM_BUCKETS = 32
NORM_EPS = 1e-6
LANES = 128
MASKED = -1e30
MESH = pl.DeviceIdType.MESH
BF16 = jnp.bfloat16
F32 = jnp.float32

ROW_ATTN, ROW_FFN, ROW_FINAL, ROW_BIAS, ROW_LEN, SMALL_ROWS = 0, 2, 4, 5, 6, 8

OWN, RT, LT, OP = 0, 1, 2, 3
TO_RIGHT = {OWN: LT, RT: OWN, LT: OP, OP: RT}
TO_LEFT = {OWN: RT, RT: OP, LT: OWN, OP: LT}


def bucket_of(rel_pos):
    half_buckets = NUM_BUCKETS // 2
    max_exact = half_buckets // 2
    distance = jnp.abs(rel_pos)
    log_bucket = jnp.full_like(distance, max_exact)
    for step in range(1, half_buckets - max_exact):
        log_bucket += jnp.where(distance * distance >= max_exact * max_exact * 2**step, 1, 0)
    return jnp.where(rel_pos > 0, half_buckets, 0) + jnp.where(distance < max_exact, distance, log_bucket)


def dot(a, b):
    return jnp.dot(a, b, preferred_element_type=F32)


def dot_rows(a, b):
    return lax.dot_general(a, b, (((1,), (1,)), ((), ())), preferred_element_type=F32)


def kernel(n, lengths, attn_gain, ffn_gain, final_gain, bias_table, tok, wq, wk, wv, wo, win0, win1, wout, out,
           smalls, sm_all, gainb, lenb, biasb, tokb, nb, mb, wqkvb, wob, winb, woutb, qb, kb, vb, cb, c1b, hb, pb,
           relay_a, relay_b, recv_l, recv_r, send_sem, recv_sem, load_sem):
    seq, d_model = tok.shape[1], tok.shape[2]
    layers = wq.shape[0]
    half, rows_half = d_model // 2, seq // 2
    share, ff_share = wq.shape[2], wout.shape[1]
    chip_cols = 2 * share

    me = lax.axis_index("fsdp")
    right, left = lax.rem(me + 2, n), lax.rem(me + n - 2, n)
    opposite = lax.rem(me + n // 2, n)
    partner = me + 1 - 2 * lax.rem(me, 2)
    counts = {"remote": 0, "local": 0}
    sent, done = [], set()

    def remote(src, dst, device):
        index = counts["remote"]
        counts["remote"] += 1
        copy = pltpu.make_async_remote_copy(
            src_ref=src, dst_ref=dst, send_sem=send_sem.at[index], recv_sem=recv_sem.at[index],
            device_id={"fsdp": device}, device_id_type=MESH)
        sent.append(copy)
        return copy

    def load(src, dst):
        index = counts["local"]
        counts["local"] += 1
        copy = pltpu.make_async_copy(src, dst, load_sem.at[index])
        copy.start()
        return copy

    def rows(slot, count=1):
        return pl.ds(slot * seq, count * seq)

    def part(ref, slot, r, c):
        row = pl.ds(slot * seq, seq) if r is None else pl.ds(slot * seq + r * rows_half, rows_half)
        col = slice(None) if c is None else pl.ds(c * half, half)
        return ref.at[row, col]

    tok_load = load(tok.at[0], tokb.at[rows(OWN), :])
    qkv_loads = []
    for layer in range(layers):
        qkv_loads.append([load(w.at[layer], wqkvb.at[layer, :, pl.ds(i * chip_cols, share)])
                          for i, w in enumerate((wq, wk, wv))])
        if layer == 0:
            wo_loads = [load(wo.at[k], wob.at[k, OWN, pl.ds(0, share), :]) for k in range(layers)]
            in_loads = []
            out_loads = []
        in_loads.append([load(w.at[layer], winb.at[layer, i, pl.ds(0, ff_share), :]) for i, w in enumerate((win0, win1))])
        out_loads.append(load(wout.at[layer], woutb.at[layer, pl.ds(0, ff_share), :]))

    smalls[ROW_ATTN:ROW_ATTN + layers, :] = attn_gain[...].astype(F32)
    smalls[ROW_FFN:ROW_FFN + layers, :] = ffn_gain[...].astype(F32)
    smalls[ROW_FINAL:ROW_FINAL + 1, :] = final_gain[...].astype(F32)
    table = bias_table[...].astype(F32)
    smalls[ROW_BIAS:ROW_BIAS + 1, :] = jnp.concatenate([table[i:i + 1] for i in range(table.shape[0])], axis=1)
    smalls[ROW_LEN:SMALL_ROWS, :] = jnp.full((SMALL_ROWS - ROW_LEN, LANES), lengths[0], jnp.int32).astype(F32)

    barrier = pltpu.get_barrier_semaphore()
    for k in range(1, n):
        pl.semaphore_signal(barrier, inc=1, device_id={"fsdp": lax.rem(me + k, n)}, device_id_type=MESH)
    pl.semaphore_wait(barrier, n - 1)

    def block_sends(src, dst):
        to_right = [remote(src(c), dst(LT, c), right) for c in range(2)]
        to_left = [remote(src(c), dst(RT, c), left) for c in range(2)]
        return to_right, to_left

    def block_forwards(dst):
        return remote(dst(LT, 0), dst(OP, 0), right), remote(dst(RT, 1), dst(OP, 1), left)

    small_sends = [remote(smalls, sm_all.at[me], lax.rem(me + k, n)) for k in range(1, n)]
    tok_src = lambda c: part(tokb, OWN, None, c)
    tok_dst = lambda slot, c: part(tokb, slot, None, c)
    tok_r, tok_l = block_sends(tok_src, tok_dst)
    qkv_push = [[remote(w.at[layer], wqkvb.at[layer, :, pl.ds(i * chip_cols + share, share)], partner)
                 for i, w in enumerate((wq, wk, wv))] for layer in range(layers)]
    in_push = [[remote(w.at[layer], winb.at[layer, i, pl.ds(ff_share, ff_share), :], partner) for i, w in enumerate((win0, win1))]
               for layer in range(layers)]
    out_push = [remote(wout.at[layer], woutb.at[layer, pl.ds(ff_share, ff_share), :], partner) for layer in range(layers)]
    wo_push = [remote(wo.at[layer], wob.at[layer, OWN, pl.ds(share, share), :], partner) for layer in range(layers)]

    tok_load.wait()
    tok_r[0].start()
    tok_l[1].start()
    for copy in small_sends:
        copy.start()
    tok_r[1].start()
    tok_l[0].start()
    for copy in qkv_push[0]:
        copy.start()
    wo_push[0].start()

    sm_all[me] = smalls[...]
    for copy in small_sends:
        copy.wait_recv()
    for k in range(n):
        gainb[:, k * LANES:(k + 1) * LANES] = sm_all[k]
    for slot, device in ((OWN, me), (RT, right), (LT, left), (OP, opposite)):
        lenb[slot] = jnp.broadcast_to(sm_all[device, ROW_LEN:ROW_LEN + 1, :], (8, LANES))

    def norm_rows(load_row, gain_row, dst, start, count):
        step = 32

        def body(i, carry):
            r = pl.multiple_of(start + i * step, step)
            x = load_row(r, step)
            mean_sq = jnp.mean(x * x, axis=-1, keepdims=True)
            normed = x * lax.rsqrt(mean_sq + NORM_EPS) * gainb[gain_row:gain_row + 1, :]
            dst[pl.ds(r, step), :] = normed.astype(BF16)
            return carry

        lax.fori_loop(0, count // step, body, 0)

    def token_row(r, step):
        return tokb[pl.ds(r, step), :].astype(F32)

    def hidden_row(r, step):
        return hb[pl.ds(r, step), :]

    lane_low = lax.rem(lax.broadcasted_iota(jnp.int32, (1, chip_cols), 1), 2 * HEAD_DIM) < HEAD_DIM

    def project(layer, src, slot, count):
        x = src[rows(slot, count), :]
        q = dot(x, wqkvb[layer, :, 0:chip_cols])
        qb[rows(slot, count), :] = q.astype(BF16)
        for i, ref in ((1, kb), (2, vb)):
            y = dot(x, wqkvb[layer, :, i * chip_cols:(i + 1) * chip_cols])
            ref[0, rows(slot, count), :] = jnp.where(lane_low, y, 0.0).astype(BF16)
            ref[1, rows(slot, count), :] = jnp.where(lane_low, 0.0, y).astype(BF16)

    key_index = lax.broadcasted_iota(jnp.int32, (1, seq), 1).astype(F32)

    def attend(layer, slot, count):
        def body(i, carry):
            s = slot + i
            row = pl.ds(pl.multiple_of(s * seq, seq), seq)
            key_ok = key_index < lenb[s, 0:1, :]
            for pair in range(chip_cols // LANES):
                col = pl.ds(pair * LANES, LANES)
                keys = jnp.concatenate([kb[0, row, col], kb[1, row, col]], axis=0)
                scores = dot_rows(qb[row, col], keys)
                scores = scores + biasb[layer, pair]
                probs = []
                for h in range(2):
                    x = jnp.where(key_ok, scores[:, h * seq:(h + 1) * seq], MASKED)
                    e = jnp.exp(x - jnp.max(x, axis=-1, keepdims=True))
                    probs.append((e / jnp.sum(e, axis=-1, keepdims=True)).astype(BF16))
                values = jnp.concatenate([vb[0, row, col], vb[1, row, col]], axis=0)
                cb[0, row, col] = dot(jnp.concatenate(probs, axis=1), values).astype(BF16)
            return carry

        lax.fori_loop(0, count, body, 0)

    def build_bias():
        rel = lax.broadcasted_iota(jnp.int32, (LANES, 2 * seq), 1)
        rel = jnp.where(rel < seq, rel, rel - 2 * seq)
        lane = lax.broadcasted_iota(jnp.int32, (LANES, 2 * seq), 0)
        one_hot = jnp.where(bucket_of(rel) == lax.rem(lane, NUM_BUCKETS), 1.0, 0.0).astype(BF16)
        table_row = lax.broadcasted_iota(jnp.int32, (8, LANES), 0)
        table_lane = lax.broadcasted_iota(jnp.int32, (8, LANES), 1)
        own_lanes = table_row == table_lane // NUM_BUCKETS
        for pair, device in ((0, me), (1, partner)):
            tables = jnp.where(own_lanes, sm_all[device, ROW_BIAS:ROW_BIAS + 1, :], 0.0)
            lines = dot(tables.astype(BF16), one_hot)
            for layer in range(layers):
                for h in range(2):
                    row = 2 * layer + h
                    line = jnp.broadcast_to(lines[row:row + 1, :], (seq, 2 * seq))
                    shifted = pltpu.roll(line, 0, 1, stride=1, stride_axis=0)
                    biasb[layer, pair, :, h * seq:(h + 1) * seq] = shifted[:, 0:seq]

    norm_rows(token_row, ROW_ATTN, nb, OWN * seq, seq)
    build_bias()
    for copy in qkv_loads[0]:
        copy.wait()
    for copy in qkv_push[0]:
        copy.wait_recv()
    project(0, nb, OWN, 1)
    attend(0, OWN, 1)

    tok_fr, tok_fl = block_forwards(tok_dst)
    tok_r[0].wait_recv()
    tok_fr.start()
    tok_l[1].wait_recv()
    tok_fl.start()

    def c_part(src, slot, pair):
        return cb.at[src, rows(slot), pl.ds(pair * LANES, LANES)]

    c_r, c_l = {}, {}

    def send_context(slot):
        c_r[slot] = [remote(c_part(0, slot, p), c_part(LT, TO_RIGHT[slot], p), right) for p in range(2)]
        c_l[slot] = [remote(c_part(0, slot, p), c_part(RT, TO_LEFT[slot], p), left) for p in range(2)]
        c_r[slot][0].start()
        c_l[slot][1].start()
        c_r[slot][1].start()
        c_l[slot][0].start()

    send_context(OWN)

    def wo_copies(layer):
        src = lambda c: wo.at[layer, :, pl.ds(c * half, half)]
        dst = lambda slot, c: wob.at[layer, slot, pl.ds(0, share), pl.ds(c * half, half)]
        to_right, to_left = block_sends(src, dst)
        fr, fl = block_forwards(dst)
        push = {s: remote(wob.at[layer, s, pl.ds(0, share), :], wob.at[layer, s, pl.ds(share, share), :], partner)
                for s in (RT, LT, OP)}
        return to_right, to_left, fr, fl, push

    wo_r, wo_l, wo_fr, wo_fl, wo_share = zip(*[wo_copies(layer) for layer in range(layers)])

    def start_wo(layer):
        wo_r[layer][0].start()
        wo_l[layer][1].start()
        wo_r[layer][1].start()
        wo_l[layer][0].start()

    def forward_wo(layer):
        wo_r[layer][0].wait_recv()
        wo_fr[layer].start()
        wo_l[layer][1].wait_recv()
        wo_fl[layer].start()

    def share_wo_near(layer):
        wo_r[layer][1].wait_recv()
        wo_share[layer][LT].start()
        wo_l[layer][0].wait_recv()
        wo_share[layer][RT].start()

    def share_wo_far(layer):
        wo_fr[layer].wait_recv()
        wo_fl[layer].wait_recv()
        wo_share[layer][OP].start()

    start_wo(0)
    for copy in in_push[0]:
        copy.start()
    out_push[0].start()

    tok_r[1].wait_recv()
    tok_l[0].wait_recv()
    norm_rows(token_row, ROW_ATTN, nb, RT * seq, 2 * seq)
    project(0, nb, RT, 2)
    attend(0, RT, 2)
    send_context(RT)
    send_context(LT)

    tok_fr.wait_recv()
    tok_fl.wait_recv()
    norm_rows(token_row, ROW_ATTN, nb, OP * seq, seq)
    project(0, nb, OP, 1)
    attend(0, OP, 1)
    forward_wo(0)
    send_context(OP)

    def add_context(layer, src, slot, count, first):
        for j in range(0, d_model, chip_cols):
            col = pl.ds(j, chip_cols)
            y = dot(cb[src, rows(slot, count), :], wob[layer, src, :, col])
            if first:
                hb[rows(slot, count), col] = tokb[rows(slot, count), col].astype(F32) + y
            else:
                hb[rows(slot, count), col] += y

    c_fr, c_fl = {}, {}

    def forward_context(slot):
        near, far = TO_RIGHT[slot], TO_RIGHT[TO_RIGHT[slot]]
        c_fr[slot] = remote(c_part(LT, near, 0), c_part(OP, far, 0), right)
        c_r[slot][0].wait_recv()
        c_fr[slot].start()
        near, far = TO_LEFT[slot], TO_LEFT[TO_LEFT[slot]]
        c_fl[slot] = remote(c_part(RT, near, 1), c_part(OP, far, 1), left)
        c_l[slot][1].wait_recv()
        c_fl[slot].start()

    forward_context(OWN)
    wo_loads[0].wait()
    wo_push[0].wait_recv()
    add_context(0, OWN, OWN, 4, True)
    share_wo_near(0)
    forward_context(RT)
    forward_context(LT)
    share_wo_far(0)
    forward_context(OP)
    for slot in (OWN, RT, LT, OP):
        c_r[slot][1].wait_recv()
        c_l[slot][0].wait_recv()
    for slot in (RT, LT, OP):
        wo_share[0][slot].wait_recv()
    start_wo(1)
    add_context(0, LT, OWN, 4, False)
    add_context(0, RT, OWN, 4, False)
    for copy in in_loads[0]:
        copy.wait()
    out_loads[0].wait()
    for copy in in_push[0]:
        copy.wait_recv()
    out_push[0].wait_recv()

    def feed_forward(layer, slot, count):
        x = mb[layer, rows(slot, count), :]
        gate = dot_rows(x, winb[layer, 0])
        lin = dot_rows(x, winb[layer, 1])
        mixed = (jax.nn.gelu(gate, approximate=True) * lin).astype(BF16)
        for j in range(0, d_model, chip_cols):
            col = pl.ds(j, chip_cols)
            pb[layer, rows(slot, count), col] = dot(mixed, woutb[layer, :, col])

    def scatter_copies(layer):
        p, ra, rb = pb.at[layer], relay_a.at[layer], relay_b.at[layer]
        rl, rr = recv_l.at[layer], recv_r.at[layer]
        row = lambda r: pl.ds(r * rows_half, rows_half)
        copies = {}
        for r in range(2):
            copies["op_r", r] = remote(part(p, OP, r, 0), ra.at[row(r), :], right)
            copies["op_l", r] = remote(part(p, OP, r, 1), rb.at[row(r), :], left)
            copies["plain_r", r] = remote(part(p, RT, r, 1), part(rl, 0, r, 1), right)
            copies["plain_l", r] = remote(part(p, LT, r, 0), part(rr, 0, r, 0), left)
            copies["sum_r", r] = remote(part(p, RT, r, 0), part(rl, 0, r, 0), right)
            copies["sum_l", r] = remote(part(p, LT, r, 1), part(rr, 0, r, 1), left)
        return copies

    def pass_on(layer, copies, r):
        a = pl.ds(RT * seq + r * rows_half, rows_half)
        b = pl.ds(LT * seq + r * rows_half, rows_half)
        row = pl.ds(r * rows_half, rows_half)
        copies["op_r", r].wait_recv()
        pb[layer, a, 0:half] += relay_a[layer, row, :]
        copies["sum_r", r].start()
        copies["op_l", r].wait_recv()
        pb[layer, b, half:d_model] += relay_b[layer, row, :]
        copies["sum_l", r].start()

    def collect(layer, copies, r):
        for name in ("plain_r", "plain_l", "sum_r", "sum_l"):
            copies[name, r].wait_recv()
        row = pl.ds(r * rows_half, rows_half)
        hb[row, :] = hb[row, :] + ((pb[layer, row, :] + recv_l[layer, row, :]) + recv_r[layer, row, :])

    rs = scatter_copies(0)
    for slot in (OWN, RT, LT, OP):
        c_fr[slot].wait_recv()
        c_fl[slot].wait_recv()
    add_context(0, OP, OP, 1, False)
    norm_rows(hidden_row, ROW_FFN, mb.at[0], OP * seq, seq)
    feed_forward(0, OP, 1)
    for r in range(2):
        rs["op_r", r].start()
        rs["op_l", r].start()
    add_context(0, OP, OWN, 3, False)
    norm_rows(hidden_row, ROW_FFN, mb.at[0], OWN * seq, 3 * seq)
    feed_forward(0, RT, 2)
    rs["plain_r", 0].start()
    rs["plain_l", 0].start()
    feed_forward(0, OWN, 1)
    pass_on(0, rs, 0)
    rs["plain_r", 1].start()
    rs["plain_l", 1].start()
    pass_on(0, rs, 1)
    for copy in qkv_push[1]:
        copy.start()
    wo_push[1].start()
    for copy in in_push[1]:
        copy.start()
    out_push[1].start()

    def gather_copies(ref, r):
        to_right = [remote(part(ref, OWN, r, c), part(ref, LT, r, c), right) for c in range(2)]
        to_left = [remote(part(ref, OWN, r, c), part(ref, RT, r, c), left) for c in range(2)]
        fr = remote(part(ref, LT, r, 0), part(ref, OP, r, 0), right)
        fl = remote(part(ref, RT, r, 1), part(ref, OP, r, 1), left)
        return to_right, to_left, fr, fl

    n_gather = [gather_copies(mb.at[2], r) for r in range(2)]
    for r in range(2):
        collect(0, rs, r)
        norm_rows(hidden_row, 1, mb.at[2], r * rows_half, rows_half)
        to_right, to_left, _, _ = n_gather[r]
        to_right[0].start()
        to_left[1].start()
        to_right[1].start()
        to_left[0].start()

    def forward_gather(gather):
        to_right, to_left, fr, fl = gather
        to_right[0].wait_recv()
        fr.start()
        to_left[1].wait_recv()
        fl.start()

    forward_gather(n_gather[0])
    for copy in qkv_loads[1]:
        copy.wait()
    for copy in qkv_push[1]:
        copy.wait_recv()
    for copies in c_r, c_l:
        for slot in (OWN, RT, LT, OP):
            for copy in copies[slot]:
                copy.wait_send()
                done.add(id(copy))
    project(1, mb.at[2], OWN, 1)
    attend(1, OWN, 1)
    forward_gather(n_gather[1])
    forward_wo(1)
    share_wo_near(1)
    for r in range(2):
        n_gather[r][0][1].wait_recv()
        n_gather[r][1][0].wait_recv()
    project(1, mb.at[2], RT, 2)
    attend(1, RT, 2)
    ctx_r = remote(cb.at[0, rows(RT), :], c1b.at[LT], right)
    ctx_l = remote(cb.at[0, rows(LT), :], c1b.at[RT], left)
    ctx_o = remote(cb.at[0, rows(OP), :], c1b.at[OP], opposite)
    ctx_r.start()
    ctx_l.start()
    for r in range(2):
        n_gather[r][2].wait_recv()
        n_gather[r][3].wait_recv()
    project(1, mb.at[2], OP, 1)
    attend(1, OP, 1)
    ctx_o.start()
    share_wo_far(1)
    wo_loads[1].wait()
    wo_push[1].wait_recv()

    def add_second(src, context):
        for j in range(0, d_model, chip_cols):
            col = pl.ds(j, chip_cols)
            hb[rows(OWN), col] += dot(context, wob[1, src, :, col])

    add_second(OWN, cb[0, rows(OWN), :])
    for slot, copy in ((LT, ctx_r), (RT, ctx_l), (OP, ctx_o)):
        wo_share[1][slot].wait_recv()
        copy.wait_recv()
        add_second(slot, c1b[slot])
    norm_rows(hidden_row, ROW_FFN + 1, mb.at[1], OWN * seq, seq)
    m_gather = [gather_copies(mb.at[1], r) for r in range(2)]
    for first, second in ((0, 1), (1, 0)):
        for r in range(2):
            m_gather[r][0][first].start()
            m_gather[r][1][second].start()
    for copy in in_loads[1]:
        copy.wait()
    out_loads[1].wait()
    for copy in in_push[1]:
        copy.wait_recv()
    out_push[1].wait_recv()
    rs = scatter_copies(1)
    feed_forward(1, OWN, 1)
    for r in range(2):
        forward_gather(m_gather[r])
    for r in range(2):
        m_gather[r][0][1].wait_recv()
        m_gather[r][1][0].wait_recv()
    feed_forward(1, RT, 2)
    rs["plain_r", 0].start()
    rs["plain_l", 0].start()
    for r in range(2):
        m_gather[r][2].wait_recv()
        m_gather[r][3].wait_recv()
    feed_forward(1, OP, 1)
    for r in range(2):
        rs["op_r", r].start()
        rs["op_l", r].start()
    rs["plain_r", 1].start()
    rs["plain_l", 1].start()
    for r in range(2):
        pass_on(1, rs, r)
    for r in range(2):
        collect(1, rs, r)
        norm_rows(hidden_row, ROW_FINAL, out, r * rows_half, rows_half)
    for copy in sent:
        if id(copy) not in done:
            copy.wait_send()


def encode(n, lengths, attn_gain, ffn_gain, final_gain, bias_table, tokens, w_q, w_k, w_v, w_o, w_in0, w_in1, w_out):
    _, seq, d_model = tokens.shape
    layers, _, share = w_q.shape
    ff_share = w_out.shape[1]
    chip_cols = 2 * share
    ring = n // 2
    any_spec = pl.BlockSpec(memory_space=pl.ANY)
    vmem = pl.BlockSpec(memory_space=pltpu.VMEM)
    scratch = [
        pltpu.VMEM((SMALL_ROWS, LANES), F32),
        pltpu.VMEM((n, SMALL_ROWS, LANES), F32),
        pltpu.VMEM((8, d_model), F32),
        pltpu.VMEM((ring, 8, LANES), F32),
        pltpu.VMEM((layers, 2, seq, 2 * seq), F32),
        pltpu.VMEM((ring * seq, d_model), BF16),
        pltpu.VMEM((ring * seq, d_model), BF16),
        pltpu.VMEM((layers + 1, ring * seq, d_model), BF16),
        pltpu.VMEM((layers, d_model, 3 * chip_cols), BF16),
        pltpu.VMEM((layers, ring, chip_cols, d_model), BF16),
        pltpu.VMEM((layers, 2, 2 * ff_share, d_model), BF16),
        pltpu.VMEM((layers, 2 * ff_share, d_model), BF16),
        pltpu.VMEM((ring * seq, chip_cols), BF16),
        pltpu.VMEM((2, ring * seq, chip_cols), BF16),
        pltpu.VMEM((2, ring * seq, chip_cols), BF16),
        pltpu.VMEM((ring, ring * seq, chip_cols), BF16),
        pltpu.VMEM((ring, seq, chip_cols), BF16),
        pltpu.VMEM((ring * seq, d_model), F32),
        pltpu.VMEM((layers, ring * seq, d_model), F32),
        pltpu.VMEM((layers, seq, d_model // 2), F32),
        pltpu.VMEM((layers, seq, d_model // 2), F32),
        pltpu.VMEM((layers, seq, d_model), F32),
        pltpu.VMEM((layers, seq, d_model), F32),
        pltpu.SemaphoreType.DMA((160,)),
        pltpu.SemaphoreType.DMA((160,)),
        pltpu.SemaphoreType.DMA((24,)),
    ]
    return pl.pallas_call(
        functools.partial(kernel, n),
        out_shape=pltpu.VMEM((seq, d_model), BF16),
        in_specs=[pl.BlockSpec(memory_space=pltpu.SMEM)] + [vmem] * 4 + [any_spec] * 8,
        out_specs=vmem,
        scratch_shapes=scratch,
        compiler_params=pltpu.CompilerParams(
            collective_id=0, has_side_effects=True, vmem_limit_bytes=56 * 1024 * 1024),
    )(lengths, attn_gain, ffn_gain, final_gain, bias_table, tokens, w_q, w_k, w_v, w_o, w_in0, w_in1, w_out)


def solution(mesh):
    n = mesh.shape["fsdp"]
    batch_spec = P(("dp", "fsdp"))
    col_spec = P(None, None, "fsdp")
    row_spec = P(None, "fsdp", None)
    gain_spec = P(None, "fsdp")
    in_specs = (batch_spec, batch_spec, gain_spec, col_spec, col_spec, col_spec, row_spec, col_spec, gain_spec,
                col_spec, col_spec, row_spec, P("fsdp"))

    def local_forward(tokens, lengths, attn_gain, w_q, w_k, w_v, w_o, rel_bias, ffn_gain, w_in0, w_in1, w_out, final_gain):
        seq_len = tokens.shape[1]
        layers, buckets, heads = rel_bias.shape
        bias_table = jnp.swapaxes(rel_bias, 1, 2).reshape(layers * heads, buckets)
        normed_out = encode(n, lengths, attn_gain, ffn_gain, final_gain[None], bias_table, tokens, w_q, w_k, w_v, w_o,
                            jnp.swapaxes(w_in0, 1, 2), jnp.swapaxes(w_in1, 1, 2), w_out)
        key_ok = jnp.arange(seq_len, dtype=jnp.int32)[:, None] < lengths
        return jnp.where(key_ok, normed_out, jnp.zeros_like(normed_out))[None]

    return jax.shard_map(local_forward, mesh=mesh, in_specs=in_specs, out_specs=batch_spec, check_vma=False)
```

```python
import functools

import jax
import jax.numpy as jnp
from jax import lax
from jax.experimental import pallas as pl
from jax.experimental.pallas import tpu as pltpu
from jax.sharding import PartitionSpec as P

HEAD_DIM = 64
NUM_BUCKETS = 32
NORM_EPS = 1e-6
LANES = 128
MASKED = -1e30
MESH = pl.DeviceIdType.MESH
BF16 = jnp.bfloat16
F32 = jnp.float32

ROW_ATTN, ROW_FFN, ROW_FINAL, ROW_BIAS, ROW_LEN, SMALL_ROWS = 0, 2, 4, 5, 6, 8

OWN, RT, LT, OP = 0, 1, 2, 3
TO_RIGHT = {OWN: LT, RT: OWN, LT: OP, OP: RT}
TO_LEFT = {OWN: RT, RT: OP, LT: OWN, OP: LT}


def bucket_of(rel_pos):
    half_buckets = NUM_BUCKETS // 2
    max_exact = half_buckets // 2
    distance = jnp.abs(rel_pos)
    log_bucket = jnp.full_like(distance, max_exact)
    for step in range(1, half_buckets - max_exact):
        log_bucket += jnp.where(distance * distance >= max_exact * max_exact * 2**step, 1, 0)
    return jnp.where(rel_pos > 0, half_buckets, 0) + jnp.where(distance < max_exact, distance, log_bucket)


def dot(a, b):
    return jnp.dot(a, b, preferred_element_type=F32)


def dot_rows(a, b):
    return lax.dot_general(a, b, (((1,), (1,)), ((), ())), preferred_element_type=F32)


def kernel(n, groups, lengths, attn_gain, ffn_gain, final_gain, bias_table, tok, wq, wk, wv, wo, win0, win1, wout, out,
           smalls, sm_all, gainb, lenb, biasb, tokb, nb, mb, wqkvb, wob, winb, woutb, qb, kb, vb, cb, c1b, hb, pb,
           relay_a, relay_b, recv_l, recv_r, send_sem, recv_sem, load_sem):
    seq, d_model = tok.shape[1], tok.shape[2]
    layers = wq.shape[0]
    half, rows_half = d_model // 2, seq // 2
    share, ff_share = wq.shape[2], wout.shape[1]
    chip_cols = 2 * share

    me, group = lax.axis_index("fsdp"), lax.axis_index("dp")
    right, left = lax.rem(me + 2, n), lax.rem(me + n - 2, n)
    opposite = lax.rem(me + n // 2, n)
    partner = me + 1 - 2 * lax.rem(me, 2)
    counts = {"remote": 0, "local": 0}
    sent, done = [], set()

    def remote(src, dst, device, axis="fsdp"):
        index = counts["remote"]
        counts["remote"] += 1
        copy = pltpu.make_async_remote_copy(
            src_ref=src, dst_ref=dst, send_sem=send_sem.at[index], recv_sem=recv_sem.at[index],
            device_id={axis: device}, device_id_type=MESH)
        sent.append(copy)
        return copy

    def load(src, dst):
        index = counts["local"]
        counts["local"] += 1
        copy = pltpu.make_async_copy(src, dst, load_sem.at[index])
        copy.start()
        return copy

    def rows(slot, count=1):
        return pl.ds(slot * seq, count * seq)

    def part(ref, slot, r, c):
        row = pl.ds(slot * seq, seq) if r is None else pl.ds(slot * seq + r * rows_half, rows_half)
        col = slice(None) if c is None else pl.ds(c * half, half)
        return ref.at[row, col]

    tok_load = load(tok.at[0], tokb.at[rows(OWN), :])
    qkv_loads = []
    for layer in range(layers):
        qkv_loads.append([load(w.at[layer], wqkvb.at[layer, :, pl.ds(i * chip_cols, share)])
                          for i, w in enumerate((wq, wk, wv))])
        if layer == 0:
            wo_loads = [load(wo.at[k], wob.at[k, OWN, pl.ds(0, share), :]) for k in range(layers)]
            in_loads = []
            out_loads = []
        in_loads.append([load(w.at[layer], winb.at[layer, i, pl.ds(0, ff_share), :]) for i, w in enumerate((win0, win1))])
        out_loads.append(load(wout.at[layer], woutb.at[layer, pl.ds(0, ff_share), :]))

    smalls[ROW_ATTN:ROW_ATTN + layers, :] = attn_gain[...].astype(F32)
    smalls[ROW_FFN:ROW_FFN + layers, :] = ffn_gain[...].astype(F32)
    smalls[ROW_FINAL:ROW_FINAL + 1, :] = final_gain[...].astype(F32)
    table = bias_table[...].astype(F32)
    smalls[ROW_BIAS:ROW_BIAS + 1, :] = jnp.concatenate([table[i:i + 1] for i in range(table.shape[0])], axis=1)
    smalls[ROW_LEN:SMALL_ROWS, :] = jnp.full((SMALL_ROWS - ROW_LEN, LANES), lengths[0], jnp.int32).astype(F32)

    barrier = pltpu.get_barrier_semaphore()
    for k in range(1, n):
        pl.semaphore_signal(barrier, inc=1, device_id={"fsdp": lax.rem(me + k, n)}, device_id_type=MESH)
    for k in range(1, groups):
        pl.semaphore_signal(barrier, inc=1, device_id={"dp": lax.rem(group + k, groups)}, device_id_type=MESH)
    pl.semaphore_wait(barrier, n - 1 + groups - 1)

    def block_sends(src, dst):
        to_right = [remote(src(c), dst(LT, c), right) for c in range(2)]
        to_left = [remote(src(c), dst(RT, c), left) for c in range(2)]
        return to_right, to_left

    def block_forwards(dst):
        return remote(dst(LT, 0), dst(OP, 0), right), remote(dst(RT, 1), dst(OP, 1), left)

    row_pieces = min(groups, share // 16)
    col_pieces = groups // row_pieces
    piece_rows, piece_cols = share // row_pieces, d_model // col_pieces
    piece_row = pl.multiple_of(group // col_pieces * piece_rows, piece_rows)
    piece_col = pl.multiple_of(lax.rem(group, col_pieces) * piece_cols, piece_cols)

    def wo_copies(layer):
        col = lambda c: pl.ds(pl.multiple_of(piece_col + c * (piece_cols // 2), LANES), piece_cols // 2)
        src = lambda c: wo.at[layer, pl.ds(piece_row, piece_rows), col(c)]
        dst = lambda slot, c: wob.at[layer, slot, pl.ds(piece_row, piece_rows), col(c)]
        to_right, to_left = block_sends(src, dst)
        fr, fl = block_forwards(dst)
        piece = lambda slot, count: wob.at[layer, pl.ds(slot, count), pl.ds(piece_row, piece_rows), pl.ds(piece_col, piece_cols)]
        spread = [[remote(piece(slot, count), piece(slot, count), lax.rem(group + k, groups), "dp") for k in range(1, groups)]
                  for slot, count in ((RT, 2), (OP, 1))]
        push = {s: remote(wob.at[layer, s, pl.ds(0, share), :], wob.at[layer, s, pl.ds(share, share), :], partner)
                for s in (RT, LT, OP)}
        return to_right, to_left, fr, fl, spread, push

    wo_r, wo_l, wo_fr, wo_fl, wo_spread, wo_share = zip(*[wo_copies(layer) for layer in range(layers)])

    def start_wo(layer):
        wo_r[layer][0].start()
        wo_l[layer][1].start()
        wo_r[layer][1].start()
        wo_l[layer][0].start()

    def forward_wo(layer):
        wo_r[layer][0].wait_recv()
        wo_fr[layer].start()
        wo_l[layer][1].wait_recv()
        wo_fl[layer].start()
        wo_r[layer][1].wait_recv()
        wo_l[layer][0].wait_recv()
        for copy in wo_spread[layer][0]:
            copy.start()

    def spread_far_wo(layer):
        wo_fr[layer].wait_recv()
        wo_fl[layer].wait_recv()
        for copy in wo_spread[layer][1]:
            copy.start()

    def share_wo_near(layer):
        for copy in wo_spread[layer][0]:
            copy.wait_recv()
        wo_share[layer][LT].start()
        wo_share[layer][RT].start()

    def share_wo_far(layer):
        for copy in wo_spread[layer][1]:
            copy.wait_recv()
        wo_share[layer][OP].start()

    small_sends = [remote(smalls, sm_all.at[me], lax.rem(me + k, n)) for k in range(1, n)]
    tok_src = lambda c: part(tokb, OWN, None, c)
    tok_dst = lambda slot, c: part(tokb, slot, None, c)
    tok_r, tok_l = block_sends(tok_src, tok_dst)
    qkv_push = [[remote(w.at[layer], wqkvb.at[layer, :, pl.ds(i * chip_cols + share, share)], partner)
                 for i, w in enumerate((wq, wk, wv))] for layer in range(layers)]
    in_push = [[remote(w.at[layer], winb.at[layer, i, pl.ds(ff_share, ff_share), :], partner) for i, w in enumerate((win0, win1))]
               for layer in range(layers)]
    out_push = [remote(wout.at[layer], woutb.at[layer, pl.ds(ff_share, ff_share), :], partner) for layer in range(layers)]
    wo_push = [remote(wo.at[layer], wob.at[layer, OWN, pl.ds(share, share), :], partner) for layer in range(layers)]

    start_wo(0)
    tok_load.wait()
    tok_r[0].start()
    tok_l[1].start()
    for copy in small_sends:
        copy.start()
    tok_r[1].start()
    tok_l[0].start()
    for copy in qkv_push[0]:
        copy.start()
    wo_push[0].start()

    sm_all[me] = smalls[...]
    for copy in small_sends:
        copy.wait_recv()
    for k in range(n):
        gainb[:, k * LANES:(k + 1) * LANES] = sm_all[k]
    for slot, device in ((OWN, me), (RT, right), (LT, left), (OP, opposite)):
        lenb[slot] = jnp.broadcast_to(sm_all[device, ROW_LEN:ROW_LEN + 1, :], (8, LANES))

    def norm_rows(load_row, gain_row, dst, start, count):
        step = 32

        def body(i, carry):
            r = pl.multiple_of(start + i * step, step)
            x = load_row(r, step)
            mean_sq = jnp.mean(x * x, axis=-1, keepdims=True)
            normed = x * lax.rsqrt(mean_sq + NORM_EPS) * gainb[gain_row:gain_row + 1, :]
            dst[pl.ds(r, step), :] = normed.astype(BF16)
            return carry

        lax.fori_loop(0, count // step, body, 0)

    def token_row(r, step):
        return tokb[pl.ds(r, step), :].astype(F32)

    def hidden_row(r, step):
        return hb[pl.ds(r, step), :]

    lane_low = lax.rem(lax.broadcasted_iota(jnp.int32, (1, chip_cols), 1), 2 * HEAD_DIM) < HEAD_DIM

    def project(layer, src, slot, count):
        x = src[rows(slot, count), :]
        q = dot(x, wqkvb[layer, :, 0:chip_cols])
        qb[rows(slot, count), :] = q.astype(BF16)
        for i, ref in ((1, kb), (2, vb)):
            y = dot(x, wqkvb[layer, :, i * chip_cols:(i + 1) * chip_cols])
            ref[0, rows(slot, count), :] = jnp.where(lane_low, y, 0.0).astype(BF16)
            ref[1, rows(slot, count), :] = jnp.where(lane_low, 0.0, y).astype(BF16)

    key_index = lax.broadcasted_iota(jnp.int32, (1, seq), 1).astype(F32)

    def attend(layer, slot, count):
        def body(i, carry):
            s = slot + i
            row = pl.ds(pl.multiple_of(s * seq, seq), seq)
            key_ok = key_index < lenb[s, 0:1, :]
            for pair in range(chip_cols // LANES):
                col = pl.ds(pair * LANES, LANES)
                keys = jnp.concatenate([kb[0, row, col], kb[1, row, col]], axis=0)
                scores = dot_rows(qb[row, col], keys)
                scores = scores + biasb[layer, pair]
                probs = []
                for h in range(2):
                    x = jnp.where(key_ok, scores[:, h * seq:(h + 1) * seq], MASKED)
                    e = jnp.exp(x - jnp.max(x, axis=-1, keepdims=True))
                    probs.append((e / jnp.sum(e, axis=-1, keepdims=True)).astype(BF16))
                values = jnp.concatenate([vb[0, row, col], vb[1, row, col]], axis=0)
                cb[0, row, col] = dot(jnp.concatenate(probs, axis=1), values).astype(BF16)
            return carry

        lax.fori_loop(0, count, body, 0)

    def build_bias():
        rel = lax.broadcasted_iota(jnp.int32, (LANES, 2 * seq), 1)
        rel = jnp.where(rel < seq, rel, rel - 2 * seq)
        lane = lax.broadcasted_iota(jnp.int32, (LANES, 2 * seq), 0)
        one_hot = jnp.where(bucket_of(rel) == lax.rem(lane, NUM_BUCKETS), 1.0, 0.0).astype(BF16)
        table_row = lax.broadcasted_iota(jnp.int32, (8, LANES), 0)
        table_lane = lax.broadcasted_iota(jnp.int32, (8, LANES), 1)
        own_lanes = table_row == table_lane // NUM_BUCKETS
        for pair, device in ((0, me), (1, partner)):
            tables = jnp.where(own_lanes, sm_all[device, ROW_BIAS:ROW_BIAS + 1, :], 0.0)
            lines = dot(tables.astype(BF16), one_hot)
            for layer in range(layers):
                for h in range(2):
                    row = 2 * layer + h
                    line = jnp.broadcast_to(lines[row:row + 1, :], (seq, 2 * seq))
                    shifted = pltpu.roll(line, 0, 1, stride=1, stride_axis=0)
                    biasb[layer, pair, :, h * seq:(h + 1) * seq] = shifted[:, 0:seq]

    norm_rows(token_row, ROW_ATTN, nb, OWN * seq, seq)
    build_bias()
    for copy in qkv_loads[0]:
        copy.wait()
    for copy in qkv_push[0]:
        copy.wait_recv()
    project(0, nb, OWN, 1)
    attend(0, OWN, 1)

    forward_wo(0)
    tok_fr, tok_fl = block_forwards(tok_dst)
    tok_r[0].wait_recv()
    tok_fr.start()
    tok_l[1].wait_recv()
    tok_fl.start()

    def c_part(src, slot, pair):
        return cb.at[src, rows(slot), pl.ds(pair * LANES, LANES)]

    c_r, c_l = {}, {}

    def send_context(slot):
        c_r[slot] = [remote(c_part(0, slot, p), c_part(LT, TO_RIGHT[slot], p), right) for p in range(2)]
        c_l[slot] = [remote(c_part(0, slot, p), c_part(RT, TO_LEFT[slot], p), left) for p in range(2)]
        c_r[slot][0].start()
        c_l[slot][1].start()
        c_r[slot][1].start()
        c_l[slot][0].start()

    send_context(OWN)

    for copy in in_push[0]:
        copy.start()
    out_push[0].start()

    tok_r[1].wait_recv()
    tok_l[0].wait_recv()
    norm_rows(token_row, ROW_ATTN, nb, RT * seq, 2 * seq)
    project(0, nb, RT, 2)
    attend(0, RT, 2)
    send_context(RT)
    send_context(LT)

    spread_far_wo(0)
    tok_fr.wait_recv()
    tok_fl.wait_recv()
    norm_rows(token_row, ROW_ATTN, nb, OP * seq, seq)
    project(0, nb, OP, 1)
    attend(0, OP, 1)
    send_context(OP)

    def add_context(layer, src, slot, count, first):
        for j in range(0, d_model, chip_cols):
            col = pl.ds(j, chip_cols)
            y = dot(cb[src, rows(slot, count), :], wob[layer, src, :, col])
            if first:
                hb[rows(slot, count), col] = tokb[rows(slot, count), col].astype(F32) + y
            else:
                hb[rows(slot, count), col] += y

    c_fr, c_fl = {}, {}

    def forward_context(slot):
        near, far = TO_RIGHT[slot], TO_RIGHT[TO_RIGHT[slot]]
        c_fr[slot] = remote(c_part(LT, near, 0), c_part(OP, far, 0), right)
        c_r[slot][0].wait_recv()
        c_fr[slot].start()
        near, far = TO_LEFT[slot], TO_LEFT[TO_LEFT[slot]]
        c_fl[slot] = remote(c_part(RT, near, 1), c_part(OP, far, 1), left)
        c_l[slot][1].wait_recv()
        c_fl[slot].start()

    forward_context(OWN)
    wo_loads[0].wait()
    wo_push[0].wait_recv()
    add_context(0, OWN, OWN, 4, True)
    forward_context(RT)
    forward_context(LT)
    share_wo_near(0)
    forward_context(OP)
    share_wo_far(0)
    for slot in (OWN, RT, LT, OP):
        c_r[slot][1].wait_recv()
        c_l[slot][0].wait_recv()
    for slot in (RT, LT, OP):
        wo_share[0][slot].wait_recv()
    start_wo(1)
    add_context(0, LT, OWN, 4, False)
    add_context(0, RT, OWN, 4, False)
    for copy in in_loads[0]:
        copy.wait()
    out_loads[0].wait()
    for copy in in_push[0]:
        copy.wait_recv()
    out_push[0].wait_recv()

    def feed_forward(layer, slot, count):
        x = mb[layer, rows(slot, count), :]
        gate = dot_rows(x, winb[layer, 0])
        lin = dot_rows(x, winb[layer, 1])
        mixed = (jax.nn.gelu(gate, approximate=True) * lin).astype(BF16)
        for j in range(0, d_model, chip_cols):
            col = pl.ds(j, chip_cols)
            pb[layer, rows(slot, count), col] = dot(mixed, woutb[layer, :, col])

    def scatter_copies(layer):
        p, ra, rb = pb.at[layer], relay_a.at[layer], relay_b.at[layer]
        rl, rr = recv_l.at[layer], recv_r.at[layer]
        row = lambda r: pl.ds(r * rows_half, rows_half)
        copies = {}
        for r in range(2):
            copies["op_r", r] = remote(part(p, OP, r, 0), ra.at[row(r), :], right)
            copies["op_l", r] = remote(part(p, OP, r, 1), rb.at[row(r), :], left)
            copies["plain_r", r] = remote(part(p, RT, r, 1), part(rl, 0, r, 1), right)
            copies["plain_l", r] = remote(part(p, LT, r, 0), part(rr, 0, r, 0), left)
            copies["sum_r", r] = remote(part(p, RT, r, 0), part(rl, 0, r, 0), right)
            copies["sum_l", r] = remote(part(p, LT, r, 1), part(rr, 0, r, 1), left)
        return copies

    def pass_on(layer, copies, r):
        a = pl.ds(RT * seq + r * rows_half, rows_half)
        b = pl.ds(LT * seq + r * rows_half, rows_half)
        row = pl.ds(r * rows_half, rows_half)
        copies["op_r", r].wait_recv()
        pb[layer, a, 0:half] += relay_a[layer, row, :]
        copies["sum_r", r].start()
        copies["op_l", r].wait_recv()
        pb[layer, b, half:d_model] += relay_b[layer, row, :]
        copies["sum_l", r].start()

    def collect(layer, copies, r):
        for name in ("plain_r", "plain_l", "sum_r", "sum_l"):
            copies[name, r].wait_recv()
        row = pl.ds(r * rows_half, rows_half)
        hb[row, :] = hb[row, :] + ((pb[layer, row, :] + recv_l[layer, row, :]) + recv_r[layer, row, :])

    rs = scatter_copies(0)
    for slot in (OWN, RT, LT, OP):
        c_fr[slot].wait_recv()
        c_fl[slot].wait_recv()
    add_context(0, OP, OP, 1, False)
    norm_rows(hidden_row, ROW_FFN, mb.at[0], OP * seq, seq)
    feed_forward(0, OP, 1)
    for r in range(2):
        rs["op_r", r].start()
        rs["op_l", r].start()
    add_context(0, OP, OWN, 3, False)
    norm_rows(hidden_row, ROW_FFN, mb.at[0], OWN * seq, 3 * seq)
    feed_forward(0, RT, 2)
    rs["plain_r", 0].start()
    rs["plain_l", 0].start()
    forward_wo(1)
    feed_forward(0, OWN, 1)
    pass_on(0, rs, 0)
    rs["plain_r", 1].start()
    rs["plain_l", 1].start()
    pass_on(0, rs, 1)
    spread_far_wo(1)
    for copy in qkv_push[1]:
        copy.start()
    wo_push[1].start()
    for copy in in_push[1]:
        copy.start()
    out_push[1].start()

    def gather_copies(ref, r):
        to_right = [remote(part(ref, OWN, r, c), part(ref, LT, r, c), right) for c in range(2)]
        to_left = [remote(part(ref, OWN, r, c), part(ref, RT, r, c), left) for c in range(2)]
        fr = remote(part(ref, LT, r, 0), part(ref, OP, r, 0), right)
        fl = remote(part(ref, RT, r, 1), part(ref, OP, r, 1), left)
        return to_right, to_left, fr, fl

    n_gather = [gather_copies(mb.at[2], r) for r in range(2)]
    for r in range(2):
        collect(0, rs, r)
        norm_rows(hidden_row, 1, mb.at[2], r * rows_half, rows_half)
        to_right, to_left, _, _ = n_gather[r]
        to_right[0].start()
        to_left[1].start()
        to_right[1].start()
        to_left[0].start()

    def forward_gather(gather):
        to_right, to_left, fr, fl = gather
        to_right[0].wait_recv()
        fr.start()
        to_left[1].wait_recv()
        fl.start()

    forward_gather(n_gather[0])
    for copy in qkv_loads[1]:
        copy.wait()
    for copy in qkv_push[1]:
        copy.wait_recv()
    for copies in c_r, c_l:
        for slot in (OWN, RT, LT, OP):
            for copy in copies[slot]:
                copy.wait_send()
                done.add(id(copy))
    project(1, mb.at[2], OWN, 1)
    attend(1, OWN, 1)
    forward_gather(n_gather[1])
    share_wo_near(1)
    share_wo_far(1)
    for r in range(2):
        n_gather[r][0][1].wait_recv()
        n_gather[r][1][0].wait_recv()
    project(1, mb.at[2], RT, 2)
    attend(1, RT, 2)
    ctx_r = remote(cb.at[0, rows(RT), :], c1b.at[LT], right)
    ctx_l = remote(cb.at[0, rows(LT), :], c1b.at[RT], left)
    ctx_o = remote(cb.at[0, rows(OP), :], c1b.at[OP], opposite)
    ctx_r.start()
    ctx_l.start()
    for r in range(2):
        n_gather[r][2].wait_recv()
        n_gather[r][3].wait_recv()
    project(1, mb.at[2], OP, 1)
    attend(1, OP, 1)
    ctx_o.start()
    wo_loads[1].wait()
    wo_push[1].wait_recv()

    def add_second(src, context):
        for j in range(0, d_model, chip_cols):
            col = pl.ds(j, chip_cols)
            hb[rows(OWN), col] += dot(context, wob[1, src, :, col])

    add_second(OWN, cb[0, rows(OWN), :])
    for slot, copy in ((LT, ctx_r), (RT, ctx_l), (OP, ctx_o)):
        wo_share[1][slot].wait_recv()
        copy.wait_recv()
        add_second(slot, c1b[slot])
    norm_rows(hidden_row, ROW_FFN + 1, mb.at[1], OWN * seq, seq)
    m_gather = [gather_copies(mb.at[1], r) for r in range(2)]
    for first, second in ((0, 1), (1, 0)):
        for r in range(2):
            m_gather[r][0][first].start()
            m_gather[r][1][second].start()
    for copy in in_loads[1]:
        copy.wait()
    out_loads[1].wait()
    for copy in in_push[1]:
        copy.wait_recv()
    out_push[1].wait_recv()
    rs = scatter_copies(1)
    feed_forward(1, OWN, 1)
    for r in range(2):
        forward_gather(m_gather[r])
    for r in range(2):
        m_gather[r][0][1].wait_recv()
        m_gather[r][1][0].wait_recv()
    feed_forward(1, RT, 2)
    rs["plain_r", 0].start()
    rs["plain_l", 0].start()
    for r in range(2):
        m_gather[r][2].wait_recv()
        m_gather[r][3].wait_recv()
    feed_forward(1, OP, 1)
    for r in range(2):
        rs["op_r", r].start()
        rs["op_l", r].start()
    rs["plain_r", 1].start()
    rs["plain_l", 1].start()
    for r in range(2):
        pass_on(1, rs, r)
    for r in range(2):
        collect(1, rs, r)
        norm_rows(hidden_row, ROW_FINAL, out, r * rows_half, rows_half)
    for copy in sent:
        if id(copy) not in done:
            copy.wait_send()


def encode(n, groups, lengths, attn_gain, ffn_gain, final_gain, bias_table, tokens, w_q, w_k, w_v, w_o, w_in0, w_in1, w_out):
    _, seq, d_model = tokens.shape
    layers, _, share = w_q.shape
    ff_share = w_out.shape[1]
    chip_cols = 2 * share
    ring = n // 2
    any_spec = pl.BlockSpec(memory_space=pl.ANY)
    vmem = pl.BlockSpec(memory_space=pltpu.VMEM)
    scratch = [
        pltpu.VMEM((SMALL_ROWS, LANES), F32),
        pltpu.VMEM((n, SMALL_ROWS, LANES), F32),
        pltpu.VMEM((8, d_model), F32),
        pltpu.VMEM((ring, 8, LANES), F32),
        pltpu.VMEM((layers, 2, seq, 2 * seq), F32),
        pltpu.VMEM((ring * seq, d_model), BF16),
        pltpu.VMEM((ring * seq, d_model), BF16),
        pltpu.VMEM((layers + 1, ring * seq, d_model), BF16),
        pltpu.VMEM((layers, d_model, 3 * chip_cols), BF16),
        pltpu.VMEM((layers, ring, chip_cols, d_model), BF16),
        pltpu.VMEM((layers, 2, 2 * ff_share, d_model), BF16),
        pltpu.VMEM((layers, 2 * ff_share, d_model), BF16),
        pltpu.VMEM((ring * seq, chip_cols), BF16),
        pltpu.VMEM((2, ring * seq, chip_cols), BF16),
        pltpu.VMEM((2, ring * seq, chip_cols), BF16),
        pltpu.VMEM((ring, ring * seq, chip_cols), BF16),
        pltpu.VMEM((ring, seq, chip_cols), BF16),
        pltpu.VMEM((ring * seq, d_model), F32),
        pltpu.VMEM((layers, ring * seq, d_model), F32),
        pltpu.VMEM((layers, seq, d_model // 2), F32),
        pltpu.VMEM((layers, seq, d_model // 2), F32),
        pltpu.VMEM((layers, seq, d_model), F32),
        pltpu.VMEM((layers, seq, d_model), F32),
        pltpu.SemaphoreType.DMA((160 + 4 * groups,)),
        pltpu.SemaphoreType.DMA((160 + 4 * groups,)),
        pltpu.SemaphoreType.DMA((24,)),
    ]
    return pl.pallas_call(
        functools.partial(kernel, n, groups),
        out_shape=pltpu.VMEM((seq, d_model), BF16),
        in_specs=[pl.BlockSpec(memory_space=pltpu.SMEM)] + [vmem] * 4 + [any_spec] * 8,
        out_specs=vmem,
        scratch_shapes=scratch,
        compiler_params=pltpu.CompilerParams(
            collective_id=0, has_side_effects=True, vmem_limit_bytes=56 * 1024 * 1024),
    )(lengths, attn_gain, ffn_gain, final_gain, bias_table, tokens, w_q, w_k, w_v, w_o, w_in0, w_in1, w_out)


def solution(mesh):
    n, groups = mesh.shape["fsdp"], mesh.shape["dp"]
    batch_spec = P(("dp", "fsdp"))
    col_spec = P(None, None, "fsdp")
    row_spec = P(None, "fsdp", None)
    gain_spec = P(None, "fsdp")
    in_specs = (batch_spec, batch_spec, gain_spec, col_spec, col_spec, col_spec, row_spec, col_spec, gain_spec,
                col_spec, col_spec, row_spec, P("fsdp"))

    def local_forward(tokens, lengths, attn_gain, w_q, w_k, w_v, w_o, rel_bias, ffn_gain, w_in0, w_in1, w_out, final_gain):
        seq_len = tokens.shape[1]
        layers, buckets, heads = rel_bias.shape
        bias_table = jnp.swapaxes(rel_bias, 1, 2).reshape(layers * heads, buckets)
        normed_out = encode(n, groups, lengths, attn_gain, ffn_gain, final_gain[None], bias_table, tokens, w_q, w_k, w_v, w_o,
                            jnp.swapaxes(w_in0, 1, 2), jnp.swapaxes(w_in1, 1, 2), w_out)
        key_ok = jnp.arange(seq_len, dtype=jnp.int32)[:, None] < lengths
        return jnp.where(key_ok, normed_out, jnp.zeros_like(normed_out))[None]

    return jax.shard_map(local_forward, mesh=mesh, in_specs=in_specs, out_specs=batch_spec, check_vma=False)
```

```python
import functools

import jax
import jax.numpy as jnp
from jax import lax
from jax.experimental import pallas as pl
from jax.experimental.pallas import tpu as pltpu
from jax.sharding import PartitionSpec as P

HEAD_DIM = 64
NUM_BUCKETS = 32
NORM_EPS = 1e-6
LANES = 128
MASKED = -1e30
MESH = pl.DeviceIdType.MESH
BF16 = jnp.bfloat16
F32 = jnp.float32

ROW_ATTN, ROW_FFN, ROW_FINAL, ROW_BIAS, ROW_LEN, SMALL_ROWS = 0, 2, 4, 5, 6, 8

OWN, RT, LT, OP = 0, 1, 2, 3
TO_RIGHT = {OWN: LT, RT: OWN, LT: OP, OP: RT}
TO_LEFT = {OWN: RT, RT: OP, LT: OWN, OP: LT}


def bucket_of(rel_pos):
    half_buckets = NUM_BUCKETS // 2
    max_exact = half_buckets // 2
    distance = jnp.abs(rel_pos)
    log_bucket = jnp.full_like(distance, max_exact)
    for step in range(1, half_buckets - max_exact):
        log_bucket += jnp.where(distance * distance >= max_exact * max_exact * 2**step, 1, 0)
    return jnp.where(rel_pos > 0, half_buckets, 0) + jnp.where(distance < max_exact, distance, log_bucket)


def dot(a, b):
    return jnp.dot(a, b, preferred_element_type=F32)


def dot_rows(a, b):
    return lax.dot_general(a, b, (((1,), (1,)), ((), ())), preferred_element_type=F32)


def kernel(n, groups, lengths, attn_gain, ffn_gain, final_gain, bias_table, tok, wq, wk, wv, wo, win0, win1, wout, out,
           smalls, sm_all, gainb, lenb, biasb, tokb, nb, mb, wqkvb, wob, winb, woutb, qb, kb, vb, cb, c1b, hb, pb,
           relay_a, relay_b, recv_l, recv_r, send_sem, recv_sem, load_sem):
    seq, d_model = tok.shape[1], tok.shape[2]
    layers = wq.shape[0]
    half, rows_half = d_model // 2, seq // 2
    share, ff_share = wq.shape[2], wout.shape[1]
    chip_cols = 2 * share

    me, group = lax.axis_index("fsdp"), lax.axis_index("dp")
    right, left = lax.rem(me + 2, n), lax.rem(me + n - 2, n)
    opposite = lax.rem(me + n // 2, n)
    partner = me + 1 - 2 * lax.rem(me, 2)
    counts = {"remote": 0, "local": 0}
    sent, done = [], set()

    def remote(src, dst, device, axis="fsdp"):
        index = counts["remote"]
        counts["remote"] += 1
        copy = pltpu.make_async_remote_copy(
            src_ref=src, dst_ref=dst, send_sem=send_sem.at[index], recv_sem=recv_sem.at[index],
            device_id={axis: device}, device_id_type=MESH)
        sent.append(copy)
        return copy

    def load(src, dst):
        index = counts["local"]
        counts["local"] += 1
        copy = pltpu.make_async_copy(src, dst, load_sem.at[index])
        copy.start()
        return copy

    def rows(slot, count=1):
        return pl.ds(slot * seq, count * seq)

    def part(ref, slot, r, c):
        row = pl.ds(slot * seq, seq) if r is None else pl.ds(slot * seq + r * rows_half, rows_half)
        col = slice(None) if c is None else pl.ds(c * half, half)
        return ref.at[row, col]

    tok_load = load(tok.at[0], tokb.at[rows(OWN), :])
    qkv_loads = []
    for layer in range(layers):
        qkv_loads.append([load(w.at[layer], wqkvb.at[layer, :, pl.ds(i * chip_cols, share)])
                          for i, w in enumerate((wq, wk, wv))])
        if layer == 0:
            wo_loads = [load(wo.at[k], wob.at[k, OWN, pl.ds(0, share), :]) for k in range(layers)]
            in_loads = []
            out_loads = []
        in_loads.append([load(w.at[layer], winb.at[layer, i, pl.ds(0, ff_share), :]) for i, w in enumerate((win0, win1))])
        out_loads.append(load(wout.at[layer], woutb.at[layer, pl.ds(0, ff_share), :]))

    smalls[ROW_ATTN:ROW_ATTN + layers, :] = attn_gain[...].astype(F32)
    smalls[ROW_FFN:ROW_FFN + layers, :] = ffn_gain[...].astype(F32)
    smalls[ROW_FINAL:ROW_FINAL + 1, :] = final_gain[...].astype(F32)
    table = bias_table[...].astype(F32)
    smalls[ROW_BIAS:ROW_BIAS + 1, :] = jnp.concatenate([table[i:i + 1] for i in range(table.shape[0])], axis=1)
    smalls[ROW_LEN:SMALL_ROWS, :] = jnp.full((SMALL_ROWS - ROW_LEN, LANES), lengths[0], jnp.int32).astype(F32)

    barrier = pltpu.get_barrier_semaphore()
    for k in range(1, n):
        pl.semaphore_signal(barrier, inc=1, device_id={"fsdp": lax.rem(me + k, n)}, device_id_type=MESH)
    for k in range(1, groups):
        pl.semaphore_signal(barrier, inc=1, device_id={"dp": lax.rem(group + k, groups)}, device_id_type=MESH)
    pl.semaphore_wait(barrier, n - 1 + groups - 1)

    def block_sends(src, dst):
        to_right = [remote(src(c), dst(LT, c), right) for c in range(2)]
        to_left = [remote(src(c), dst(RT, c), left) for c in range(2)]
        return to_right, to_left

    def block_forwards(dst):
        return remote(dst(LT, 0), dst(OP, 0), right), remote(dst(RT, 1), dst(OP, 1), left)

    row_pieces = min(groups, share // 16)
    col_pieces = groups // row_pieces
    piece_rows, piece_cols = share // row_pieces, d_model // col_pieces
    piece_row = pl.multiple_of(group // col_pieces * piece_rows, piece_rows)
    piece_col = pl.multiple_of(lax.rem(group, col_pieces) * piece_cols, piece_cols)

    def wo_copies(layer):
        col = lambda c: pl.ds(pl.multiple_of(piece_col + c * (piece_cols // 2), LANES), piece_cols // 2)
        src = lambda c: wo.at[layer, pl.ds(piece_row, piece_rows), col(c)]
        dst = lambda slot, c: wob.at[layer, slot, pl.ds(piece_row, piece_rows), col(c)]
        to_right, to_left = block_sends(src, dst)
        fr, fl = block_forwards(dst)
        piece = lambda slot, count: wob.at[layer, pl.ds(slot, count), pl.ds(piece_row, piece_rows), pl.ds(piece_col, piece_cols)]
        spread = [[remote(piece(slot, count), piece(slot, count), lax.rem(group + k, groups), "dp") for k in range(1, groups)]
                  for slot, count in ((RT, 2), (OP, 1))]
        push = {s: remote(wob.at[layer, s, pl.ds(0, share), :], wob.at[layer, s, pl.ds(share, share), :], partner)
                for s in (RT, LT, OP)}
        return to_right, to_left, fr, fl, spread, push

    wo_r, wo_l, wo_fr, wo_fl, wo_spread, wo_share = zip(*[wo_copies(layer) for layer in range(layers)])

    def start_wo(layer):
        wo_r[layer][0].start()
        wo_l[layer][1].start()
        wo_r[layer][1].start()
        wo_l[layer][0].start()

    def forward_wo(layer):
        wo_r[layer][0].wait_recv()
        wo_fr[layer].start()
        wo_l[layer][1].wait_recv()
        wo_fl[layer].start()
        wo_r[layer][1].wait_recv()
        wo_l[layer][0].wait_recv()
        for copy in wo_spread[layer][0]:
            copy.start()

    def spread_far_wo(layer):
        wo_fr[layer].wait_recv()
        wo_fl[layer].wait_recv()
        for copy in wo_spread[layer][1]:
            copy.start()

    def share_wo_near(layer):
        for copy in wo_spread[layer][0]:
            copy.wait_recv()
        wo_share[layer][LT].start()
        wo_share[layer][RT].start()

    def share_wo_far(layer):
        for copy in wo_spread[layer][1]:
            copy.wait_recv()
        wo_share[layer][OP].start()

    small_sends = [remote(smalls, sm_all.at[me], lax.rem(me + k, n)) for k in range(1, n)]
    tok_src = lambda c: part(tokb, OWN, None, c)
    tok_dst = lambda slot, c: part(tokb, slot, None, c)
    tok_r, tok_l = block_sends(tok_src, tok_dst)
    qkv_push = [[remote(w.at[layer], wqkvb.at[layer, :, pl.ds(i * chip_cols + share, share)], partner)
                 for i, w in enumerate((wq, wk, wv))] for layer in range(layers)]
    in_push = [[remote(w.at[layer], winb.at[layer, i, pl.ds(ff_share, ff_share), :], partner) for i, w in enumerate((win0, win1))]
               for layer in range(layers)]
    out_push = [remote(wout.at[layer], woutb.at[layer, pl.ds(ff_share, ff_share), :], partner) for layer in range(layers)]
    wo_push = [remote(wo.at[layer], wob.at[layer, OWN, pl.ds(share, share), :], partner) for layer in range(layers)]

    start_wo(0)
    tok_load.wait()
    tok_r[0].start()
    tok_l[1].start()
    for copy in small_sends:
        copy.start()
    tok_r[1].start()
    tok_l[0].start()
    start_wo(1)
    for copy in qkv_push[0]:
        copy.start()
    wo_push[0].start()

    sm_all[me] = smalls[...]
    for copy in small_sends:
        copy.wait_recv()
    for k in range(n):
        gainb[:, k * LANES:(k + 1) * LANES] = sm_all[k]
    for slot, device in ((OWN, me), (RT, right), (LT, left), (OP, opposite)):
        lenb[slot] = jnp.broadcast_to(sm_all[device, ROW_LEN:ROW_LEN + 1, :], (8, LANES))

    def norm_rows(load_row, gain_row, dst, start, count):
        step = 32

        def body(i, carry):
            r = pl.multiple_of(start + i * step, step)
            x = load_row(r, step)
            mean_sq = jnp.mean(x * x, axis=-1, keepdims=True)
            normed = x * lax.rsqrt(mean_sq + NORM_EPS) * gainb[gain_row:gain_row + 1, :]
            dst[pl.ds(r, step), :] = normed.astype(BF16)
            return carry

        lax.fori_loop(0, count // step, body, 0)

    def token_row(r, step):
        return tokb[pl.ds(r, step), :].astype(F32)

    def hidden_row(r, step):
        return hb[pl.ds(r, step), :]

    lane_low = lax.rem(lax.broadcasted_iota(jnp.int32, (1, chip_cols), 1), 2 * HEAD_DIM) < HEAD_DIM

    def project(layer, src, slot, count):
        x = src[rows(slot, count), :]
        q = dot(x, wqkvb[layer, :, 0:chip_cols])
        qb[rows(slot, count), :] = q.astype(BF16)
        for i, ref in ((1, kb), (2, vb)):
            y = dot(x, wqkvb[layer, :, i * chip_cols:(i + 1) * chip_cols])
            ref[0, rows(slot, count), :] = jnp.where(lane_low, y, 0.0).astype(BF16)
            ref[1, rows(slot, count), :] = jnp.where(lane_low, 0.0, y).astype(BF16)

    key_index = lax.broadcasted_iota(jnp.int32, (1, seq), 1).astype(F32)

    def attend(layer, slot, count):
        def body(i, carry):
            s = slot + i
            row = pl.ds(pl.multiple_of(s * seq, seq), seq)
            key_ok = key_index < lenb[s, 0:1, :]
            for pair in range(chip_cols // LANES):
                col = pl.ds(pair * LANES, LANES)
                keys = jnp.concatenate([kb[0, row, col], kb[1, row, col]], axis=0)
                scores = dot_rows(qb[row, col], keys)
                scores = scores + biasb[layer, pair]
                probs = []
                for h in range(2):
                    x = jnp.where(key_ok, scores[:, h * seq:(h + 1) * seq], MASKED)
                    e = jnp.exp(x - jnp.max(x, axis=-1, keepdims=True))
                    probs.append((e / jnp.sum(e, axis=-1, keepdims=True)).astype(BF16))
                values = jnp.concatenate([vb[0, row, col], vb[1, row, col]], axis=0)
                cb[0, row, col] = dot(jnp.concatenate(probs, axis=1), values).astype(BF16)
            return carry

        lax.fori_loop(0, count, body, 0)

    def build_bias():
        rel = lax.broadcasted_iota(jnp.int32, (LANES, 2 * seq), 1)
        rel = jnp.where(rel < seq, rel, rel - 2 * seq)
        lane = lax.broadcasted_iota(jnp.int32, (LANES, 2 * seq), 0)
        one_hot = jnp.where(bucket_of(rel) == lax.rem(lane, NUM_BUCKETS), 1.0, 0.0).astype(BF16)
        table_row = lax.broadcasted_iota(jnp.int32, (8, LANES), 0)
        table_lane = lax.broadcasted_iota(jnp.int32, (8, LANES), 1)
        own_lanes = table_row == table_lane // NUM_BUCKETS
        for pair, device in ((0, me), (1, partner)):
            tables = jnp.where(own_lanes, sm_all[device, ROW_BIAS:ROW_BIAS + 1, :], 0.0)
            lines = dot(tables.astype(BF16), one_hot)
            for layer in range(layers):
                for h in range(2):
                    row = 2 * layer + h
                    line = jnp.broadcast_to(lines[row:row + 1, :], (seq, 2 * seq))
                    shifted = pltpu.roll(line, 0, 1, stride=1, stride_axis=0)
                    biasb[layer, pair, :, h * seq:(h + 1) * seq] = shifted[:, 0:seq]

    norm_rows(token_row, ROW_ATTN, nb, OWN * seq, seq)
    build_bias()
    for copy in qkv_loads[0]:
        copy.wait()
    for copy in qkv_push[0]:
        copy.wait_recv()
    project(0, nb, OWN, 1)
    attend(0, OWN, 1)

    forward_wo(0)
    tok_fr, tok_fl = block_forwards(tok_dst)
    tok_r[0].wait_recv()
    tok_fr.start()
    tok_l[1].wait_recv()
    tok_fl.start()

    def c_part(src, slot, pair):
        return cb.at[src, rows(slot), pl.ds(pair * LANES, LANES)]

    c_r, c_l = {}, {}

    for slot in (OWN, RT, LT, OP):
        c_r[slot] = [remote(c_part(0, slot, p), c_part(LT, TO_RIGHT[slot], p), right) for p in range(2)]
        c_l[slot] = [remote(c_part(0, slot, p), c_part(RT, TO_LEFT[slot], p), left) for p in range(2)]

    def send_context(to_right, to_left):
        c_r[to_right][0].start()
        c_l[to_left][1].start()
        c_r[to_right][1].start()
        c_l[to_left][0].start()

    c_fr, c_fl = {}, {}

    def forward_context(slot):
        near, far = TO_RIGHT[slot], TO_RIGHT[TO_RIGHT[slot]]
        c_fr[slot] = remote(c_part(LT, near, 0), c_part(OP, far, 0), right)
        c_r[slot][0].wait_recv()
        c_fr[slot].start()
        near, far = TO_LEFT[slot], TO_LEFT[TO_LEFT[slot]]
        c_fl[slot] = remote(c_part(RT, near, 1), c_part(OP, far, 1), left)
        c_l[slot][1].wait_recv()
        c_fl[slot].start()

    send_context(OWN, OWN)

    for copy in in_push[0]:
        copy.start()
    out_push[0].start()

    spread_far_wo(0)
    tok_r[1].wait_recv()
    tok_l[0].wait_recv()
    norm_rows(token_row, ROW_ATTN, nb, RT * seq, 2 * seq)
    project(0, nb, RT, 2)
    attend(0, RT, 2)
    send_context(LT, RT)
    send_context(RT, LT)

    forward_context(OWN)
    tok_fr.wait_recv()
    tok_fl.wait_recv()
    norm_rows(token_row, ROW_ATTN, nb, OP * seq, seq)
    project(0, nb, OP, 1)
    attend(0, OP, 1)
    send_context(OP, OP)

    def add_context(slot, count):
        for j in range(0, d_model, chip_cols):
            col = pl.ds(j, chip_cols)
            y = tokb[rows(slot, count), col].astype(F32)
            for src in (OWN, RT, LT, OP):
                y += dot(cb[src, rows(slot, count), :], wob[0, src, :, col])
            hb[rows(slot, count), col] = y

    share_wo_near(0)
    forward_context(LT)
    forward_context(RT)
    share_wo_far(0)
    wo_loads[0].wait()
    wo_push[0].wait_recv()
    for copy in in_loads[0]:
        copy.wait()
    out_loads[0].wait()
    for copy in in_push[0]:
        copy.wait_recv()
    out_push[0].wait_recv()

    def feed_forward(layer, slot, count):
        x = mb[layer, rows(slot, count), :]
        gate = dot_rows(x, winb[layer, 0])
        lin = dot_rows(x, winb[layer, 1])
        mixed = (jax.nn.gelu(gate, approximate=True) * lin).astype(BF16)
        for j in range(0, d_model, chip_cols):
            col = pl.ds(j, chip_cols)
            pb[layer, rows(slot, count), col] = dot(mixed, woutb[layer, :, col])

    def scatter_copies(layer):
        p, ra, rb = pb.at[layer], relay_a.at[layer], relay_b.at[layer]
        rl, rr = recv_l.at[layer], recv_r.at[layer]
        row = lambda r: pl.ds(r * rows_half, rows_half)
        copies = {}
        for r in range(2):
            copies["op_r", r] = remote(part(p, OP, r, 0), ra.at[row(r), :], right)
            copies["op_l", r] = remote(part(p, OP, r, 1), rb.at[row(r), :], left)
            copies["plain_r", r] = remote(part(p, RT, r, 1), part(rl, 0, r, 1), right)
            copies["plain_l", r] = remote(part(p, LT, r, 0), part(rr, 0, r, 0), left)
            copies["sum_r", r] = remote(part(p, RT, r, 0), part(rl, 0, r, 0), right)
            copies["sum_l", r] = remote(part(p, LT, r, 1), part(rr, 0, r, 1), left)
        return copies

    def pass_on(layer, copies, r):
        a = pl.ds(RT * seq + r * rows_half, rows_half)
        b = pl.ds(LT * seq + r * rows_half, rows_half)
        row = pl.ds(r * rows_half, rows_half)
        copies["op_r", r].wait_recv()
        pb[layer, a, 0:half] += relay_a[layer, row, :]
        copies["sum_r", r].start()
        copies["op_l", r].wait_recv()
        pb[layer, b, half:d_model] += relay_b[layer, row, :]
        copies["sum_l", r].start()

    def collect(layer, copies, r):
        for name in ("plain_r", "plain_l", "sum_r", "sum_l"):
            copies[name, r].wait_recv()
        row = pl.ds(r * rows_half, rows_half)
        hb[row, :] = hb[row, :] + ((pb[layer, row, :] + recv_l[layer, row, :]) + recv_r[layer, row, :])

    rs = scatter_copies(0)
    c_r[LT][1].wait_recv()
    c_l[RT][0].wait_recv()
    c_fr[OWN].wait_recv()
    c_fl[OWN].wait_recv()
    for slot in (RT, LT, OP):
        wo_share[0][slot].wait_recv()
    add_context(OP, 1)
    norm_rows(hidden_row, ROW_FFN, mb.at[0], OP * seq, seq)
    feed_forward(0, OP, 1)
    for r in range(2):
        rs["op_r", r].start()
        rs["op_l", r].start()
    forward_context(OP)
    for slot in (OWN, OP):
        c_r[slot][1].wait_recv()
        c_l[slot][0].wait_recv()
    for slot in (RT, LT):
        c_fr[slot].wait_recv()
        c_fl[slot].wait_recv()
    add_context(RT, 2)
    norm_rows(hidden_row, ROW_FFN, mb.at[0], RT * seq, 2 * seq)
    feed_forward(0, RT, 2)
    rs["plain_r", 0].start()
    rs["plain_l", 0].start()
    forward_wo(1)
    c_r[RT][1].wait_recv()
    c_l[LT][0].wait_recv()
    c_fr[OP].wait_recv()
    c_fl[OP].wait_recv()
    add_context(OWN, 1)
    norm_rows(hidden_row, ROW_FFN, mb.at[0], OWN * seq, seq)
    feed_forward(0, OWN, 1)
    pass_on(0, rs, 0)
    rs["plain_r", 1].start()
    rs["plain_l", 1].start()
    pass_on(0, rs, 1)
    spread_far_wo(1)
    for copy in qkv_push[1]:
        copy.start()
    wo_push[1].start()
    for copy in in_push[1]:
        copy.start()
    out_push[1].start()

    def gather_copies(ref, r):
        to_right = [remote(part(ref, OWN, r, c), part(ref, LT, r, c), right) for c in range(2)]
        to_left = [remote(part(ref, OWN, r, c), part(ref, RT, r, c), left) for c in range(2)]
        fr = remote(part(ref, LT, r, 0), part(ref, OP, r, 0), right)
        fl = remote(part(ref, RT, r, 1), part(ref, OP, r, 1), left)
        return to_right, to_left, fr, fl

    n_gather = [gather_copies(mb.at[2], r) for r in range(2)]
    for r in range(2):
        collect(0, rs, r)
        norm_rows(hidden_row, 1, mb.at[2], r * rows_half, rows_half)
        to_right, to_left, _, _ = n_gather[r]
        to_right[0].start()
        to_left[1].start()
        to_right[1].start()
        to_left[0].start()

    def forward_gather(gather):
        to_right, to_left, fr, fl = gather
        to_right[0].wait_recv()
        fr.start()
        to_left[1].wait_recv()
        fl.start()

    forward_gather(n_gather[0])
    for copy in qkv_loads[1]:
        copy.wait()
    for copy in qkv_push[1]:
        copy.wait_recv()
    for copies in c_r, c_l:
        for slot in (OWN, RT, LT, OP):
            for copy in copies[slot]:
                copy.wait_send()
                done.add(id(copy))
    project(1, mb.at[2], OWN, 1)
    attend(1, OWN, 1)
    forward_gather(n_gather[1])
    share_wo_near(1)
    share_wo_far(1)
    for r in range(2):
        n_gather[r][0][1].wait_recv()
        n_gather[r][1][0].wait_recv()
    project(1, mb.at[2], RT, 2)
    attend(1, RT, 2)
    ctx_r = remote(cb.at[0, rows(RT), :], c1b.at[LT], right)
    ctx_l = remote(cb.at[0, rows(LT), :], c1b.at[RT], left)
    half_rows = lambda r: pl.ds(r * rows_half, rows_half)
    ctx_o = [remote(cb.at[0, pl.ds(OP * seq + r * rows_half, rows_half), :], c1b.at[OP, half_rows(r), :], opposite)
             for r in range(2)]
    ctx_r.start()
    ctx_l.start()
    for r in range(2):
        n_gather[r][2].wait_recv()
        n_gather[r][3].wait_recv()
    project(1, mb.at[2], OP, 1)
    attend(1, OP, 1)
    for copy in ctx_o:
        copy.start()
    wo_loads[1].wait()
    wo_push[1].wait_recv()

    def add_second(src, context, r=None):
        row = rows(OWN) if r is None else half_rows(r)
        for j in range(0, d_model, chip_cols):
            col = pl.ds(j, chip_cols)
            hb[row, col] += dot(context, wob[1, src, :, col])

    add_second(OWN, cb[0, rows(OWN), :])
    for slot, copy in ((LT, ctx_r), (RT, ctx_l)):
        wo_share[1][slot].wait_recv()
        copy.wait_recv()
        add_second(slot, c1b[slot])
    wo_share[1][OP].wait_recv()
    m_gather = [gather_copies(mb.at[1], r) for r in range(2)]
    for r in range(2):
        ctx_o[r].wait_recv()
        add_second(OP, c1b[OP, half_rows(r), :], r)
        norm_rows(hidden_row, ROW_FFN + 1, mb.at[1], r * rows_half, rows_half)
        to_right, to_left, _, _ = m_gather[r]
        to_right[0].start()
        to_left[1].start()
        to_right[1].start()
        to_left[0].start()
    for copy in in_loads[1]:
        copy.wait()
    out_loads[1].wait()
    for copy in in_push[1]:
        copy.wait_recv()
    out_push[1].wait_recv()
    rs = scatter_copies(1)
    feed_forward(1, OWN, 1)
    for r in range(2):
        forward_gather(m_gather[r])
    for r in range(2):
        m_gather[r][0][1].wait_recv()
        m_gather[r][1][0].wait_recv()
    feed_forward(1, RT, 2)
    rs["plain_r", 0].start()
    rs["plain_l", 0].start()
    for r in range(2):
        m_gather[r][2].wait_recv()
        m_gather[r][3].wait_recv()
    feed_forward(1, OP, 1)
    for r in range(2):
        rs["op_r", r].start()
        rs["op_l", r].start()
    rs["plain_r", 1].start()
    rs["plain_l", 1].start()
    for r in range(2):
        pass_on(1, rs, r)
    for r in range(2):
        collect(1, rs, r)
        norm_rows(hidden_row, ROW_FINAL, out, r * rows_half, rows_half)
    for copy in sent:
        if id(copy) not in done:
            copy.wait_send()


def encode(n, groups, lengths, attn_gain, ffn_gain, final_gain, bias_table, tokens, w_q, w_k, w_v, w_o, w_in0, w_in1, w_out):
    _, seq, d_model = tokens.shape
    layers, _, share = w_q.shape
    ff_share = w_out.shape[1]
    chip_cols = 2 * share
    ring = n // 2
    any_spec = pl.BlockSpec(memory_space=pl.ANY)
    vmem = pl.BlockSpec(memory_space=pltpu.VMEM)
    scratch = [
        pltpu.VMEM((SMALL_ROWS, LANES), F32),
        pltpu.VMEM((n, SMALL_ROWS, LANES), F32),
        pltpu.VMEM((8, d_model), F32),
        pltpu.VMEM((ring, 8, LANES), F32),
        pltpu.VMEM((layers, 2, seq, 2 * seq), F32),
        pltpu.VMEM((ring * seq, d_model), BF16),
        pltpu.VMEM((ring * seq, d_model), BF16),
        pltpu.VMEM((layers + 1, ring * seq, d_model), BF16),
        pltpu.VMEM((layers, d_model, 3 * chip_cols), BF16),
        pltpu.VMEM((layers, ring, chip_cols, d_model), BF16),
        pltpu.VMEM((layers, 2, 2 * ff_share, d_model), BF16),
        pltpu.VMEM((layers, 2 * ff_share, d_model), BF16),
        pltpu.VMEM((ring * seq, chip_cols), BF16),
        pltpu.VMEM((2, ring * seq, chip_cols), BF16),
        pltpu.VMEM((2, ring * seq, chip_cols), BF16),
        pltpu.VMEM((ring, ring * seq, chip_cols), BF16),
        pltpu.VMEM((ring, seq, chip_cols), BF16),
        pltpu.VMEM((ring * seq, d_model), F32),
        pltpu.VMEM((layers, ring * seq, d_model), F32),
        pltpu.VMEM((layers, seq, d_model // 2), F32),
        pltpu.VMEM((layers, seq, d_model // 2), F32),
        pltpu.VMEM((layers, seq, d_model), F32),
        pltpu.VMEM((layers, seq, d_model), F32),
        pltpu.SemaphoreType.DMA((160 + 4 * groups,)),
        pltpu.SemaphoreType.DMA((160 + 4 * groups,)),
        pltpu.SemaphoreType.DMA((24,)),
    ]
    return pl.pallas_call(
        functools.partial(kernel, n, groups),
        out_shape=pltpu.VMEM((seq, d_model), BF16),
        in_specs=[pl.BlockSpec(memory_space=pltpu.SMEM)] + [vmem] * 4 + [any_spec] * 8,
        out_specs=vmem,
        scratch_shapes=scratch,
        compiler_params=pltpu.CompilerParams(
            collective_id=0, has_side_effects=True, vmem_limit_bytes=56 * 1024 * 1024),
    )(lengths, attn_gain, ffn_gain, final_gain, bias_table, tokens, w_q, w_k, w_v, w_o, w_in0, w_in1, w_out)


def solution(mesh):
    n, groups = mesh.shape["fsdp"], mesh.shape["dp"]
    batch_spec = P(("dp", "fsdp"))
    col_spec = P(None, None, "fsdp")
    row_spec = P(None, "fsdp", None)
    gain_spec = P(None, "fsdp")
    in_specs = (batch_spec, batch_spec, gain_spec, col_spec, col_spec, col_spec, row_spec, col_spec, gain_spec,
                col_spec, col_spec, row_spec, P("fsdp"))

    def local_forward(tokens, lengths, attn_gain, w_q, w_k, w_v, w_o, rel_bias, ffn_gain, w_in0, w_in1, w_out, final_gain):
        seq_len = tokens.shape[1]
        layers, buckets, heads = rel_bias.shape
        bias_table = jnp.swapaxes(rel_bias, 1, 2).reshape(layers * heads, buckets)
        normed_out = encode(n, groups, lengths, attn_gain, ffn_gain, final_gain[None], bias_table, tokens, w_q, w_k, w_v, w_o,
                            jnp.swapaxes(w_in0, 1, 2), jnp.swapaxes(w_in1, 1, 2), w_out)
        key_ok = jnp.arange(seq_len, dtype=jnp.int32)[:, None] < lengths
        return jnp.where(key_ok, normed_out, jnp.zeros_like(normed_out))[None]

    return jax.shard_map(local_forward, mesh=mesh, in_specs=in_specs, out_specs=batch_spec, check_vma=False)
```

```python
import functools

import jax
import jax.numpy as jnp
from jax import lax
from jax.experimental import pallas as pl
from jax.experimental.pallas import tpu as pltpu
from jax.sharding import PartitionSpec as P

HEAD_DIM = 64
NUM_BUCKETS = 32
NORM_EPS = 1e-6
LANES = 128
MASKED = -1e30
MESH = pl.DeviceIdType.MESH
BF16 = jnp.bfloat16
F32 = jnp.float32

ROW_ATTN, ROW_FFN, ROW_FINAL, ROW_BIAS, ROW_LEN, SMALL_ROWS = 0, 2, 4, 5, 6, 8

OWN, RT, LT, OP = 0, 1, 2, 3
TO_RIGHT = {OWN: LT, RT: OWN, LT: OP, OP: RT}
TO_LEFT = {OWN: RT, RT: OP, LT: OWN, OP: LT}


def bucket_of(rel_pos):
    half_buckets = NUM_BUCKETS // 2
    max_exact = half_buckets // 2
    distance = jnp.abs(rel_pos)
    log_bucket = jnp.full_like(distance, max_exact)
    for step in range(1, half_buckets - max_exact):
        log_bucket += jnp.where(distance * distance >= max_exact * max_exact * 2**step, 1, 0)
    return jnp.where(rel_pos > 0, half_buckets, 0) + jnp.where(distance < max_exact, distance, log_bucket)


def dot(a, b):
    return jnp.dot(a, b, preferred_element_type=F32)


def dot_rows(a, b):
    return lax.dot_general(a, b, (((1,), (1,)), ((), ())), preferred_element_type=F32)


def kernel(n, groups, lengths, attn_gain, ffn_gain, final_gain, bias_table, tok, wq, wk, wv, wo, win0, win1, wout, out,
           smalls, sm_all, gainb, lenb, biasb, tokb, nb, mb, wqkvb, wob, winb, woutb, qb, kb, vb, cb, c1b, hb, pb,
           relay_a, relay_b, recv_l, recv_r, send_sem, recv_sem, load_sem):
    seq, d_model = tok.shape[1], tok.shape[2]
    layers = wq.shape[0]
    half, rows_half = d_model // 2, seq // 2
    share, ff_share = wq.shape[2], wout.shape[1]
    chip_cols = 2 * share

    me, group = lax.axis_index("fsdp"), lax.axis_index("dp")
    right, left = lax.rem(me + 2, n), lax.rem(me + n - 2, n)
    opposite = lax.rem(me + n // 2, n)
    partner = me + 1 - 2 * lax.rem(me, 2)
    counts = {"remote": 0, "local": 0}
    sent, done = [], set()

    def remote(src, dst, device, axis="fsdp"):
        index = counts["remote"]
        counts["remote"] += 1
        copy = pltpu.make_async_remote_copy(
            src_ref=src, dst_ref=dst, send_sem=send_sem.at[index], recv_sem=recv_sem.at[index],
            device_id={axis: device}, device_id_type=MESH)
        sent.append(copy)
        return copy

    def load(src, dst):
        index = counts["local"]
        counts["local"] += 1
        copy = pltpu.make_async_copy(src, dst, load_sem.at[index])
        copy.start()
        return copy

    def rows(slot, count=1):
        return pl.ds(slot * seq, count * seq)

    def part(ref, slot, r, c):
        row = pl.ds(slot * seq, seq) if r is None else pl.ds(slot * seq + r * rows_half, rows_half)
        col = slice(None) if c is None else pl.ds(c * half, half)
        return ref.at[row, col]

    tok_load = load(tok.at[0], tokb.at[rows(OWN), :])
    qkv_loads = []
    for layer in range(layers):
        qkv_loads.append([load(w.at[layer], wqkvb.at[layer, :, pl.ds(i * chip_cols, share)])
                          for i, w in enumerate((wq, wk, wv))])
        if layer == 0:
            wo_loads = [load(wo.at[k], wob.at[k, OWN, pl.ds(0, share), :]) for k in range(layers)]
            in_loads = []
            out_loads = []
        in_loads.append([load(w.at[layer], winb.at[layer, i, pl.ds(0, ff_share), :]) for i, w in enumerate((win0, win1))])
        out_loads.append(load(wout.at[layer], woutb.at[layer, pl.ds(0, ff_share), :]))

    smalls[ROW_ATTN:ROW_ATTN + layers, :] = attn_gain[...].astype(F32)
    smalls[ROW_FFN:ROW_FFN + layers, :] = ffn_gain[...].astype(F32)
    smalls[ROW_FINAL:ROW_FINAL + 1, :] = final_gain[...].astype(F32)
    table = bias_table[...].astype(F32)
    smalls[ROW_BIAS:ROW_BIAS + 1, :] = jnp.concatenate([table[i:i + 1] for i in range(table.shape[0])], axis=1)
    smalls[ROW_LEN:SMALL_ROWS, :] = jnp.full((SMALL_ROWS - ROW_LEN, LANES), lengths[0], jnp.int32).astype(F32)

    barrier = pltpu.get_barrier_semaphore()
    for k in range(1, n):
        pl.semaphore_signal(barrier, inc=1, device_id={"fsdp": lax.rem(me + k, n)}, device_id_type=MESH)
    for k in range(1, groups):
        pl.semaphore_signal(barrier, inc=1, device_id={"dp": lax.rem(group + k, groups)}, device_id_type=MESH)
    pl.semaphore_wait(barrier, n - 1 + groups - 1)

    def block_sends(src, dst):
        to_right = [remote(src(c), dst(LT, c), right) for c in range(2)]
        to_left = [remote(src(c), dst(RT, c), left) for c in range(2)]
        return to_right, to_left

    def block_forwards(dst):
        return remote(dst(LT, 0), dst(OP, 0), right), remote(dst(RT, 1), dst(OP, 1), left)

    row_pieces = min(groups, share // 16)
    col_pieces = groups // row_pieces
    piece_rows, piece_cols = share // row_pieces, d_model // col_pieces
    piece_row = pl.multiple_of(group // col_pieces * piece_rows, piece_rows)
    piece_col = pl.multiple_of(lax.rem(group, col_pieces) * piece_cols, piece_cols)

    def wo_copies(layer):
        col = lambda c: pl.ds(pl.multiple_of(piece_col + c * (piece_cols // 2), LANES), piece_cols // 2)
        src = lambda c: wo.at[layer, pl.ds(piece_row, piece_rows), col(c)]
        dst = lambda slot, c: wob.at[layer, slot, pl.ds(piece_row, piece_rows), col(c)]
        to_right, to_left = block_sends(src, dst)
        fr, fl = block_forwards(dst)
        piece = lambda slot, count: wob.at[layer, pl.ds(slot, count), pl.ds(piece_row, piece_rows), pl.ds(piece_col, piece_cols)]
        spread = [[remote(piece(slot, count), piece(slot, count), lax.rem(group + k, groups), "dp") for k in range(1, groups)]
                  for slot, count in ((RT, 2), (OP, 1))]
        push = {s: remote(wob.at[layer, s, pl.ds(0, share), :], wob.at[layer, s, pl.ds(share, share), :], partner)
                for s in (RT, LT, OP)}
        return to_right, to_left, fr, fl, spread, push

    wo_r, wo_l, wo_fr, wo_fl, wo_spread, wo_share = zip(*[wo_copies(layer) for layer in range(layers)])

    def start_wo(layer):
        wo_r[layer][0].start()
        wo_l[layer][1].start()
        wo_r[layer][1].start()
        wo_l[layer][0].start()

    def forward_wo(layer):
        wo_r[layer][0].wait_recv()
        wo_fr[layer].start()
        wo_l[layer][1].wait_recv()
        wo_fl[layer].start()
        wo_r[layer][1].wait_recv()
        wo_l[layer][0].wait_recv()
        for copy in wo_spread[layer][0]:
            copy.start()

    def spread_far_wo(layer):
        wo_fr[layer].wait_recv()
        wo_fl[layer].wait_recv()
        for copy in wo_spread[layer][1]:
            copy.start()

    def share_wo_near(layer):
        for copy in wo_spread[layer][0]:
            copy.wait_recv()
        wo_share[layer][LT].start()
        wo_share[layer][RT].start()

    def share_wo_far(layer):
        for copy in wo_spread[layer][1]:
            copy.wait_recv()
        wo_share[layer][OP].start()

    small_sends = [remote(smalls, sm_all.at[me], lax.rem(me + k, n)) for k in range(1, n)]
    tok_src = lambda c: part(tokb, OWN, None, c)
    tok_dst = lambda slot, c: part(tokb, slot, None, c)
    tok_r, tok_l = block_sends(tok_src, tok_dst)
    qkv_push = [[remote(w.at[layer], wqkvb.at[layer, :, pl.ds(i * chip_cols + share, share)], partner)
                 for i, w in enumerate((wq, wk, wv))] for layer in range(layers)]
    in_push = [[remote(w.at[layer], winb.at[layer, i, pl.ds(ff_share, ff_share), :], partner) for i, w in enumerate((win0, win1))]
               for layer in range(layers)]
    out_push = [remote(wout.at[layer], woutb.at[layer, pl.ds(ff_share, ff_share), :], partner) for layer in range(layers)]
    wo_push = [remote(wo.at[layer], wob.at[layer, OWN, pl.ds(share, share), :], partner) for layer in range(layers)]

    for copy in small_sends:
        copy.start()
    start_wo(0)
    tok_load.wait()
    tok_r[0].start()
    tok_l[1].start()
    tok_r[1].start()
    tok_l[0].start()
    for copy in qkv_push[0]:
        copy.start()
    wo_push[0].start()

    sm_all[me] = smalls[...]
    for copy in small_sends:
        copy.wait_recv()
    for k in range(n):
        gainb[:, k * LANES:(k + 1) * LANES] = sm_all[k]
    for slot, device in ((OWN, me), (RT, right), (LT, left), (OP, opposite)):
        lenb[slot] = jnp.broadcast_to(sm_all[device, ROW_LEN:ROW_LEN + 1, :], (8, LANES))

    def norm_rows(load_row, gain_row, dst, start, count):
        step = 32

        def body(i, carry):
            r = pl.multiple_of(start + i * step, step)
            x = load_row(r, step)
            mean_sq = jnp.mean(x * x, axis=-1, keepdims=True)
            normed = x * lax.rsqrt(mean_sq + NORM_EPS) * gainb[gain_row:gain_row + 1, :]
            dst[pl.ds(r, step), :] = normed.astype(BF16)
            return carry

        lax.fori_loop(0, count // step, body, 0)

    def token_row(r, step):
        return tokb[pl.ds(r, step), :].astype(F32)

    def hidden_row(r, step):
        return hb[pl.ds(r, step), :]

    lane_low = lax.rem(lax.broadcasted_iota(jnp.int32, (1, chip_cols), 1), 2 * HEAD_DIM) < HEAD_DIM

    def project(layer, src, slot, count):
        x = src[rows(slot, count), :]
        q = dot(x, wqkvb[layer, :, 0:chip_cols])
        qb[rows(slot, count), :] = q.astype(BF16)
        for i, ref in ((1, kb), (2, vb)):
            y = dot(x, wqkvb[layer, :, i * chip_cols:(i + 1) * chip_cols])
            ref[0, rows(slot, count), :] = jnp.where(lane_low, y, 0.0).astype(BF16)
            ref[1, rows(slot, count), :] = jnp.where(lane_low, 0.0, y).astype(BF16)

    key_index = lax.broadcasted_iota(jnp.int32, (1, seq), 1).astype(F32)

    def attend(layer, slot, count):
        def body(i, carry):
            s = slot + i
            row = pl.ds(pl.multiple_of(s * seq, seq), seq)
            key_ok = key_index < lenb[s, 0:1, :]
            for pair in range(chip_cols // LANES):
                col = pl.ds(pair * LANES, LANES)
                keys = jnp.concatenate([kb[0, row, col], kb[1, row, col]], axis=0)
                scores = dot_rows(qb[row, col], keys)
                scores = scores + biasb[layer, pair]
                probs = []
                for h in range(2):
                    x = jnp.where(key_ok, scores[:, h * seq:(h + 1) * seq], MASKED)
                    e = jnp.exp(x - jnp.max(x, axis=-1, keepdims=True))
                    probs.append((e / jnp.sum(e, axis=-1, keepdims=True)).astype(BF16))
                values = jnp.concatenate([vb[0, row, col], vb[1, row, col]], axis=0)
                cb[0, row, col] = dot(jnp.concatenate(probs, axis=1), values).astype(BF16)
            return carry

        lax.fori_loop(0, count, body, 0)

    def build_bias():
        rel = lax.broadcasted_iota(jnp.int32, (LANES, 2 * seq), 1)
        rel = jnp.where(rel < seq, rel, rel - 2 * seq)
        lane = lax.broadcasted_iota(jnp.int32, (LANES, 2 * seq), 0)
        one_hot = jnp.where(bucket_of(rel) == lax.rem(lane, NUM_BUCKETS), 1.0, 0.0).astype(BF16)
        table_row = lax.broadcasted_iota(jnp.int32, (8, LANES), 0)
        table_lane = lax.broadcasted_iota(jnp.int32, (8, LANES), 1)
        own_lanes = table_row == table_lane // NUM_BUCKETS
        for pair, device in ((0, me), (1, partner)):
            tables = jnp.where(own_lanes, sm_all[device, ROW_BIAS:ROW_BIAS + 1, :], 0.0)
            lines = dot(tables.astype(BF16), one_hot)
            for layer in range(layers):
                for h in range(2):
                    row = 2 * layer + h
                    line = jnp.broadcast_to(lines[row:row + 1, :], (seq, 2 * seq))
                    shifted = pltpu.roll(line, 0, 1, stride=1, stride_axis=0)
                    biasb[layer, pair, :, h * seq:(h + 1) * seq] = shifted[:, 0:seq]

    norm_rows(token_row, ROW_ATTN, nb, OWN * seq, seq)
    build_bias()
    for copy in qkv_loads[0]:
        copy.wait()
    for copy in qkv_push[0]:
        copy.wait_recv()
    project(0, nb, OWN, 1)
    attend(0, OWN, 1)

    forward_wo(0)
    tok_fr, tok_fl = block_forwards(tok_dst)
    tok_r[0].wait_recv()
    tok_fr.start()
    tok_l[1].wait_recv()
    tok_fl.start()

    def c_part(src, slot, pair):
        return cb.at[src, rows(slot), pl.ds(pair * LANES, LANES)]

    c_r, c_l = {}, {}

    for slot in (OWN, RT, LT, OP):
        c_r[slot] = [remote(c_part(0, slot, p), c_part(LT, TO_RIGHT[slot], p), right) for p in range(2)]
        c_l[slot] = [remote(c_part(0, slot, p), c_part(RT, TO_LEFT[slot], p), left) for p in range(2)]

    def send_context(to_right, to_left):
        c_r[to_right][0].start()
        c_l[to_left][1].start()
        c_r[to_right][1].start()
        c_l[to_left][0].start()

    c_fr, c_fl = {}, {}

    def forward_context(slot):
        near, far = TO_RIGHT[slot], TO_RIGHT[TO_RIGHT[slot]]
        c_fr[slot] = remote(c_part(LT, near, 0), c_part(OP, far, 0), right)
        c_r[slot][0].wait_recv()
        c_fr[slot].start()
        near, far = TO_LEFT[slot], TO_LEFT[TO_LEFT[slot]]
        c_fl[slot] = remote(c_part(RT, near, 1), c_part(OP, far, 1), left)
        c_l[slot][1].wait_recv()
        c_fl[slot].start()

    send_context(OWN, OWN)

    for copy in in_push[0]:
        copy.start()
    out_push[0].start()

    spread_far_wo(0)
    tok_r[1].wait_recv()
    tok_l[0].wait_recv()
    norm_rows(token_row, ROW_ATTN, nb, RT * seq, 2 * seq)
    project(0, nb, RT, 2)
    attend(0, RT, 2)
    send_context(LT, RT)
    send_context(RT, LT)

    forward_context(OWN)
    tok_fr.wait_recv()
    tok_fl.wait_recv()
    norm_rows(token_row, ROW_ATTN, nb, OP * seq, seq)
    project(0, nb, OP, 1)
    attend(0, OP, 1)
    send_context(OP, OP)
    start_wo(1)

    def add_context(slot, count):
        for j in range(0, d_model, chip_cols):
            col = pl.ds(j, chip_cols)
            y = tokb[rows(slot, count), col].astype(F32)
            for src in (OWN, RT, LT, OP):
                y += dot(cb[src, rows(slot, count), :], wob[0, src, :, col])
            hb[rows(slot, count), col] = y

    forward_context(LT)
    forward_context(RT)
    share_wo_near(0)
    share_wo_far(0)
    wo_loads[0].wait()
    wo_push[0].wait_recv()
    for copy in in_loads[0]:
        copy.wait()
    out_loads[0].wait()
    for copy in in_push[0]:
        copy.wait_recv()
    out_push[0].wait_recv()

    def feed_forward(layer, slot, count):
        x = mb[layer, rows(slot, count), :]
        gate = dot_rows(x, winb[layer, 0])
        lin = dot_rows(x, winb[layer, 1])
        mixed = (jax.nn.gelu(gate, approximate=True) * lin).astype(BF16)
        for j in range(0, d_model, chip_cols):
            col = pl.ds(j, chip_cols)
            pb[layer, rows(slot, count), col] = dot(mixed, woutb[layer, :, col])

    def scatter_copies(layer):
        p, ra, rb = pb.at[layer], relay_a.at[layer], relay_b.at[layer]
        rl, rr = recv_l.at[layer], recv_r.at[layer]
        row = lambda r: pl.ds(r * rows_half, rows_half)
        copies = {}
        for r in range(2):
            copies["op_r", r] = remote(part(p, OP, r, 0), ra.at[row(r), :], right)
            copies["op_l", r] = remote(part(p, OP, r, 1), rb.at[row(r), :], left)
            copies["plain_r", r] = remote(part(p, RT, r, 1), part(rl, 0, r, 1), right)
            copies["plain_l", r] = remote(part(p, LT, r, 0), part(rr, 0, r, 0), left)
            copies["sum_r", r] = remote(part(p, RT, r, 0), part(rl, 0, r, 0), right)
            copies["sum_l", r] = remote(part(p, LT, r, 1), part(rr, 0, r, 1), left)
        return copies

    def pass_on(layer, copies, r):
        a = pl.ds(RT * seq + r * rows_half, rows_half)
        b = pl.ds(LT * seq + r * rows_half, rows_half)
        row = pl.ds(r * rows_half, rows_half)
        copies["op_r", r].wait_recv()
        pb[layer, a, 0:half] += relay_a[layer, row, :]
        copies["sum_r", r].start()
        copies["op_l", r].wait_recv()
        pb[layer, b, half:d_model] += relay_b[layer, row, :]
        copies["sum_l", r].start()

    def collect(layer, copies, r):
        for name in ("plain_r", "plain_l", "sum_r", "sum_l"):
            copies[name, r].wait_recv()
        row = pl.ds(r * rows_half, rows_half)
        hb[row, :] = hb[row, :] + ((pb[layer, row, :] + recv_l[layer, row, :]) + recv_r[layer, row, :])

    rs = scatter_copies(0)
    c_r[LT][1].wait_recv()
    c_l[RT][0].wait_recv()
    c_fr[OWN].wait_recv()
    c_fl[OWN].wait_recv()
    for slot in (RT, LT, OP):
        wo_share[0][slot].wait_recv()
    add_context(OP, 1)
    norm_rows(hidden_row, ROW_FFN, mb.at[0], OP * seq, seq)
    feed_forward(0, OP, 1)
    forward_context(OP)
    for r in range(2):
        rs["op_r", r].start()
        rs["op_l", r].start()
    for slot in (OWN, OP):
        c_r[slot][1].wait_recv()
        c_l[slot][0].wait_recv()
    for slot in (RT, LT):
        c_fr[slot].wait_recv()
        c_fl[slot].wait_recv()
    add_context(RT, 2)
    norm_rows(hidden_row, ROW_FFN, mb.at[0], RT * seq, 2 * seq)
    feed_forward(0, RT, 2)
    rs["plain_r", 0].start()
    rs["plain_l", 0].start()
    forward_wo(1)
    c_r[RT][1].wait_recv()
    c_l[LT][0].wait_recv()
    c_fr[OP].wait_recv()
    c_fl[OP].wait_recv()
    add_context(OWN, 1)
    norm_rows(hidden_row, ROW_FFN, mb.at[0], OWN * seq, seq)
    feed_forward(0, OWN, 1)
    pass_on(0, rs, 0)
    rs["plain_r", 1].start()
    rs["plain_l", 1].start()
    pass_on(0, rs, 1)
    spread_far_wo(1)
    for copy in qkv_push[1]:
        copy.start()
    wo_push[1].start()
    for copy in in_push[1]:
        copy.start()
    out_push[1].start()

    def gather_copies(ref, r):
        to_right = [remote(part(ref, OWN, r, c), part(ref, LT, r, c), right) for c in range(2)]
        to_left = [remote(part(ref, OWN, r, c), part(ref, RT, r, c), left) for c in range(2)]
        fr = remote(part(ref, LT, r, 0), part(ref, OP, r, 0), right)
        fl = remote(part(ref, RT, r, 1), part(ref, OP, r, 1), left)
        return to_right, to_left, fr, fl

    n_gather = [gather_copies(mb.at[2], r) for r in range(2)]
    for r in range(2):
        collect(0, rs, r)
        norm_rows(hidden_row, 1, mb.at[2], r * rows_half, rows_half)
        to_right, to_left, _, _ = n_gather[r]
        to_right[0].start()
        to_left[1].start()
        to_right[1].start()
        to_left[0].start()

    def forward_gather(gather):
        to_right, to_left, fr, fl = gather
        to_right[0].wait_recv()
        fr.start()
        to_left[1].wait_recv()
        fl.start()

    forward_gather(n_gather[0])
    for copy in qkv_loads[1]:
        copy.wait()
    for copy in qkv_push[1]:
        copy.wait_recv()
    for copies in c_r, c_l:
        for slot in (OWN, RT, LT, OP):
            for copy in copies[slot]:
                copy.wait_send()
                done.add(id(copy))
    project(1, mb.at[2], OWN, 1)
    attend(1, OWN, 1)
    forward_gather(n_gather[1])
    share_wo_near(1)
    share_wo_far(1)
    for r in range(2):
        n_gather[r][0][1].wait_recv()
        n_gather[r][1][0].wait_recv()
    project(1, mb.at[2], RT, 2)
    attend(1, RT, 2)
    ctx_r = remote(cb.at[0, rows(RT), :], c1b.at[LT], right)
    ctx_l = remote(cb.at[0, rows(LT), :], c1b.at[RT], left)
    half_rows = lambda r: pl.ds(r * rows_half, rows_half)
    ctx_o = [remote(cb.at[0, pl.ds(OP * seq + r * rows_half, rows_half), :], c1b.at[OP, half_rows(r), :], opposite)
             for r in range(2)]
    ctx_r.start()
    ctx_l.start()
    for r in range(2):
        n_gather[r][2].wait_recv()
        n_gather[r][3].wait_recv()
    project(1, mb.at[2], OP, 1)
    attend(1, OP, 1)
    for copy in ctx_o:
        copy.start()
    wo_loads[1].wait()
    wo_push[1].wait_recv()

    def add_second(src, context, r=None):
        row = rows(OWN) if r is None else half_rows(r)
        for j in range(0, d_model, chip_cols):
            col = pl.ds(j, chip_cols)
            hb[row, col] += dot(context, wob[1, src, :, col])

    add_second(OWN, cb[0, rows(OWN), :])
    for slot, copy in ((LT, ctx_r), (RT, ctx_l)):
        wo_share[1][slot].wait_recv()
        copy.wait_recv()
        add_second(slot, c1b[slot])
    wo_share[1][OP].wait_recv()
    m_gather = [gather_copies(mb.at[1], r) for r in range(2)]
    for r in range(2):
        ctx_o[r].wait_recv()
        add_second(OP, c1b[OP, half_rows(r), :], r)
        norm_rows(hidden_row, ROW_FFN + 1, mb.at[1], r * rows_half, rows_half)
        to_right, to_left, _, _ = m_gather[r]
        to_right[0].start()
        to_left[1].start()
        to_right[1].start()
        to_left[0].start()
    for copy in in_loads[1]:
        copy.wait()
    out_loads[1].wait()
    for copy in in_push[1]:
        copy.wait_recv()
    out_push[1].wait_recv()
    rs = scatter_copies(1)
    feed_forward(1, OWN, 1)
    for r in range(2):
        forward_gather(m_gather[r])
    for r in range(2):
        m_gather[r][0][1].wait_recv()
        m_gather[r][1][0].wait_recv()
    feed_forward(1, RT, 2)
    rs["plain_r", 0].start()
    rs["plain_l", 0].start()
    for r in range(2):
        m_gather[r][2].wait_recv()
        m_gather[r][3].wait_recv()
    feed_forward(1, OP, 1)
    for r in range(2):
        rs["op_r", r].start()
        rs["op_l", r].start()
    rs["plain_r", 1].start()
    rs["plain_l", 1].start()
    for r in range(2):
        pass_on(1, rs, r)
    for r in range(2):
        collect(1, rs, r)
        norm_rows(hidden_row, ROW_FINAL, out, r * rows_half, rows_half)
    for copy in sent:
        if id(copy) not in done:
            copy.wait_send()


def encode(n, groups, lengths, attn_gain, ffn_gain, final_gain, bias_table, tokens, w_q, w_k, w_v, w_o, w_in0, w_in1, w_out):
    _, seq, d_model = tokens.shape
    layers, _, share = w_q.shape
    ff_share = w_out.shape[1]
    chip_cols = 2 * share
    ring = n // 2
    any_spec = pl.BlockSpec(memory_space=pl.ANY)
    vmem = pl.BlockSpec(memory_space=pltpu.VMEM)
    scratch = [
        pltpu.VMEM((SMALL_ROWS, LANES), F32),
        pltpu.VMEM((n, SMALL_ROWS, LANES), F32),
        pltpu.VMEM((8, d_model), F32),
        pltpu.VMEM((ring, 8, LANES), F32),
        pltpu.VMEM((layers, 2, seq, 2 * seq), F32),
        pltpu.VMEM((ring * seq, d_model), BF16),
        pltpu.VMEM((ring * seq, d_model), BF16),
        pltpu.VMEM((layers + 1, ring * seq, d_model), BF16),
        pltpu.VMEM((layers, d_model, 3 * chip_cols), BF16),
        pltpu.VMEM((layers, ring, chip_cols, d_model), BF16),
        pltpu.VMEM((layers, 2, 2 * ff_share, d_model), BF16),
        pltpu.VMEM((layers, 2 * ff_share, d_model), BF16),
        pltpu.VMEM((ring * seq, chip_cols), BF16),
        pltpu.VMEM((2, ring * seq, chip_cols), BF16),
        pltpu.VMEM((2, ring * seq, chip_cols), BF16),
        pltpu.VMEM((ring, ring * seq, chip_cols), BF16),
        pltpu.VMEM((ring, seq, chip_cols), BF16),
        pltpu.VMEM((ring * seq, d_model), F32),
        pltpu.VMEM((layers, ring * seq, d_model), F32),
        pltpu.VMEM((layers, seq, d_model // 2), F32),
        pltpu.VMEM((layers, seq, d_model // 2), F32),
        pltpu.VMEM((layers, seq, d_model), F32),
        pltpu.VMEM((layers, seq, d_model), F32),
        pltpu.SemaphoreType.DMA((160 + 4 * groups,)),
        pltpu.SemaphoreType.DMA((160 + 4 * groups,)),
        pltpu.SemaphoreType.DMA((24,)),
    ]
    return pl.pallas_call(
        functools.partial(kernel, n, groups),
        out_shape=pltpu.VMEM((seq, d_model), BF16),
        in_specs=[pl.BlockSpec(memory_space=pltpu.SMEM)] + [vmem] * 4 + [any_spec] * 8,
        out_specs=vmem,
        scratch_shapes=scratch,
        compiler_params=pltpu.CompilerParams(
            collective_id=0, has_side_effects=True, vmem_limit_bytes=56 * 1024 * 1024),
    )(lengths, attn_gain, ffn_gain, final_gain, bias_table, tokens, w_q, w_k, w_v, w_o, w_in0, w_in1, w_out)


def solution(mesh):
    n, groups = mesh.shape["fsdp"], mesh.shape["dp"]
    batch_spec = P(("dp", "fsdp"))
    col_spec = P(None, None, "fsdp")
    row_spec = P(None, "fsdp", None)
    gain_spec = P(None, "fsdp")
    in_specs = (batch_spec, batch_spec, gain_spec, col_spec, col_spec, col_spec, row_spec, col_spec, gain_spec,
                col_spec, col_spec, row_spec, P("fsdp"))

    def local_forward(tokens, lengths, attn_gain, w_q, w_k, w_v, w_o, rel_bias, ffn_gain, w_in0, w_in1, w_out, final_gain):
        seq_len = tokens.shape[1]
        layers, buckets, heads = rel_bias.shape
        bias_table = jnp.swapaxes(rel_bias, 1, 2).reshape(layers * heads, buckets)
        normed_out = encode(n, groups, lengths, attn_gain, ffn_gain, final_gain[None], bias_table, tokens, w_q, w_k, w_v, w_o,
                            jnp.swapaxes(w_in0, 1, 2), jnp.swapaxes(w_in1, 1, 2), w_out)
        key_ok = jnp.arange(seq_len, dtype=jnp.int32)[:, None] < lengths
        return jnp.where(key_ok, normed_out, jnp.zeros_like(normed_out))[None]

    return jax.shard_map(local_forward, mesh=mesh, in_specs=in_specs, out_specs=batch_spec, check_vma=False)
```

```python
import functools

import jax
import jax.numpy as jnp
from jax import lax
from jax.experimental import pallas as pl
from jax.experimental.pallas import tpu as pltpu
from jax.sharding import PartitionSpec as P

HEAD_DIM = 64
NUM_BUCKETS = 32
NORM_EPS = 1e-6
LANES = 128
MASKED = -1e30
MESH = pl.DeviceIdType.MESH
BF16 = jnp.bfloat16
F32 = jnp.float32

ROW_ATTN, ROW_FFN, ROW_FINAL, ROW_BIAS, ROW_LEN, SMALL_ROWS = 0, 2, 4, 5, 6, 8

OWN, RT, LT, OP = 0, 1, 2, 3
TO_RIGHT = {OWN: LT, RT: OWN, LT: OP, OP: RT}
TO_LEFT = {OWN: RT, RT: OP, LT: OWN, OP: LT}


def bucket_of(rel_pos):
    half_buckets = NUM_BUCKETS // 2
    max_exact = half_buckets // 2
    distance = jnp.abs(rel_pos)
    log_bucket = jnp.full_like(distance, max_exact)
    for step in range(1, half_buckets - max_exact):
        log_bucket += jnp.where(distance * distance >= max_exact * max_exact * 2**step, 1, 0)
    return jnp.where(rel_pos > 0, half_buckets, 0) + jnp.where(distance < max_exact, distance, log_bucket)


def dot(a, b):
    return jnp.dot(a, b, preferred_element_type=F32)


def dot_rows(a, b):
    return lax.dot_general(a, b, (((1,), (1,)), ((), ())), preferred_element_type=F32)


def kernel(n, groups, lengths, attn_gain, ffn_gain, final_gain, bias_table, tok, wq, wk, wv, wo, win0, win1, wout, out,
           smalls, sm_all, gainb, lenb, biasb, tokb, nb, mb, wqkvb, wob, winb, woutb, qb, kb, vb, cb, c1b, hb, pb,
           relay_a, relay_b, recv_l, recv_r, send_sem, recv_sem, load_sem):
    seq, d_model = tok.shape[1], tok.shape[2]
    layers = wq.shape[0]
    half, rows_half = d_model // 2, seq // 2
    share, ff_share = wq.shape[2], wout.shape[1]
    chip_cols = 2 * share

    me, group = lax.axis_index("fsdp"), lax.axis_index("dp")
    right, left = lax.rem(me + 2, n), lax.rem(me + n - 2, n)
    opposite = lax.rem(me + n // 2, n)
    partner = me + 1 - 2 * lax.rem(me, 2)
    counts = {"remote": 0, "local": 0}
    sent, done = [], set()

    def remote(src, dst, device, axis="fsdp"):
        index = counts["remote"]
        counts["remote"] += 1
        copy = pltpu.make_async_remote_copy(
            src_ref=src, dst_ref=dst, send_sem=send_sem.at[index], recv_sem=recv_sem.at[index],
            device_id={axis: device}, device_id_type=MESH)
        sent.append(copy)
        return copy

    def load(src, dst):
        index = counts["local"]
        counts["local"] += 1
        copy = pltpu.make_async_copy(src, dst, load_sem.at[index])
        copy.start()
        return copy

    def rows(slot, count=1):
        return pl.ds(slot * seq, count * seq)

    def part(ref, slot, r, c):
        row = pl.ds(slot * seq, seq) if r is None else pl.ds(slot * seq + r * rows_half, rows_half)
        col = slice(None) if c is None else pl.ds(c * half, half)
        return ref.at[row, col]

    tok_load = load(tok.at[0], tokb.at[rows(OWN), :])
    qkv_loads = []
    for layer in range(layers):
        qkv_loads.append([load(w.at[layer], wqkvb.at[layer, :, pl.ds(i * chip_cols, share)])
                          for i, w in enumerate((wq, wk, wv))])
        if layer == 0:
            wo_loads = [load(wo.at[k], wob.at[k, OWN, pl.ds(0, share), :]) for k in range(layers)]
            in_loads = []
            out_loads = []
        in_loads.append([load(w.at[layer], winb.at[layer, i, pl.ds(0, ff_share), :]) for i, w in enumerate((win0, win1))])
        out_loads.append(load(wout.at[layer], woutb.at[layer, pl.ds(0, ff_share), :]))

    smalls[ROW_ATTN:ROW_ATTN + layers, :] = attn_gain[...].astype(F32)
    smalls[ROW_FFN:ROW_FFN + layers, :] = ffn_gain[...].astype(F32)
    smalls[ROW_FINAL:ROW_FINAL + 1, :] = final_gain[...].astype(F32)
    table = bias_table[...].astype(F32)
    smalls[ROW_BIAS:ROW_BIAS + 1, :] = jnp.concatenate([table[i:i + 1] for i in range(table.shape[0])], axis=1)
    smalls[ROW_LEN:SMALL_ROWS, :] = jnp.full((SMALL_ROWS - ROW_LEN, LANES), lengths[0], jnp.int32).astype(F32)

    barrier = pltpu.get_barrier_semaphore()
    for k in range(1, n):
        pl.semaphore_signal(barrier, inc=1, device_id={"fsdp": lax.rem(me + k, n)}, device_id_type=MESH)
    for k in range(1, groups):
        pl.semaphore_signal(barrier, inc=1, device_id={"dp": lax.rem(group + k, groups)}, device_id_type=MESH)
    pl.semaphore_wait(barrier, n - 1 + groups - 1)

    def block_sends(src, dst):
        to_right = [remote(src(c), dst(LT, c), right) for c in range(2)]
        to_left = [remote(src(c), dst(RT, c), left) for c in range(2)]
        return to_right, to_left

    def block_forwards(dst):
        return remote(dst(LT, 0), dst(OP, 0), right), remote(dst(RT, 1), dst(OP, 1), left)

    row_pieces = min(groups, share // 16)
    col_pieces = groups // row_pieces
    piece_rows, piece_cols = share // row_pieces, d_model // col_pieces
    piece_row = pl.multiple_of(group // col_pieces * piece_rows, piece_rows)
    piece_col = pl.multiple_of(lax.rem(group, col_pieces) * piece_cols, piece_cols)

    def wo_copies(layer):
        col = lambda c: pl.ds(pl.multiple_of(piece_col + c * (piece_cols // 2), LANES), piece_cols // 2)
        src = lambda c: wo.at[layer, pl.ds(piece_row, piece_rows), col(c)]
        dst = lambda slot, c: wob.at[layer, slot, pl.ds(piece_row, piece_rows), col(c)]
        to_right, to_left = block_sends(src, dst)
        fr, fl = block_forwards(dst)
        piece = lambda slot, count: wob.at[layer, pl.ds(slot, count), pl.ds(piece_row, piece_rows), pl.ds(piece_col, piece_cols)]
        spread = [[remote(piece(slot, count), piece(slot, count), lax.rem(group + k, groups), "dp") for k in range(1, groups)]
                  for slot, count in ((RT, 2), (OP, 1))]
        push = {s: remote(wob.at[layer, s, pl.ds(0, share), :], wob.at[layer, s, pl.ds(share, share), :], partner)
                for s in (RT, LT, OP)}
        return to_right, to_left, fr, fl, spread, push

    wo_r, wo_l, wo_fr, wo_fl, wo_spread, wo_share = zip(*[wo_copies(layer) for layer in range(layers)])

    def start_wo(layer):
        wo_r[layer][0].start()
        wo_l[layer][1].start()
        wo_r[layer][1].start()
        wo_l[layer][0].start()

    def forward_wo(layer):
        wo_r[layer][0].wait_recv()
        wo_fr[layer].start()
        wo_l[layer][1].wait_recv()
        wo_fl[layer].start()
        wo_r[layer][1].wait_recv()
        wo_l[layer][0].wait_recv()
        for copy in wo_spread[layer][0]:
            copy.start()

    def spread_far_wo(layer):
        wo_fr[layer].wait_recv()
        wo_fl[layer].wait_recv()
        for copy in wo_spread[layer][1]:
            copy.start()

    def share_wo_near(layer):
        for copy in wo_spread[layer][0]:
            copy.wait_recv()
        wo_share[layer][LT].start()
        wo_share[layer][RT].start()

    def share_wo_far(layer):
        for copy in wo_spread[layer][1]:
            copy.wait_recv()
        wo_share[layer][OP].start()

    small_sends = [remote(smalls, sm_all.at[me], lax.rem(me + k, n)) for k in range(1, n)]
    tok_src = lambda c: part(tokb, OWN, None, c)
    tok_dst = lambda slot, c: part(tokb, slot, None, c)
    tok_r, tok_l = block_sends(tok_src, tok_dst)
    def to_partner(ref):
        return lambda own, other: remote(ref(own), ref(other), partner)

    qkv_push = [[to_partner(lambda o, i=i: wqkvb.at[layer, :, pl.ds(i * chip_cols + o * share, share)])(0, 1)
                 for i in range(3)] for layer in range(layers)]
    in_push = [[to_partner(lambda o, i=i: winb.at[layer, i, pl.ds(o * ff_share, ff_share), :])(0, 1) for i in range(2)]
               for layer in range(layers)]
    out_push = [to_partner(lambda o: woutb.at[layer, pl.ds(o * ff_share, ff_share), :])(0, 1) for layer in range(layers)]
    wo_push = [to_partner(lambda o: wob.at[layer, OWN, pl.ds(o * share, share), :])(0, 1) for layer in range(layers)]

    for copy in small_sends:
        copy.start()
    start_wo(0)
    tok_load.wait()
    tok_r[0].start()
    tok_l[1].start()
    tok_r[1].start()
    tok_l[0].start()
    for load_copy, copy in zip(qkv_loads[0], qkv_push[0]):
        load_copy.wait()
        copy.start()
    wo_loads[0].wait()
    wo_push[0].start()
    for load_copy, copy in zip(in_loads[0], in_push[0]):
        load_copy.wait()
        copy.start()
    out_loads[0].wait()
    out_push[0].start()

    sm_all[me] = smalls[...]
    for copy in small_sends:
        copy.wait_recv()
    for k in range(n):
        gainb[:, k * LANES:(k + 1) * LANES] = sm_all[k]
    for slot, device in ((OWN, me), (RT, right), (LT, left), (OP, opposite)):
        lenb[slot] = jnp.broadcast_to(sm_all[device, ROW_LEN:ROW_LEN + 1, :], (8, LANES))

    def norm_rows(load_row, gain_row, dst, start, count):
        step = 32

        def body(i, carry):
            r = pl.multiple_of(start + i * step, step)
            x = load_row(r, step)
            mean_sq = jnp.mean(x * x, axis=-1, keepdims=True)
            normed = x * lax.rsqrt(mean_sq + NORM_EPS) * gainb[gain_row:gain_row + 1, :]
            dst[pl.ds(r, step), :] = normed.astype(BF16)
            return carry

        lax.fori_loop(0, count // step, body, 0)

    def token_row(r, step):
        return tokb[pl.ds(r, step), :].astype(F32)

    def hidden_row(r, step):
        return hb[pl.ds(r, step), :]

    lane_low = lax.rem(lax.broadcasted_iota(jnp.int32, (1, chip_cols), 1), 2 * HEAD_DIM) < HEAD_DIM

    def project(layer, src, slot, count):
        x = src[rows(slot, count), :]
        q = dot(x, wqkvb[layer, :, 0:chip_cols])
        qb[rows(slot, count), :] = q.astype(BF16)
        for i, ref in ((1, kb), (2, vb)):
            y = dot(x, wqkvb[layer, :, i * chip_cols:(i + 1) * chip_cols])
            ref[0, rows(slot, count), :] = jnp.where(lane_low, y, 0.0).astype(BF16)
            ref[1, rows(slot, count), :] = jnp.where(lane_low, 0.0, y).astype(BF16)

    key_index = lax.broadcasted_iota(jnp.int32, (1, seq), 1).astype(F32)

    def attend(layer, slot, count):
        def body(i, carry):
            s = slot + i
            row = pl.ds(pl.multiple_of(s * seq, seq), seq)
            key_ok = key_index < lenb[s, 0:1, :]
            for pair in range(chip_cols // LANES):
                col = pl.ds(pair * LANES, LANES)
                keys = jnp.concatenate([kb[0, row, col], kb[1, row, col]], axis=0)
                scores = dot_rows(qb[row, col], keys)
                scores = scores + biasb[layer, pair]
                probs = []
                for h in range(2):
                    x = jnp.where(key_ok, scores[:, h * seq:(h + 1) * seq], MASKED)
                    e = jnp.exp(x - jnp.max(x, axis=-1, keepdims=True))
                    probs.append((e / jnp.sum(e, axis=-1, keepdims=True)).astype(BF16))
                values = jnp.concatenate([vb[0, row, col], vb[1, row, col]], axis=0)
                cb[0, row, col] = dot(jnp.concatenate(probs, axis=1), values).astype(BF16)
            return carry

        lax.fori_loop(0, count, body, 0)

    def build_bias():
        rel = lax.broadcasted_iota(jnp.int32, (LANES, 2 * seq), 1)
        rel = jnp.where(rel < seq, rel, rel - 2 * seq)
        lane = lax.broadcasted_iota(jnp.int32, (LANES, 2 * seq), 0)
        one_hot = jnp.where(bucket_of(rel) == lax.rem(lane, NUM_BUCKETS), 1.0, 0.0).astype(BF16)
        table_row = lax.broadcasted_iota(jnp.int32, (8, LANES), 0)
        table_lane = lax.broadcasted_iota(jnp.int32, (8, LANES), 1)
        own_lanes = table_row == table_lane // NUM_BUCKETS
        for pair, device in ((0, me), (1, partner)):
            tables = jnp.where(own_lanes, sm_all[device, ROW_BIAS:ROW_BIAS + 1, :], 0.0)
            lines = dot(tables.astype(BF16), one_hot)
            for layer in range(layers):
                for h in range(2):
                    row = 2 * layer + h
                    line = jnp.broadcast_to(lines[row:row + 1, :], (seq, 2 * seq))
                    shifted = pltpu.roll(line, 0, 1, stride=1, stride_axis=0)
                    biasb[layer, pair, :, h * seq:(h + 1) * seq] = shifted[:, 0:seq]

    norm_rows(token_row, ROW_ATTN, nb, OWN * seq, seq)
    build_bias()
    for copy in qkv_push[0]:
        copy.wait_recv()
    project(0, nb, OWN, 1)
    attend(0, OWN, 1)

    forward_wo(0)
    tok_fr, tok_fl = block_forwards(tok_dst)
    tok_r[0].wait_recv()
    tok_fr.start()
    tok_l[1].wait_recv()
    tok_fl.start()

    def c_part(src, slot, pair):
        return cb.at[src, rows(slot), pl.ds(pair * LANES, LANES)]

    c_r, c_l = {}, {}

    for slot in (OWN, RT, LT, OP):
        c_r[slot] = [remote(c_part(0, slot, p), c_part(LT, TO_RIGHT[slot], p), right) for p in range(2)]
        c_l[slot] = [remote(c_part(0, slot, p), c_part(RT, TO_LEFT[slot], p), left) for p in range(2)]

    def send_context(to_right, to_left):
        c_r[to_right][0].start()
        c_l[to_left][1].start()
        c_r[to_right][1].start()
        c_l[to_left][0].start()

    c_fr, c_fl = {}, {}

    def forward_context(slot):
        near, far = TO_RIGHT[slot], TO_RIGHT[TO_RIGHT[slot]]
        c_fr[slot] = remote(c_part(LT, near, 0), c_part(OP, far, 0), right)
        c_r[slot][0].wait_recv()
        c_fr[slot].start()
        near, far = TO_LEFT[slot], TO_LEFT[TO_LEFT[slot]]
        c_fl[slot] = remote(c_part(RT, near, 1), c_part(OP, far, 1), left)
        c_l[slot][1].wait_recv()
        c_fl[slot].start()

    send_context(OWN, OWN)

    spread_far_wo(0)
    tok_r[1].wait_recv()
    tok_l[0].wait_recv()
    norm_rows(token_row, ROW_ATTN, nb, RT * seq, 2 * seq)
    project(0, nb, RT, 2)
    attend(0, RT, 2)
    send_context(LT, RT)
    send_context(RT, LT)

    forward_context(OWN)
    tok_fr.wait_recv()
    tok_fl.wait_recv()
    norm_rows(token_row, ROW_ATTN, nb, OP * seq, seq)
    project(0, nb, OP, 1)
    attend(0, OP, 1)
    send_context(OP, OP)
    start_wo(1)

    def add_context(slot, count):
        for j in range(0, d_model, chip_cols):
            col = pl.ds(j, chip_cols)
            y = tokb[rows(slot, count), col].astype(F32)
            for src in (OWN, RT, LT, OP):
                y += dot(cb[src, rows(slot, count), :], wob[0, src, :, col])
            hb[rows(slot, count), col] = y

    forward_context(LT)
    forward_context(RT)
    share_wo_near(0)
    share_wo_far(0)
    wo_push[0].wait_recv()
    for copy in in_push[0]:
        copy.wait_recv()
    out_push[0].wait_recv()

    def feed_forward(layer, slot, count):
        x = mb[layer, rows(slot, count), :]
        gate = dot_rows(x, winb[layer, 0])
        lin = dot_rows(x, winb[layer, 1])
        mixed = (jax.nn.gelu(gate, approximate=True) * lin).astype(BF16)
        for j in range(0, d_model, chip_cols):
            col = pl.ds(j, chip_cols)
            pb[layer, rows(slot, count), col] = dot(mixed, woutb[layer, :, col])

    def scatter_copies(layer):
        p, ra, rb = pb.at[layer], relay_a.at[layer], relay_b.at[layer]
        rl, rr = recv_l.at[layer], recv_r.at[layer]
        row = lambda r: pl.ds(r * rows_half, rows_half)
        copies = {}
        for r in range(2):
            copies["op_r", r] = remote(part(p, OP, r, 0), ra.at[row(r), :], right)
            copies["op_l", r] = remote(part(p, OP, r, 1), rb.at[row(r), :], left)
            copies["plain_r", r] = remote(part(p, RT, r, 1), part(rl, 0, r, 1), right)
            copies["plain_l", r] = remote(part(p, LT, r, 0), part(rr, 0, r, 0), left)
            copies["sum_r", r] = remote(part(p, RT, r, 0), part(rl, 0, r, 0), right)
            copies["sum_l", r] = remote(part(p, LT, r, 1), part(rr, 0, r, 1), left)
        return copies

    def pass_on(layer, copies, r):
        a = pl.ds(RT * seq + r * rows_half, rows_half)
        b = pl.ds(LT * seq + r * rows_half, rows_half)
        row = pl.ds(r * rows_half, rows_half)
        copies["op_r", r].wait_recv()
        pb[layer, a, 0:half] += relay_a[layer, row, :]
        copies["sum_r", r].start()
        copies["op_l", r].wait_recv()
        pb[layer, b, half:d_model] += relay_b[layer, row, :]
        copies["sum_l", r].start()

    def collect(layer, copies, r):
        for name in ("plain_r", "plain_l", "sum_r", "sum_l"):
            copies[name, r].wait_recv()
        row = pl.ds(r * rows_half, rows_half)
        hb[row, :] = hb[row, :] + ((pb[layer, row, :] + recv_l[layer, row, :]) + recv_r[layer, row, :])

    rs = scatter_copies(0)
    c_r[LT][1].wait_recv()
    c_l[RT][0].wait_recv()
    c_fr[OWN].wait_recv()
    c_fl[OWN].wait_recv()
    for slot in (RT, LT, OP):
        wo_share[0][slot].wait_recv()
    add_context(OP, 1)
    norm_rows(hidden_row, ROW_FFN, mb.at[0], OP * seq, seq)
    feed_forward(0, OP, 1)
    forward_context(OP)
    for r in range(2):
        rs["op_r", r].start()
        rs["op_l", r].start()
    for slot in (OWN, OP):
        c_r[slot][1].wait_recv()
        c_l[slot][0].wait_recv()
    for slot in (RT, LT):
        c_fr[slot].wait_recv()
        c_fl[slot].wait_recv()
    add_context(RT, 2)
    norm_rows(hidden_row, ROW_FFN, mb.at[0], RT * seq, 2 * seq)
    feed_forward(0, RT, 2)
    rs["plain_r", 0].start()
    rs["plain_l", 0].start()
    forward_wo(1)
    c_r[RT][1].wait_recv()
    c_l[LT][0].wait_recv()
    c_fr[OP].wait_recv()
    c_fl[OP].wait_recv()
    add_context(OWN, 1)
    norm_rows(hidden_row, ROW_FFN, mb.at[0], OWN * seq, seq)
    feed_forward(0, OWN, 1)
    pass_on(0, rs, 0)
    rs["plain_r", 1].start()
    rs["plain_l", 1].start()
    pass_on(0, rs, 1)
    spread_far_wo(1)
    for load_copy, copy in zip(qkv_loads[1], qkv_push[1]):
        load_copy.wait()
        copy.start()
    wo_loads[1].wait()
    wo_push[1].start()
    for load_copy, copy in zip(in_loads[1], in_push[1]):
        load_copy.wait()
        copy.start()
    out_loads[1].wait()
    out_push[1].start()

    def gather_copies(ref, r):
        to_right = [remote(part(ref, OWN, r, c), part(ref, LT, r, c), right) for c in range(2)]
        to_left = [remote(part(ref, OWN, r, c), part(ref, RT, r, c), left) for c in range(2)]
        fr = remote(part(ref, LT, r, 0), part(ref, OP, r, 0), right)
        fl = remote(part(ref, RT, r, 1), part(ref, OP, r, 1), left)
        return to_right, to_left, fr, fl

    n_gather = [gather_copies(mb.at[2], r) for r in range(2)]
    for r in range(2):
        collect(0, rs, r)
        norm_rows(hidden_row, 1, mb.at[2], r * rows_half, rows_half)
        to_right, to_left, _, _ = n_gather[r]
        to_right[0].start()
        to_left[1].start()
        to_right[1].start()
        to_left[0].start()

    def forward_gather(gather):
        to_right, to_left, fr, fl = gather
        to_right[0].wait_recv()
        fr.start()
        to_left[1].wait_recv()
        fl.start()

    forward_gather(n_gather[0])
    for copy in qkv_push[1]:
        copy.wait_recv()
    for copies in c_r, c_l:
        for slot in (OWN, RT, LT, OP):
            for copy in copies[slot]:
                copy.wait_send()
                done.add(id(copy))
    project(1, mb.at[2], OWN, 1)
    attend(1, OWN, 1)
    forward_gather(n_gather[1])
    share_wo_near(1)
    share_wo_far(1)
    for r in range(2):
        n_gather[r][0][1].wait_recv()
        n_gather[r][1][0].wait_recv()
    project(1, mb.at[2], RT, 2)
    attend(1, RT, 2)
    ctx_r = remote(cb.at[0, rows(RT), :], c1b.at[LT], right)
    ctx_l = remote(cb.at[0, rows(LT), :], c1b.at[RT], left)
    half_rows = lambda r: pl.ds(r * rows_half, rows_half)
    ctx_o = [remote(cb.at[0, pl.ds(OP * seq + r * rows_half, rows_half), :], c1b.at[OP, half_rows(r), :], opposite)
             for r in range(2)]
    ctx_r.start()
    ctx_l.start()
    for r in range(2):
        n_gather[r][2].wait_recv()
        n_gather[r][3].wait_recv()
    project(1, mb.at[2], OP, 1)
    attend(1, OP, 1)
    for copy in ctx_o:
        copy.start()
    wo_push[1].wait_recv()

    def add_second(src, context, r=None):
        row = rows(OWN) if r is None else half_rows(r)
        for j in range(0, d_model, chip_cols):
            col = pl.ds(j, chip_cols)
            hb[row, col] += dot(context, wob[1, src, :, col])

    add_second(OWN, cb[0, rows(OWN), :])
    for slot, copy in ((LT, ctx_r), (RT, ctx_l)):
        wo_share[1][slot].wait_recv()
        copy.wait_recv()
        add_second(slot, c1b[slot])
    wo_share[1][OP].wait_recv()
    m_gather = [gather_copies(mb.at[1], r) for r in range(2)]
    for r in range(2):
        ctx_o[r].wait_recv()
        add_second(OP, c1b[OP, half_rows(r), :], r)
        norm_rows(hidden_row, ROW_FFN + 1, mb.at[1], r * rows_half, rows_half)
        to_right, to_left, _, _ = m_gather[r]
        to_right[0].start()
        to_left[1].start()
        to_right[1].start()
        to_left[0].start()
    for copy in in_push[1]:
        copy.wait_recv()
    out_push[1].wait_recv()
    rs = scatter_copies(1)
    feed_forward(1, OWN, 1)
    for r in range(2):
        forward_gather(m_gather[r])
    for r in range(2):
        m_gather[r][0][1].wait_recv()
        m_gather[r][1][0].wait_recv()
    feed_forward(1, RT, 2)
    rs["plain_r", 0].start()
    rs["plain_l", 0].start()
    for r in range(2):
        m_gather[r][2].wait_recv()
        m_gather[r][3].wait_recv()
    feed_forward(1, OP, 1)
    for r in range(2):
        rs["op_r", r].start()
        rs["op_l", r].start()
    rs["plain_r", 1].start()
    rs["plain_l", 1].start()
    for r in range(2):
        pass_on(1, rs, r)
    for r in range(2):
        collect(1, rs, r)
        norm_rows(hidden_row, ROW_FINAL, out, r * rows_half, rows_half)
    for copy in sent:
        if id(copy) not in done:
            copy.wait_send()


def encode(n, groups, lengths, attn_gain, ffn_gain, final_gain, bias_table, tokens, w_q, w_k, w_v, w_o, w_in0, w_in1, w_out):
    _, seq, d_model = tokens.shape
    layers, _, share = w_q.shape
    ff_share = w_out.shape[1]
    chip_cols = 2 * share
    ring = n // 2
    any_spec = pl.BlockSpec(memory_space=pl.ANY)
    vmem = pl.BlockSpec(memory_space=pltpu.VMEM)
    scratch = [
        pltpu.VMEM((SMALL_ROWS, LANES), F32),
        pltpu.VMEM((n, SMALL_ROWS, LANES), F32),
        pltpu.VMEM((8, d_model), F32),
        pltpu.VMEM((ring, 8, LANES), F32),
        pltpu.VMEM((layers, 2, seq, 2 * seq), F32),
        pltpu.VMEM((ring * seq, d_model), BF16),
        pltpu.VMEM((ring * seq, d_model), BF16),
        pltpu.VMEM((layers + 1, ring * seq, d_model), BF16),
        pltpu.VMEM((layers, d_model, 3 * chip_cols), BF16),
        pltpu.VMEM((layers, ring, chip_cols, d_model), BF16),
        pltpu.VMEM((layers, 2, 2 * ff_share, d_model), BF16),
        pltpu.VMEM((layers, 2 * ff_share, d_model), BF16),
        pltpu.VMEM((ring * seq, chip_cols), BF16),
        pltpu.VMEM((2, ring * seq, chip_cols), BF16),
        pltpu.VMEM((2, ring * seq, chip_cols), BF16),
        pltpu.VMEM((ring, ring * seq, chip_cols), BF16),
        pltpu.VMEM((ring, seq, chip_cols), BF16),
        pltpu.VMEM((ring * seq, d_model), F32),
        pltpu.VMEM((layers, ring * seq, d_model), F32),
        pltpu.VMEM((layers, seq, d_model // 2), F32),
        pltpu.VMEM((layers, seq, d_model // 2), F32),
        pltpu.VMEM((layers, seq, d_model), F32),
        pltpu.VMEM((layers, seq, d_model), F32),
        pltpu.SemaphoreType.DMA((160 + 4 * groups,)),
        pltpu.SemaphoreType.DMA((160 + 4 * groups,)),
        pltpu.SemaphoreType.DMA((24,)),
    ]
    return pl.pallas_call(
        functools.partial(kernel, n, groups),
        out_shape=pltpu.VMEM((seq, d_model), BF16),
        in_specs=[pl.BlockSpec(memory_space=pltpu.SMEM)] + [vmem] * 4 + [any_spec] * 8,
        out_specs=vmem,
        scratch_shapes=scratch,
        compiler_params=pltpu.CompilerParams(
            collective_id=0, has_side_effects=True, vmem_limit_bytes=56 * 1024 * 1024),
    )(lengths, attn_gain, ffn_gain, final_gain, bias_table, tokens, w_q, w_k, w_v, w_o, w_in0, w_in1, w_out)


def solution(mesh):
    n, groups = mesh.shape["fsdp"], mesh.shape["dp"]
    batch_spec = P(("dp", "fsdp"))
    col_spec = P(None, None, "fsdp")
    row_spec = P(None, "fsdp", None)
    gain_spec = P(None, "fsdp")
    in_specs = (batch_spec, batch_spec, gain_spec, col_spec, col_spec, col_spec, row_spec, col_spec, gain_spec,
                col_spec, col_spec, row_spec, P("fsdp"))

    def local_forward(tokens, lengths, attn_gain, w_q, w_k, w_v, w_o, rel_bias, ffn_gain, w_in0, w_in1, w_out, final_gain):
        seq_len = tokens.shape[1]
        layers, buckets, heads = rel_bias.shape
        bias_table = jnp.swapaxes(rel_bias, 1, 2).reshape(layers * heads, buckets)
        normed_out = encode(n, groups, lengths, attn_gain, ffn_gain, final_gain[None], bias_table, tokens, w_q, w_k, w_v, w_o,
                            jnp.swapaxes(w_in0, 1, 2), jnp.swapaxes(w_in1, 1, 2), w_out)
        key_ok = jnp.arange(seq_len, dtype=jnp.int32)[:, None] < lengths
        return jnp.where(key_ok, normed_out, jnp.zeros_like(normed_out))[None]

    return jax.shard_map(local_forward, mesh=mesh, in_specs=in_specs, out_specs=batch_spec, check_vma=False)
```

```python
import functools

import jax
import jax.numpy as jnp
from jax import lax
from jax.experimental import pallas as pl
from jax.experimental.pallas import tpu as pltpu
from jax.sharding import PartitionSpec as P

HEAD_DIM = 64
NUM_BUCKETS = 32
NORM_EPS = 1e-6
LANES = 128
MASKED = -1e30
MESH = pl.DeviceIdType.MESH
BF16 = jnp.bfloat16
F32 = jnp.float32

ROW_ATTN, ROW_FFN, ROW_FINAL, ROW_BIAS, ROW_LEN, SMALL_ROWS = 0, 2, 4, 5, 6, 8

OWN, RT, LT, OP = 0, 1, 2, 3
TO_RIGHT = {OWN: LT, RT: OWN, LT: OP, OP: RT}
TO_LEFT = {OWN: RT, RT: OP, LT: OWN, OP: LT}


def bucket_of(rel_pos):
    half_buckets = NUM_BUCKETS // 2
    max_exact = half_buckets // 2
    distance = jnp.abs(rel_pos)
    log_bucket = jnp.full_like(distance, max_exact)
    for step in range(1, half_buckets - max_exact):
        log_bucket += jnp.where(distance * distance >= max_exact * max_exact * 2**step, 1, 0)
    return jnp.where(rel_pos > 0, half_buckets, 0) + jnp.where(distance < max_exact, distance, log_bucket)


def dot(a, b):
    return jnp.dot(a, b, preferred_element_type=F32)


def dot_rows(a, b):
    return lax.dot_general(a, b, (((1,), (1,)), ((), ())), preferred_element_type=F32)


def kernel(n, groups, lengths, attn_gain, ffn_gain, final_gain, bias_table, tok, wq, wk, wv, wo, win0, win1, wout, out,
           smalls, sm_all, gainb, lenb, biasb, tokb, nb, mb, wqkvb, wob, winb, woutb, qb, kb, vb, cb, c1b, relay_c, hb, pb,
           relay_a, relay_b, recv_l, recv_r, send_sem, recv_sem, load_sem):
    seq, d_model = tok.shape[1], tok.shape[2]
    layers = wq.shape[0]
    half, rows_half = d_model // 2, seq // 2
    share, ff_share = wq.shape[2], wout.shape[1]
    chip_cols = 2 * share

    me, group = lax.axis_index("fsdp"), lax.axis_index("dp")
    right, left = lax.rem(me + 2, n), lax.rem(me + n - 2, n)
    opposite = lax.rem(me + n // 2, n)
    partner = me + 1 - 2 * lax.rem(me, 2)
    counts = {"remote": 0, "local": 0}
    sent, done = [], set()

    def remote(src, dst, device, axis="fsdp"):
        index = counts["remote"]
        counts["remote"] += 1
        copy = pltpu.make_async_remote_copy(
            src_ref=src, dst_ref=dst, send_sem=send_sem.at[index], recv_sem=recv_sem.at[index],
            device_id={axis: device}, device_id_type=MESH)
        sent.append(copy)
        return copy

    def load(src, dst):
        index = counts["local"]
        counts["local"] += 1
        copy = pltpu.make_async_copy(src, dst, load_sem.at[index])
        copy.start()
        return copy

    def rows(slot, count=1):
        return pl.ds(slot * seq, count * seq)

    def part(ref, slot, r, c):
        row = pl.ds(slot * seq, seq) if r is None else pl.ds(slot * seq + r * rows_half, rows_half)
        col = slice(None) if c is None else pl.ds(c * half, half)
        return ref.at[row, col]

    tok_load = load(tok.at[0], tokb.at[rows(OWN), :])
    wo_loads = [load(wo.at[layer], wob.at[layer, OWN, pl.ds(0, share), :]) for layer in range(layers)]
    qkv_loads = []
    for layer in range(layers):
        qkv_loads.append([load(w.at[layer], wqkvb.at[layer, :, pl.ds(i * chip_cols, share)])
                          for i, w in enumerate((wq, wk, wv))])
        if layer == 0:
            in_loads = []
            out_loads = []
        in_loads.append([load(w.at[layer], winb.at[layer, i, pl.ds(0, ff_share), :]) for i, w in enumerate((win0, win1))])
        out_loads.append(load(wout.at[layer], woutb.at[layer, pl.ds(0, ff_share), :]))

    smalls[ROW_ATTN:ROW_ATTN + layers, :] = attn_gain[...].astype(F32)
    smalls[ROW_FFN:ROW_FFN + layers, :] = ffn_gain[...].astype(F32)
    smalls[ROW_FINAL:ROW_FINAL + 1, :] = final_gain[...].astype(F32)
    table = bias_table[...].astype(F32)
    smalls[ROW_BIAS:ROW_BIAS + 1, :] = jnp.concatenate([table[i:i + 1] for i in range(table.shape[0])], axis=1)
    smalls[ROW_LEN:SMALL_ROWS, :] = jnp.full((SMALL_ROWS - ROW_LEN, LANES), lengths[0], jnp.int32).astype(F32)

    barrier = pltpu.get_barrier_semaphore()
    for k in range(1, n):
        pl.semaphore_signal(barrier, inc=1, device_id={"fsdp": lax.rem(me + k, n)}, device_id_type=MESH)
    for k in range(1, groups):
        pl.semaphore_signal(barrier, inc=1, device_id={"dp": lax.rem(group + k, groups)}, device_id_type=MESH)
    pl.semaphore_wait(barrier, n - 1 + groups - 1)

    def block_sends(src, dst):
        to_right = [remote(src(c), dst(LT, c), right) for c in range(2)]
        to_left = [remote(src(c), dst(RT, c), left) for c in range(2)]
        return to_right, to_left

    def block_forwards(dst):
        return remote(dst(LT, 0), dst(OP, 0), right), remote(dst(RT, 1), dst(OP, 1), left)

    row_pieces = min(groups, share // 16)
    col_pieces = groups // row_pieces
    piece_rows, piece_cols = share // row_pieces, d_model // col_pieces
    piece_row = pl.multiple_of(group // col_pieces * piece_rows, piece_rows)
    piece_col = pl.multiple_of(lax.rem(group, col_pieces) * piece_cols, piece_cols)

    def wo_copies(layer):
        col = lambda c: pl.ds(pl.multiple_of(piece_col + c * (piece_cols // 2), LANES), piece_cols // 2)
        src = lambda c: wob.at[layer, OWN, pl.ds(piece_row, piece_rows), col(c)]
        dst = lambda slot, c: wob.at[layer, slot, pl.ds(piece_row, piece_rows), col(c)]
        to_right, to_left = block_sends(src, dst)
        fr, fl = block_forwards(dst)
        piece = lambda slot, count: wob.at[layer, pl.ds(slot, count), pl.ds(piece_row, piece_rows), pl.ds(piece_col, piece_cols)]
        spread = [[remote(piece(slot, count), piece(slot, count), lax.rem(group + k, groups), "dp") for k in range(1, groups)]
                  for slot, count in ((RT, 2), (OP, 1))]
        push = {s: remote(wob.at[layer, s, pl.ds(0, share), :], wob.at[layer, s, pl.ds(share, share), :], partner)
                for s in (RT, LT, OP)}
        return to_right, to_left, fr, fl, spread, push

    wo_r, wo_l, wo_fr, wo_fl, wo_spread, wo_share = zip(*[wo_copies(layer) for layer in range(layers)])

    def start_wo(layer):
        wo_r[layer][0].start()
        wo_l[layer][1].start()
        wo_r[layer][1].start()
        wo_l[layer][0].start()

    def forward_wo(layer):
        wo_r[layer][0].wait_recv()
        wo_fr[layer].start()
        wo_l[layer][1].wait_recv()
        wo_fl[layer].start()
        wo_r[layer][1].wait_recv()
        wo_l[layer][0].wait_recv()
        for copy in wo_spread[layer][0]:
            copy.start()

    def spread_far_wo(layer):
        wo_fr[layer].wait_recv()
        wo_fl[layer].wait_recv()
        for copy in wo_spread[layer][1]:
            copy.start()

    def share_wo_near(layer):
        for copy in wo_spread[layer][0]:
            copy.wait_recv()
        wo_share[layer][LT].start()
        wo_share[layer][RT].start()

    def share_wo_far(layer):
        for copy in wo_spread[layer][1]:
            copy.wait_recv()
        wo_share[layer][OP].start()

    small_sends = [remote(smalls, sm_all.at[me], lax.rem(me + k, n)) for k in range(1, n)]
    tok_src = lambda c: part(tokb, OWN, None, c)
    tok_dst = lambda slot, c: part(tokb, slot, None, c)
    tok_r, tok_l = block_sends(tok_src, tok_dst)
    def to_partner(ref):
        return lambda own, other: remote(ref(own), ref(other), partner)

    qkv_push = [[to_partner(lambda o, i=i: wqkvb.at[layer, :, pl.ds(i * chip_cols + o * share, share)])(0, 1)
                 for i in range(3)] for layer in range(layers)]
    in_push = [[to_partner(lambda o, i=i: winb.at[layer, i, pl.ds(o * ff_share, ff_share), :])(0, 1) for i in range(2)]
               for layer in range(layers)]
    out_push = [to_partner(lambda o: woutb.at[layer, pl.ds(o * ff_share, ff_share), :])(0, 1) for layer in range(layers)]
    wo_push = [to_partner(lambda o: wob.at[layer, OWN, pl.ds(o * share, share), :])(0, 1) for layer in range(layers)]

    for copy in small_sends:
        copy.start()
    for copy in wo_loads:
        copy.wait()
    start_wo(0)
    tok_load.wait()
    tok_r[0].start()
    tok_l[1].start()
    for load_copy, copy in zip(qkv_loads[0], qkv_push[0]):
        load_copy.wait()
        copy.start()
    wo_push[0].start()
    for load_copy, copy in zip(in_loads[0], in_push[0]):
        load_copy.wait()
        copy.start()
    out_loads[0].wait()
    out_push[0].start()

    sm_all[me] = smalls[...]
    for copy in small_sends:
        copy.wait_recv()
    for k in range(n):
        gainb[:, k * LANES:(k + 1) * LANES] = sm_all[k]
    for slot, device in ((OWN, me), (RT, right), (LT, left), (OP, opposite)):
        lenb[slot] = jnp.broadcast_to(sm_all[device, ROW_LEN:ROW_LEN + 1, :], (8, LANES))

    def norm_rows(load_row, gain_row, dst, start, count):
        step = 32

        def body(i, carry):
            r = pl.multiple_of(start + i * step, step)
            x = load_row(r, step)
            mean_sq = jnp.mean(x * x, axis=-1, keepdims=True)
            normed = x * lax.rsqrt(mean_sq + NORM_EPS) * gainb[gain_row:gain_row + 1, :]
            dst[pl.ds(r, step), :] = normed.astype(BF16)
            return carry

        lax.fori_loop(0, count // step, body, 0)

    def token_row(r, step):
        return tokb[pl.ds(r, step), :].astype(F32)

    def hidden_row(r, step):
        return hb[pl.ds(r, step), :]

    lane_low = lax.rem(lax.broadcasted_iota(jnp.int32, (1, chip_cols), 1), 2 * HEAD_DIM) < HEAD_DIM

    def project(layer, src, slot, count):
        x = src[rows(slot, count), :]
        q = dot(x, wqkvb[layer, :, 0:chip_cols])
        qb[rows(slot, count), :] = q.astype(BF16)
        for i, ref in ((1, kb), (2, vb)):
            y = dot(x, wqkvb[layer, :, i * chip_cols:(i + 1) * chip_cols])
            ref[0, rows(slot, count), :] = jnp.where(lane_low, y, 0.0).astype(BF16)
            ref[1, rows(slot, count), :] = jnp.where(lane_low, 0.0, y).astype(BF16)

    key_index = lax.broadcasted_iota(jnp.int32, (1, seq), 1).astype(F32)

    def attend(layer, slot, count):
        def body(i, carry):
            s = slot + i
            row = pl.ds(pl.multiple_of(s * seq, seq), seq)
            key_ok = key_index < lenb[s, 0:1, :]
            for pair in range(chip_cols // LANES):
                col = pl.ds(pair * LANES, LANES)
                keys = jnp.concatenate([kb[0, row, col], kb[1, row, col]], axis=0)
                scores = dot_rows(qb[row, col], keys)
                scores = scores + biasb[layer, pair]
                probs = []
                for h in range(2):
                    x = jnp.where(key_ok, scores[:, h * seq:(h + 1) * seq], MASKED)
                    e = jnp.exp(x - jnp.max(x, axis=-1, keepdims=True))
                    probs.append((e / jnp.sum(e, axis=-1, keepdims=True)).astype(BF16))
                values = jnp.concatenate([vb[0, row, col], vb[1, row, col]], axis=0)
                cb[0, row, col] = dot(jnp.concatenate(probs, axis=1), values).astype(BF16)
            return carry

        lax.fori_loop(0, count, body, 0)

    def build_bias():
        rel = lax.broadcasted_iota(jnp.int32, (LANES, 2 * seq), 1)
        rel = jnp.where(rel < seq, rel, rel - 2 * seq)
        lane = lax.broadcasted_iota(jnp.int32, (LANES, 2 * seq), 0)
        one_hot = jnp.where(bucket_of(rel) == lax.rem(lane, NUM_BUCKETS), 1.0, 0.0).astype(BF16)
        table_row = lax.broadcasted_iota(jnp.int32, (8, LANES), 0)
        table_lane = lax.broadcasted_iota(jnp.int32, (8, LANES), 1)
        own_lanes = table_row == table_lane // NUM_BUCKETS
        for pair, device in ((0, me), (1, partner)):
            tables = jnp.where(own_lanes, sm_all[device, ROW_BIAS:ROW_BIAS + 1, :], 0.0)
            lines = dot(tables.astype(BF16), one_hot)
            for layer in range(layers):
                for h in range(2):
                    row = 2 * layer + h
                    line = jnp.broadcast_to(lines[row:row + 1, :], (seq, 2 * seq))
                    shifted = pltpu.roll(line, 0, 1, stride=1, stride_axis=0)
                    biasb[layer, pair, :, h * seq:(h + 1) * seq] = shifted[:, 0:seq]

    norm_rows(token_row, ROW_ATTN, nb, OWN * seq, seq)
    build_bias()
    for copy in qkv_push[0]:
        copy.wait_recv()
    project(0, nb, OWN, 1)
    attend(0, OWN, 1)

    forward_wo(0)
    tok_r[1].start()
    tok_l[0].start()
    tok_fr, tok_fl = block_forwards(tok_dst)
    tok_r[0].wait_recv()
    tok_fr.start()
    tok_l[1].wait_recv()
    tok_fl.start()

    def c_part(src, slot, pair):
        return cb.at[src, rows(slot), pl.ds(pair * LANES, LANES)]

    c_r, c_l = {}, {}

    for slot in (OWN, RT, LT, OP):
        c_r[slot] = [remote(c_part(0, slot, p), c_part(LT, TO_RIGHT[slot], p), right) for p in range(2)]
        c_l[slot] = [remote(c_part(0, slot, p), c_part(RT, TO_LEFT[slot], p), left) for p in range(2)]

    def send_context(to_right, to_left):
        c_r[to_right][0].start()
        c_l[to_left][1].start()
        c_r[to_right][1].start()
        c_l[to_left][0].start()

    c_fr, c_fl = {}, {}

    def forward_context(slot):
        near, far = TO_RIGHT[slot], TO_RIGHT[TO_RIGHT[slot]]
        c_fr[slot] = remote(c_part(LT, near, 0), c_part(OP, far, 0), right)
        c_r[slot][0].wait_recv()
        c_fr[slot].start()
        near, far = TO_LEFT[slot], TO_LEFT[TO_LEFT[slot]]
        c_fl[slot] = remote(c_part(RT, near, 1), c_part(OP, far, 1), left)
        c_l[slot][1].wait_recv()
        c_fl[slot].start()

    send_context(OWN, OWN)

    spread_far_wo(0)
    tok_r[1].wait_recv()
    tok_l[0].wait_recv()
    norm_rows(token_row, ROW_ATTN, nb, RT * seq, 2 * seq)
    project(0, nb, RT, 2)
    attend(0, RT, 2)
    send_context(LT, RT)
    send_context(RT, LT)

    forward_context(OWN)
    tok_fr.wait_recv()
    tok_fl.wait_recv()
    norm_rows(token_row, ROW_ATTN, nb, OP * seq, seq)
    project(0, nb, OP, 1)
    attend(0, OP, 1)
    send_context(OP, OP)
    start_wo(1)

    def add_context(slot, count):
        for j in range(0, d_model, chip_cols):
            col = pl.ds(j, chip_cols)
            y = tokb[rows(slot, count), col].astype(F32)
            for src in (OWN, RT, LT, OP):
                y += dot(cb[src, rows(slot, count), :], wob[0, src, :, col])
            hb[rows(slot, count), col] = y

    forward_context(LT)
    forward_context(RT)
    share_wo_near(0)
    share_wo_far(0)
    wo_push[0].wait_recv()
    for copy in in_push[0]:
        copy.wait_recv()
    out_push[0].wait_recv()

    def feed_forward(layer, slot, count):
        x = mb[layer, rows(slot, count), :]
        gate = dot_rows(x, winb[layer, 0])
        lin = dot_rows(x, winb[layer, 1])
        mixed = (jax.nn.gelu(gate, approximate=True) * lin).astype(BF16)
        for j in range(0, d_model, chip_cols):
            col = pl.ds(j, chip_cols)
            pb[layer, rows(slot, count), col] = dot(mixed, woutb[layer, :, col])

    def scatter_copies(layer):
        p, ra, rb = pb.at[layer], relay_a.at[layer], relay_b.at[layer]
        rl, rr = recv_l.at[layer], recv_r.at[layer]
        row = lambda r: pl.ds(r * rows_half, rows_half)
        copies = {}
        for r in range(2):
            copies["op_r", r] = remote(part(p, OP, r, 0), ra.at[row(r), :], right)
            copies["op_l", r] = remote(part(p, OP, r, 1), rb.at[row(r), :], left)
            copies["plain_r", r] = remote(part(p, RT, r, 1), part(rl, 0, r, 1), right)
            copies["plain_l", r] = remote(part(p, LT, r, 0), part(rr, 0, r, 0), left)
            copies["sum_r", r] = remote(part(p, RT, r, 0), part(rl, 0, r, 0), right)
            copies["sum_l", r] = remote(part(p, LT, r, 1), part(rr, 0, r, 1), left)
        return copies

    def pass_on(layer, copies, r):
        a = pl.ds(RT * seq + r * rows_half, rows_half)
        b = pl.ds(LT * seq + r * rows_half, rows_half)
        row = pl.ds(r * rows_half, rows_half)
        copies["op_r", r].wait_recv()
        pb[layer, a, 0:half] += relay_a[layer, row, :]
        copies["sum_r", r].start()
        copies["op_l", r].wait_recv()
        pb[layer, b, half:d_model] += relay_b[layer, row, :]
        copies["sum_l", r].start()

    def collect(layer, copies, r):
        for name in ("plain_r", "plain_l", "sum_r", "sum_l"):
            copies[name, r].wait_recv()
        row = pl.ds(r * rows_half, rows_half)
        hb[row, :] = hb[row, :] + ((pb[layer, row, :] + recv_l[layer, row, :]) + recv_r[layer, row, :])

    rs = scatter_copies(0)
    c_r[LT][1].wait_recv()
    c_l[RT][0].wait_recv()
    c_fr[OWN].wait_recv()
    c_fl[OWN].wait_recv()
    for slot in (RT, LT, OP):
        wo_share[0][slot].wait_recv()
    add_context(OP, 1)
    norm_rows(hidden_row, ROW_FFN, mb.at[0], OP * seq, seq)
    feed_forward(0, OP, 1)
    forward_context(OP)
    for r in range(2):
        rs["op_r", r].start()
        rs["op_l", r].start()
    for slot in (OWN, OP):
        c_r[slot][1].wait_recv()
        c_l[slot][0].wait_recv()
    for slot in (RT, LT):
        c_fr[slot].wait_recv()
        c_fl[slot].wait_recv()
    add_context(RT, 2)
    norm_rows(hidden_row, ROW_FFN, mb.at[0], RT * seq, 2 * seq)
    feed_forward(0, RT, 2)
    rs["plain_r", 0].start()
    rs["plain_l", 0].start()
    forward_wo(1)
    c_r[RT][1].wait_recv()
    c_l[LT][0].wait_recv()
    c_fr[OP].wait_recv()
    c_fl[OP].wait_recv()
    add_context(OWN, 1)
    norm_rows(hidden_row, ROW_FFN, mb.at[0], OWN * seq, seq)
    feed_forward(0, OWN, 1)
    pass_on(0, rs, 0)
    rs["plain_r", 1].start()
    rs["plain_l", 1].start()
    pass_on(0, rs, 1)
    spread_far_wo(1)
    for load_copy, copy in zip(qkv_loads[1], qkv_push[1]):
        load_copy.wait()
        copy.start()
    wo_push[1].start()
    for load_copy, copy in zip(in_loads[1], in_push[1]):
        load_copy.wait()
        copy.start()
    out_loads[1].wait()
    out_push[1].start()

    def gather_copies(ref, r):
        to_right = [remote(part(ref, OWN, r, c), part(ref, LT, r, c), right) for c in range(2)]
        to_left = [remote(part(ref, OWN, r, c), part(ref, RT, r, c), left) for c in range(2)]
        fr = remote(part(ref, LT, r, 0), part(ref, OP, r, 0), right)
        fl = remote(part(ref, RT, r, 1), part(ref, OP, r, 1), left)
        return to_right, to_left, fr, fl

    n_gather = [gather_copies(mb.at[2], r) for r in range(2)]
    for r in range(2):
        collect(0, rs, r)
        norm_rows(hidden_row, 1, mb.at[2], r * rows_half, rows_half)
        to_right, to_left, _, _ = n_gather[r]
        to_right[0].start()
        to_left[1].start()
        to_right[1].start()
        to_left[0].start()

    def forward_gather(gather):
        to_right, to_left, fr, fl = gather
        to_right[0].wait_recv()
        fr.start()
        to_left[1].wait_recv()
        fl.start()

    forward_gather(n_gather[0])
    for copy in qkv_push[1]:
        copy.wait_recv()
    for copies in c_r, c_l:
        for slot in (OWN, RT, LT, OP):
            for copy in copies[slot]:
                copy.wait_send()
                done.add(id(copy))
    project(1, mb.at[2], OWN, 1)
    attend(1, OWN, 1)
    forward_gather(n_gather[1])
    share_wo_near(1)
    share_wo_far(1)
    for r in range(2):
        n_gather[r][0][1].wait_recv()
        n_gather[r][1][0].wait_recv()
    project(1, mb.at[2], RT, 2)
    attend(1, RT, 2)
    ctx_r = remote(cb.at[0, rows(RT), :], c1b.at[LT], right)
    ctx_l = remote(cb.at[0, rows(LT), :], c1b.at[RT], left)
    half_rows = lambda r: pl.ds(r * rows_half, rows_half)

    def far_context(r, p, device):
        col = pl.ds(p * LANES, LANES)
        out_copy = remote(cb.at[0, pl.ds(OP * seq + r * rows_half, rows_half), col], relay_c.at[p, half_rows(r), :], device)
        return out_copy, remote(relay_c.at[p, half_rows(r), :], c1b.at[OP, half_rows(r), col], device)

    ctx_o = [[far_context(r, p, device) for p, device in ((0, right), (1, left))] for r in range(2)]
    ctx_r.start()
    ctx_l.start()
    for r in range(2):
        n_gather[r][2].wait_recv()
        n_gather[r][3].wait_recv()
    project(1, mb.at[2], OP, 1)
    attend(1, OP, 1)
    for r in range(2):
        for copy, _ in ctx_o[r]:
            copy.start()
    for r in range(2):
        for copy, onward in ctx_o[r]:
            copy.wait_recv()
            onward.start()
    wo_push[1].wait_recv()

    def add_second(src, context, r=None):
        row = rows(OWN) if r is None else half_rows(r)
        for j in range(0, d_model, chip_cols):
            col = pl.ds(j, chip_cols)
            hb[row, col] += dot(context, wob[1, src, :, col])

    add_second(OWN, cb[0, rows(OWN), :])
    for slot, copy in ((LT, ctx_r), (RT, ctx_l)):
        wo_share[1][slot].wait_recv()
        copy.wait_recv()
        add_second(slot, c1b[slot])
    wo_share[1][OP].wait_recv()
    m_gather = [gather_copies(mb.at[1], r) for r in range(2)]
    for r in range(2):
        for _, onward in ctx_o[r]:
            onward.wait_recv()
        add_second(OP, c1b[OP, half_rows(r), :], r)
        norm_rows(hidden_row, ROW_FFN + 1, mb.at[1], r * rows_half, rows_half)
        to_right, to_left, _, _ = m_gather[r]
        to_right[0].start()
        to_left[1].start()
        to_right[1].start()
        to_left[0].start()
    for copy in in_push[1]:
        copy.wait_recv()
    out_push[1].wait_recv()
    rs = scatter_copies(1)
    feed_forward(1, OWN, 1)
    for r in range(2):
        forward_gather(m_gather[r])
    for r in range(2):
        m_gather[r][0][1].wait_recv()
        m_gather[r][1][0].wait_recv()
    feed_forward(1, RT, 2)
    rs["plain_r", 0].start()
    rs["plain_l", 0].start()
    for r in range(2):
        m_gather[r][2].wait_recv()
        m_gather[r][3].wait_recv()
    feed_forward(1, OP, 1)
    for r in range(2):
        rs["op_r", r].start()
        rs["op_l", r].start()
    rs["plain_r", 1].start()
    rs["plain_l", 1].start()
    for r in range(2):
        pass_on(1, rs, r)
    for r in range(2):
        collect(1, rs, r)
        norm_rows(hidden_row, ROW_FINAL, out, r * rows_half, rows_half)
    for copy in sent:
        if id(copy) not in done:
            copy.wait_send()


def encode(n, groups, lengths, attn_gain, ffn_gain, final_gain, bias_table, tokens, w_q, w_k, w_v, w_o, w_in0, w_in1, w_out):
    _, seq, d_model = tokens.shape
    layers, _, share = w_q.shape
    ff_share = w_out.shape[1]
    chip_cols = 2 * share
    ring = n // 2
    any_spec = pl.BlockSpec(memory_space=pl.ANY)
    vmem = pl.BlockSpec(memory_space=pltpu.VMEM)
    scratch = [
        pltpu.VMEM((SMALL_ROWS, LANES), F32),
        pltpu.VMEM((n, SMALL_ROWS, LANES), F32),
        pltpu.VMEM((8, d_model), F32),
        pltpu.VMEM((ring, 8, LANES), F32),
        pltpu.VMEM((layers, 2, seq, 2 * seq), F32),
        pltpu.VMEM((ring * seq, d_model), BF16),
        pltpu.VMEM((ring * seq, d_model), BF16),
        pltpu.VMEM((layers + 1, ring * seq, d_model), BF16),
        pltpu.VMEM((layers, d_model, 3 * chip_cols), BF16),
        pltpu.VMEM((layers, ring, chip_cols, d_model), BF16),
        pltpu.VMEM((layers, 2, 2 * ff_share, d_model), BF16),
        pltpu.VMEM((layers, 2 * ff_share, d_model), BF16),
        pltpu.VMEM((ring * seq, chip_cols), BF16),
        pltpu.VMEM((2, ring * seq, chip_cols), BF16),
        pltpu.VMEM((2, ring * seq, chip_cols), BF16),
        pltpu.VMEM((ring, ring * seq, chip_cols), BF16),
        pltpu.VMEM((ring, seq, chip_cols), BF16),
        pltpu.VMEM((2, seq, LANES), BF16),
        pltpu.VMEM((ring * seq, d_model), F32),
        pltpu.VMEM((layers, ring * seq, d_model), F32),
        pltpu.VMEM((layers, seq, d_model // 2), F32),
        pltpu.VMEM((layers, seq, d_model // 2), F32),
        pltpu.VMEM((layers, seq, d_model), F32),
        pltpu.VMEM((layers, seq, d_model), F32),
        pltpu.SemaphoreType.DMA((160 + 4 * groups,)),
        pltpu.SemaphoreType.DMA((160 + 4 * groups,)),
        pltpu.SemaphoreType.DMA((24,)),
    ]
    return pl.pallas_call(
        functools.partial(kernel, n, groups),
        out_shape=pltpu.VMEM((seq, d_model), BF16),
        in_specs=[pl.BlockSpec(memory_space=pltpu.SMEM)] + [vmem] * 4 + [any_spec] * 8,
        out_specs=vmem,
        scratch_shapes=scratch,
        compiler_params=pltpu.CompilerParams(
            collective_id=0, has_side_effects=True, vmem_limit_bytes=56 * 1024 * 1024),
    )(lengths, attn_gain, ffn_gain, final_gain, bias_table, tokens, w_q, w_k, w_v, w_o, w_in0, w_in1, w_out)


def solution(mesh):
    n, groups = mesh.shape["fsdp"], mesh.shape["dp"]
    batch_spec = P(("dp", "fsdp"))
    col_spec = P(None, None, "fsdp")
    row_spec = P(None, "fsdp", None)
    gain_spec = P(None, "fsdp")
    in_specs = (batch_spec, batch_spec, gain_spec, col_spec, col_spec, col_spec, row_spec, col_spec, gain_spec,
                col_spec, col_spec, row_spec, P("fsdp"))

    def local_forward(tokens, lengths, attn_gain, w_q, w_k, w_v, w_o, rel_bias, ffn_gain, w_in0, w_in1, w_out, final_gain):
        seq_len = tokens.shape[1]
        layers, buckets, heads = rel_bias.shape
        bias_table = jnp.swapaxes(rel_bias, 1, 2).reshape(layers * heads, buckets)
        normed_out = encode(n, groups, lengths, attn_gain, ffn_gain, final_gain[None], bias_table, tokens, w_q, w_k, w_v, w_o,
                            jnp.swapaxes(w_in0, 1, 2), jnp.swapaxes(w_in1, 1, 2), w_out)
        key_ok = jnp.arange(seq_len, dtype=jnp.int32)[:, None] < lengths
        return jnp.where(key_ok, normed_out, jnp.zeros_like(normed_out))[None]

    return jax.shard_map(local_forward, mesh=mesh, in_specs=in_specs, out_specs=batch_spec, check_vma=False)
```

```python
import functools

import jax
import jax.numpy as jnp
from jax import lax
from jax.experimental import pallas as pl
from jax.experimental.pallas import tpu as pltpu
from jax.sharding import PartitionSpec as P

HEAD_DIM = 64
NUM_BUCKETS = 32
NORM_EPS = 1e-6
LANES = 128
MASKED = -1e30
MESH = pl.DeviceIdType.MESH
BF16 = jnp.bfloat16
F32 = jnp.float32

ROW_ATTN, ROW_FFN, ROW_FINAL, ROW_BIAS, ROW_LEN, SMALL_ROWS = 0, 2, 4, 5, 6, 8

OWN, RT, LT, OP = 0, 1, 2, 3
TO_RIGHT = {OWN: LT, RT: OWN, LT: OP, OP: RT}
TO_LEFT = {OWN: RT, RT: OP, LT: OWN, OP: LT}


def bucket_of(rel_pos):
    half_buckets = NUM_BUCKETS // 2
    max_exact = half_buckets // 2
    distance = jnp.abs(rel_pos)
    log_bucket = jnp.full_like(distance, max_exact)
    for step in range(1, half_buckets - max_exact):
        log_bucket += jnp.where(distance * distance >= max_exact * max_exact * 2**step, 1, 0)
    return jnp.where(rel_pos > 0, half_buckets, 0) + jnp.where(distance < max_exact, distance, log_bucket)


def dot(a, b):
    return jnp.dot(a, b, preferred_element_type=F32)


def dot_rows(a, b):
    return lax.dot_general(a, b, (((1,), (1,)), ((), ())), preferred_element_type=F32)


def kernel(n, groups, lengths_in, attn_gain_in, ffn_gain_in, final_gain_in, bias_table_in,
           tok, wq, wk, wv, wo, win0, win1, wout, out,
           lengths, attn_gain, ffn_gain, final_gain, bias_table, smalls, sm_all, gainb, lenb, biasb, tokb, nb, mb, wqkvb, wob, winb, woutb, qb, kb, vb, cb, c1b, hb, pb,
           relay_a, relay_b, recv_l, recv_r, send_sem, recv_sem, load_sem):
    seq, d_model = tok.shape[1], tok.shape[2]
    layers = wq.shape[0]
    half, rows_half = d_model // 2, seq // 2
    share, ff_share = wq.shape[2], wout.shape[1]
    chip_cols = 2 * share

    me, group = lax.axis_index("fsdp"), lax.axis_index("dp")
    right, left = lax.rem(me + 2, n), lax.rem(me + n - 2, n)
    opposite = lax.rem(me + n // 2, n)
    partner = me + 1 - 2 * lax.rem(me, 2)
    counts = {"remote": 0, "local": 0}
    sent, done = [], set()

    def remote(src, dst, device, axis="fsdp"):
        index = counts["remote"]
        counts["remote"] += 1
        copy = pltpu.make_async_remote_copy(
            src_ref=src, dst_ref=dst, send_sem=send_sem.at[index], recv_sem=recv_sem.at[index],
            device_id={axis: device}, device_id_type=MESH)
        sent.append(copy)
        return copy

    def load(src, dst):
        index = counts["local"]
        counts["local"] += 1
        copy = pltpu.make_async_copy(src, dst, load_sem.at[index])
        copy.start()
        return copy

    def rows(slot, count=1):
        return pl.ds(slot * seq, count * seq)

    def part(ref, slot, r, c):
        row = pl.ds(slot * seq, seq) if r is None else pl.ds(slot * seq + r * rows_half, rows_half)
        col = slice(None) if c is None else pl.ds(c * half, half)
        return ref.at[row, col]

    barrier = pltpu.get_barrier_semaphore()
    for k in range(1, n):
        pl.semaphore_signal(barrier, inc=1, device_id={"fsdp": lax.rem(me + k, n)}, device_id_type=MESH)
    for k in range(1, groups):
        pl.semaphore_signal(barrier, inc=1, device_id={"dp": lax.rem(group + k, groups)}, device_id_type=MESH)

    small_loads = [load(src, dst) for src, dst in zip(
        (lengths_in, attn_gain_in, ffn_gain_in, final_gain_in, bias_table_in),
        (lengths, attn_gain, ffn_gain, final_gain, bias_table))]
    tok_load = load(tok.at[0], tokb.at[rows(OWN), :])
    wo_loads = [load(wo.at[layer], wob.at[layer, OWN, pl.ds(0, share), :]) for layer in range(layers)]
    qkv_loads = []
    for layer in range(layers):
        qkv_loads.append([load(w.at[layer], wqkvb.at[layer, :, pl.ds(i * chip_cols, share)])
                          for i, w in enumerate((wq, wk, wv))])
        if layer == 0:
            in_loads = []
            out_loads = []
        in_loads.append([load(w.at[layer], winb.at[layer, i, pl.ds(0, ff_share), :]) for i, w in enumerate((win0, win1))])
        out_loads.append(load(wout.at[layer], woutb.at[layer, pl.ds(0, ff_share), :]))

    for copy in small_loads:
        copy.wait()
    smalls[ROW_ATTN:ROW_ATTN + layers, :] = attn_gain[...].astype(F32)
    smalls[ROW_FFN:ROW_FFN + layers, :] = ffn_gain[...].astype(F32)
    smalls[ROW_FINAL:ROW_FINAL + 1, :] = final_gain[...].astype(F32)
    table = bias_table[...].astype(F32)
    smalls[ROW_BIAS:ROW_BIAS + 1, :] = jnp.concatenate([table[i:i + 1] for i in range(table.shape[0])], axis=1)
    smalls[ROW_LEN:SMALL_ROWS, :] = jnp.broadcast_to(lengths[...].astype(F32), (SMALL_ROWS - ROW_LEN, LANES))

    pl.semaphore_wait(barrier, n - 1 + groups - 1)

    def block_sends(src, dst):
        to_right = [remote(src(c), dst(LT, c), right) for c in range(2)]
        to_left = [remote(src(c), dst(RT, c), left) for c in range(2)]
        return to_right, to_left

    def block_forwards(dst):
        return remote(dst(LT, 0), dst(OP, 0), right), remote(dst(RT, 1), dst(OP, 1), left)

    row_pieces = min(groups, share // 16)
    col_pieces = groups // row_pieces
    piece_rows, piece_cols = share // row_pieces, d_model // col_pieces
    piece_row = pl.multiple_of(group // col_pieces * piece_rows, piece_rows)
    piece_col = pl.multiple_of(lax.rem(group, col_pieces) * piece_cols, piece_cols)

    def wo_copies(layer):
        col = lambda c: pl.ds(pl.multiple_of(piece_col + c * (piece_cols // 2), LANES), piece_cols // 2)
        src = lambda c: wob.at[layer, OWN, pl.ds(piece_row, piece_rows), col(c)]
        dst = lambda slot, c: wob.at[layer, slot, pl.ds(piece_row, piece_rows), col(c)]
        to_right, to_left = block_sends(src, dst)
        fr, fl = block_forwards(dst)
        piece = lambda slot, count: wob.at[layer, pl.ds(slot, count), pl.ds(piece_row, piece_rows), pl.ds(piece_col, piece_cols)]
        spread = [[remote(piece(slot, count), piece(slot, count), lax.rem(group + k, groups), "dp") for k in range(1, groups)]
                  for slot, count in ((RT, 2), (OP, 1))]
        push = {s: remote(wob.at[layer, s, pl.ds(0, share), :], wob.at[layer, s, pl.ds(share, share), :], partner)
                for s in (RT, LT, OP)}
        return to_right, to_left, fr, fl, spread, push

    wo_r, wo_l, wo_fr, wo_fl, wo_spread, wo_share = zip(*[wo_copies(layer) for layer in range(layers)])

    def start_wo(layer):
        wo_r[layer][0].start()
        wo_l[layer][1].start()
        wo_r[layer][1].start()
        wo_l[layer][0].start()

    def forward_wo(layer):
        wo_r[layer][0].wait_recv()
        wo_fr[layer].start()
        wo_l[layer][1].wait_recv()
        wo_fl[layer].start()
        wo_r[layer][1].wait_recv()
        wo_l[layer][0].wait_recv()
        for copy in wo_spread[layer][0]:
            copy.start()

    def spread_far_wo(layer):
        wo_fr[layer].wait_recv()
        wo_fl[layer].wait_recv()
        for copy in wo_spread[layer][1]:
            copy.start()

    def share_wo_near(layer):
        for copy in wo_spread[layer][0]:
            copy.wait_recv()
        wo_share[layer][LT].start()
        wo_share[layer][RT].start()

    def share_wo_far(layer):
        for copy in wo_spread[layer][1]:
            copy.wait_recv()
        wo_share[layer][OP].start()

    small_sends = [remote(smalls, sm_all.at[me], lax.rem(me + k, n)) for k in range(1, n)]
    tok_src = lambda c: part(tokb, OWN, None, c)
    tok_dst = lambda slot, c: part(tokb, slot, None, c)
    tok_r, tok_l = block_sends(tok_src, tok_dst)
    def to_partner(ref):
        return lambda own, other: remote(ref(own), ref(other), partner)

    qkv_push = [[to_partner(lambda o, i=i: wqkvb.at[layer, :, pl.ds(i * chip_cols + o * share, share)])(0, 1)
                 for i in range(3)] for layer in range(layers)]
    in_push = [[to_partner(lambda o, i=i: winb.at[layer, i, pl.ds(o * ff_share, ff_share), :])(0, 1) for i in range(2)]
               for layer in range(layers)]
    out_push = [to_partner(lambda o: woutb.at[layer, pl.ds(o * ff_share, ff_share), :])(0, 1) for layer in range(layers)]
    wo_push = [to_partner(lambda o: wob.at[layer, OWN, pl.ds(o * share, share), :])(0, 1) for layer in range(layers)]

    for copy in small_sends:
        copy.start()
    for copy in wo_loads:
        copy.wait()
    start_wo(0)
    tok_load.wait()
    tok_r[0].start()
    tok_l[1].start()
    for load_copy, copy in zip(qkv_loads[0], qkv_push[0]):
        load_copy.wait()
        copy.start()
    wo_push[0].start()
    for load_copy, copy in zip(in_loads[0], in_push[0]):
        load_copy.wait()
        copy.start()
    out_loads[0].wait()
    out_push[0].start()

    sm_all[me] = smalls[...]
    for copy in small_sends:
        copy.wait_recv()
    for k in range(n):
        gainb[:, k * LANES:(k + 1) * LANES] = sm_all[k]
    for slot, device in ((OWN, me), (RT, right), (LT, left), (OP, opposite)):
        lenb[slot] = jnp.broadcast_to(sm_all[device, ROW_LEN:ROW_LEN + 1, :], (8, LANES))

    def norm_rows(load_row, gain_row, dst, start, count, masked=False):
        step = 32

        def body(i, carry):
            r = pl.multiple_of(start + i * step, step)
            x = load_row(r, step)
            mean_sq = jnp.mean(x * x, axis=-1, keepdims=True)
            normed = x * lax.rsqrt(mean_sq + NORM_EPS) * gainb[gain_row:gain_row + 1, :]
            if masked:
                position = (r + lax.broadcasted_iota(jnp.int32, (step, d_model), 0)).astype(F32)
                normed = jnp.where(position < lenb[OWN, 0:1, 0:1], normed, 0.0)
            dst[pl.ds(r, step), :] = normed.astype(BF16)
            return carry

        lax.fori_loop(0, count // step, body, 0)

    def token_row(r, step):
        return tokb[pl.ds(r, step), :].astype(F32)

    def hidden_row(r, step):
        return hb[pl.ds(r, step), :]

    lane_low = lax.rem(lax.broadcasted_iota(jnp.int32, (1, chip_cols), 1), 2 * HEAD_DIM) < HEAD_DIM

    def project(layer, src, slot, count):
        x = src[rows(slot, count), :]
        q = dot(x, wqkvb[layer, :, 0:chip_cols])
        qb[rows(slot, count), :] = q.astype(BF16)
        for i, ref in ((1, kb), (2, vb)):
            y = dot(x, wqkvb[layer, :, i * chip_cols:(i + 1) * chip_cols])
            ref[0, rows(slot, count), :] = jnp.where(lane_low, y, 0.0).astype(BF16)
            ref[1, rows(slot, count), :] = jnp.where(lane_low, 0.0, y).astype(BF16)

    key_index = lax.broadcasted_iota(jnp.int32, (1, seq), 1).astype(F32)

    def attend(layer, slot, count):
        def body(i, carry):
            s = slot + i
            row = pl.ds(pl.multiple_of(s * seq, seq), seq)
            key_ok = key_index < lenb[s, 0:1, :]
            for pair in range(chip_cols // LANES):
                col = pl.ds(pair * LANES, LANES)
                keys = jnp.concatenate([kb[0, row, col], kb[1, row, col]], axis=0)
                scores = dot_rows(qb[row, col], keys)
                scores = scores + biasb[layer, pair]
                probs = []
                for h in range(2):
                    x = jnp.where(key_ok, scores[:, h * seq:(h + 1) * seq], MASKED)
                    e = jnp.exp(x - jnp.max(x, axis=-1, keepdims=True))
                    probs.append((e / jnp.sum(e, axis=-1, keepdims=True)).astype(BF16))
                values = jnp.concatenate([vb[0, row, col], vb[1, row, col]], axis=0)
                cb[0, row, col] = dot(jnp.concatenate(probs, axis=1), values).astype(BF16)
            return carry

        lax.fori_loop(0, count, body, 0)

    def build_bias():
        rel = lax.broadcasted_iota(jnp.int32, (LANES, 2 * seq), 1)
        rel = jnp.where(rel < seq, rel, rel - 2 * seq)
        lane = lax.broadcasted_iota(jnp.int32, (LANES, 2 * seq), 0)
        one_hot = jnp.where(bucket_of(rel) == lax.rem(lane, NUM_BUCKETS), 1.0, 0.0).astype(BF16)
        table_row = lax.broadcasted_iota(jnp.int32, (8, LANES), 0)
        table_lane = lax.broadcasted_iota(jnp.int32, (8, LANES), 1)
        own_lanes = table_row == table_lane // NUM_BUCKETS
        for pair, device in ((0, me), (1, partner)):
            tables = jnp.where(own_lanes, sm_all[device, ROW_BIAS:ROW_BIAS + 1, :], 0.0)
            lines = dot(tables.astype(BF16), one_hot)
            for layer in range(layers):
                for h in range(2):
                    row = 2 * layer + h
                    line = jnp.broadcast_to(lines[row:row + 1, :], (seq, 2 * seq))
                    shifted = pltpu.roll(line, 0, 1, stride=1, stride_axis=0)
                    biasb[layer, pair, :, h * seq:(h + 1) * seq] = shifted[:, 0:seq]

    norm_rows(token_row, ROW_ATTN, nb, OWN * seq, seq)
    build_bias()
    for copy in qkv_push[0]:
        copy.wait_recv()
    project(0, nb, OWN, 1)
    attend(0, OWN, 1)

    forward_wo(0)
    tok_r[1].start()
    tok_l[0].start()
    tok_fr, tok_fl = block_forwards(tok_dst)
    tok_r[0].wait_recv()
    tok_fr.start()
    tok_l[1].wait_recv()
    tok_fl.start()

    def c_part(src, slot, pair):
        return cb.at[src, rows(slot), pl.ds(pair * LANES, LANES)]

    c_r, c_l = {}, {}

    for slot in (OWN, RT, LT, OP):
        c_r[slot] = [remote(c_part(0, slot, p), c_part(LT, TO_RIGHT[slot], p), right) for p in range(2)]
        c_l[slot] = [remote(c_part(0, slot, p), c_part(RT, TO_LEFT[slot], p), left) for p in range(2)]

    def send_context(to_right, to_left):
        c_r[to_right][0].start()
        c_l[to_left][1].start()
        c_r[to_right][1].start()
        c_l[to_left][0].start()

    c_fr, c_fl = {}, {}

    def forward_context(slot):
        near, far = TO_RIGHT[slot], TO_RIGHT[TO_RIGHT[slot]]
        c_fr[slot] = remote(c_part(LT, near, 0), c_part(OP, far, 0), right)
        c_r[slot][0].wait_recv()
        c_fr[slot].start()
        near, far = TO_LEFT[slot], TO_LEFT[TO_LEFT[slot]]
        c_fl[slot] = remote(c_part(RT, near, 1), c_part(OP, far, 1), left)
        c_l[slot][1].wait_recv()
        c_fl[slot].start()

    send_context(OWN, OWN)

    spread_far_wo(0)
    tok_r[1].wait_recv()
    tok_l[0].wait_recv()
    norm_rows(token_row, ROW_ATTN, nb, RT * seq, 2 * seq)
    project(0, nb, RT, 2)
    attend(0, RT, 2)
    send_context(LT, RT)
    send_context(RT, LT)

    forward_context(OWN)
    tok_fr.wait_recv()
    tok_fl.wait_recv()
    norm_rows(token_row, ROW_ATTN, nb, OP * seq, seq)
    project(0, nb, OP, 1)
    attend(0, OP, 1)
    send_context(OP, OP)
    start_wo(1)

    def add_context(slot, count):
        for j in range(0, d_model, chip_cols):
            col = pl.ds(j, chip_cols)
            y = tokb[rows(slot, count), col].astype(F32)
            for src in (OWN, RT, LT, OP):
                y += dot(cb[src, rows(slot, count), :], wob[0, src, :, col])
            hb[rows(slot, count), col] = y

    forward_context(LT)
    forward_context(RT)
    share_wo_near(0)
    share_wo_far(0)
    wo_push[0].wait_recv()
    for copy in in_push[0]:
        copy.wait_recv()
    out_push[0].wait_recv()

    def feed_forward(layer, slot, count):
        x = mb[layer, rows(slot, count), :]
        gate = dot_rows(x, winb[layer, 0])
        lin = dot_rows(x, winb[layer, 1])
        mixed = (jax.nn.gelu(gate, approximate=True) * lin).astype(BF16)
        for j in range(0, d_model, chip_cols):
            col = pl.ds(j, chip_cols)
            pb[layer, rows(slot, count), col] = dot(mixed, woutb[layer, :, col])

    def scatter_copies(layer):
        p, ra, rb = pb.at[layer], relay_a.at[layer], relay_b.at[layer]
        rl, rr = recv_l.at[layer], recv_r.at[layer]
        row = lambda r: pl.ds(r * rows_half, rows_half)
        copies = {}
        for r in range(2):
            copies["op_r", r] = remote(part(p, OP, r, 0), ra.at[row(r), :], right)
            copies["op_l", r] = remote(part(p, OP, r, 1), rb.at[row(r), :], left)
            copies["plain_r", r] = remote(part(p, RT, r, 1), part(rl, 0, r, 1), right)
            copies["plain_l", r] = remote(part(p, LT, r, 0), part(rr, 0, r, 0), left)
            copies["sum_r", r] = remote(part(p, RT, r, 0), part(rl, 0, r, 0), right)
            copies["sum_l", r] = remote(part(p, LT, r, 1), part(rr, 0, r, 1), left)
        return copies

    def pass_on(layer, copies, r):
        a = pl.ds(RT * seq + r * rows_half, rows_half)
        b = pl.ds(LT * seq + r * rows_half, rows_half)
        row = pl.ds(r * rows_half, rows_half)
        copies["op_r", r].wait_recv()
        pb[layer, a, 0:half] += relay_a[layer, row, :]
        copies["sum_r", r].start()
        copies["op_l", r].wait_recv()
        pb[layer, b, half:d_model] += relay_b[layer, row, :]
        copies["sum_l", r].start()

    def collect(layer, copies, r):
        for name in ("plain_r", "plain_l", "sum_r", "sum_l"):
            copies[name, r].wait_recv()
        row = pl.ds(r * rows_half, rows_half)
        hb[row, :] = hb[row, :] + ((pb[layer, row, :] + recv_l[layer, row, :]) + recv_r[layer, row, :])

    rs = scatter_copies(0)
    c_r[LT][1].wait_recv()
    c_l[RT][0].wait_recv()
    c_fr[OWN].wait_recv()
    c_fl[OWN].wait_recv()
    for slot in (RT, LT, OP):
        wo_share[0][slot].wait_recv()
    add_context(OP, 1)
    norm_rows(hidden_row, ROW_FFN, mb.at[0], OP * seq, seq)
    feed_forward(0, OP, 1)
    forward_context(OP)
    for r in range(2):
        rs["op_r", r].start()
        rs["op_l", r].start()
    for slot in (OWN, OP):
        c_r[slot][1].wait_recv()
        c_l[slot][0].wait_recv()
    for slot in (RT, LT):
        c_fr[slot].wait_recv()
        c_fl[slot].wait_recv()
    add_context(RT, 2)
    norm_rows(hidden_row, ROW_FFN, mb.at[0], RT * seq, 2 * seq)
    feed_forward(0, RT, 2)
    rs["plain_r", 0].start()
    rs["plain_l", 0].start()
    forward_wo(1)
    c_r[RT][1].wait_recv()
    c_l[LT][0].wait_recv()
    c_fr[OP].wait_recv()
    c_fl[OP].wait_recv()
    add_context(OWN, 1)
    norm_rows(hidden_row, ROW_FFN, mb.at[0], OWN * seq, seq)
    feed_forward(0, OWN, 1)
    pass_on(0, rs, 0)
    rs["plain_r", 1].start()
    rs["plain_l", 1].start()
    pass_on(0, rs, 1)
    spread_far_wo(1)
    for load_copy, copy in zip(qkv_loads[1], qkv_push[1]):
        load_copy.wait()
        copy.start()
    wo_push[1].start()
    for load_copy, copy in zip(in_loads[1], in_push[1]):
        load_copy.wait()
        copy.start()
    out_loads[1].wait()
    out_push[1].start()

    def gather_copies(ref, r):
        to_right = [remote(part(ref, OWN, r, c), part(ref, LT, r, c), right) for c in range(2)]
        to_left = [remote(part(ref, OWN, r, c), part(ref, RT, r, c), left) for c in range(2)]
        fr = remote(part(ref, LT, r, 0), part(ref, OP, r, 0), right)
        fl = remote(part(ref, RT, r, 1), part(ref, OP, r, 1), left)
        return to_right, to_left, fr, fl

    n_gather = [gather_copies(mb.at[2], r) for r in range(2)]
    for r in range(2):
        collect(0, rs, r)
        norm_rows(hidden_row, 1, mb.at[2], r * rows_half, rows_half)
        to_right, to_left, _, _ = n_gather[r]
        to_right[0].start()
        to_left[1].start()
        to_right[1].start()
        to_left[0].start()

    def forward_gather(gather):
        to_right, to_left, fr, fl = gather
        to_right[0].wait_recv()
        fr.start()
        to_left[1].wait_recv()
        fl.start()

    forward_gather(n_gather[0])
    for copy in qkv_push[1]:
        copy.wait_recv()
    for copies in c_r, c_l:
        for slot in (OWN, RT, LT, OP):
            for copy in copies[slot]:
                copy.wait_send()
                done.add(id(copy))
    project(1, mb.at[2], OWN, 1)
    attend(1, OWN, 1)
    forward_gather(n_gather[1])
    share_wo_near(1)
    share_wo_far(1)
    for r in range(2):
        n_gather[r][0][1].wait_recv()
        n_gather[r][1][0].wait_recv()
    project(1, mb.at[2], RT, 2)
    attend(1, RT, 2)
    ctx_r = remote(cb.at[0, rows(RT), :], c1b.at[LT], right)
    ctx_l = remote(cb.at[0, rows(LT), :], c1b.at[RT], left)
    half_rows = lambda r: pl.ds(r * rows_half, rows_half)

    ctx_o = [remote(cb.at[0, pl.ds(OP * seq + r * rows_half, rows_half), :], c1b.at[OP, half_rows(r), :], opposite)
             for r in range(2)]
    ctx_r.start()
    ctx_l.start()
    for r in range(2):
        n_gather[r][2].wait_recv()
        n_gather[r][3].wait_recv()
    project(1, mb.at[2], OP, 1)
    attend(1, OP, 1)
    for copy in ctx_o:
        copy.start()
    wo_push[1].wait_recv()

    def add_second(src, context, r=None):
        row = rows(OWN) if r is None else half_rows(r)
        for j in range(0, d_model, chip_cols):
            col = pl.ds(j, chip_cols)
            hb[row, col] += dot(context, wob[1, src, :, col])

    add_second(OWN, cb[0, rows(OWN), :])
    for slot, copy in ((LT, ctx_r), (RT, ctx_l)):
        wo_share[1][slot].wait_recv()
        copy.wait_recv()
        add_second(slot, c1b[slot])
    wo_share[1][OP].wait_recv()
    m_gather = [gather_copies(mb.at[1], r) for r in range(2)]
    for r in range(2):
        ctx_o[r].wait_recv()
        add_second(OP, c1b[OP, half_rows(r), :], r)
        norm_rows(hidden_row, ROW_FFN + 1, mb.at[1], r * rows_half, rows_half)
        to_right, to_left, _, _ = m_gather[r]
        to_right[0].start()
        to_left[1].start()
        to_right[1].start()
        to_left[0].start()
    for copy in in_push[1]:
        copy.wait_recv()
    out_push[1].wait_recv()
    rs = scatter_copies(1)
    feed_forward(1, OWN, 1)
    for r in range(2):
        forward_gather(m_gather[r])
    for r in range(2):
        m_gather[r][0][1].wait_recv()
        m_gather[r][1][0].wait_recv()
    feed_forward(1, RT, 2)
    rs["plain_r", 0].start()
    rs["plain_l", 0].start()
    for r in range(2):
        m_gather[r][2].wait_recv()
        m_gather[r][3].wait_recv()
    feed_forward(1, OP, 1)
    for r in range(2):
        rs["op_r", r].start()
        rs["op_l", r].start()
    rs["plain_r", 1].start()
    rs["plain_l", 1].start()
    for r in range(2):
        pass_on(1, rs, r)
    for r in range(2):
        collect(1, rs, r)
        norm_rows(hidden_row, ROW_FINAL, out, r * rows_half, rows_half, masked=True)
    for copy in sent:
        if id(copy) not in done:
            copy.wait_send()


def encode(n, groups, lengths, attn_gain, ffn_gain, final_gain, bias_table, tokens, w_q, w_k, w_v, w_o, w_in0, w_in1, w_out):
    _, seq, d_model = tokens.shape
    layers, _, share = w_q.shape
    ff_share = w_out.shape[1]
    chip_cols = 2 * share
    ring = n // 2
    vmem = pl.BlockSpec(memory_space=pltpu.VMEM)
    scratch = [
        pltpu.VMEM(lengths.shape, jnp.int32),
        pltpu.VMEM(attn_gain.shape, BF16),
        pltpu.VMEM(ffn_gain.shape, BF16),
        pltpu.VMEM(final_gain.shape, BF16),
        pltpu.VMEM(bias_table.shape, BF16),
        pltpu.VMEM((SMALL_ROWS, LANES), F32),
        pltpu.VMEM((n, SMALL_ROWS, LANES), F32),
        pltpu.VMEM((8, d_model), F32),
        pltpu.VMEM((ring, 8, LANES), F32),
        pltpu.VMEM((layers, 2, seq, 2 * seq), F32),
        pltpu.VMEM((ring * seq, d_model), BF16),
        pltpu.VMEM((ring * seq, d_model), BF16),
        pltpu.VMEM((layers + 1, ring * seq, d_model), BF16),
        pltpu.VMEM((layers, d_model, 3 * chip_cols), BF16),
        pltpu.VMEM((layers, ring, chip_cols, d_model), BF16),
        pltpu.VMEM((layers, 2, 2 * ff_share, d_model), BF16),
        pltpu.VMEM((layers, 2 * ff_share, d_model), BF16),
        pltpu.VMEM((ring * seq, chip_cols), BF16),
        pltpu.VMEM((2, ring * seq, chip_cols), BF16),
        pltpu.VMEM((2, ring * seq, chip_cols), BF16),
        pltpu.VMEM((ring, ring * seq, chip_cols), BF16),
        pltpu.VMEM((ring, seq, chip_cols), BF16),
        pltpu.VMEM((ring * seq, d_model), F32),
        pltpu.VMEM((layers, ring * seq, d_model), F32),
        pltpu.VMEM((layers, seq, d_model // 2), F32),
        pltpu.VMEM((layers, seq, d_model // 2), F32),
        pltpu.VMEM((layers, seq, d_model), F32),
        pltpu.VMEM((layers, seq, d_model), F32),
        pltpu.SemaphoreType.DMA((160 + 4 * groups,)),
        pltpu.SemaphoreType.DMA((160 + 4 * groups,)),
        pltpu.SemaphoreType.DMA((32,)),
    ]
    return pl.pallas_call(
        functools.partial(kernel, n, groups),
        out_shape=pltpu.VMEM((seq, d_model), BF16),
        in_specs=[pl.BlockSpec(memory_space=pltpu.HBM)] * 13,
        out_specs=vmem,
        scratch_shapes=scratch,
        compiler_params=pltpu.CompilerParams(
            collective_id=0, has_side_effects=True, vmem_limit_bytes=56 * 1024 * 1024),
    )(lengths, attn_gain, ffn_gain, final_gain, bias_table, tokens, w_q, w_k, w_v, w_o, w_in0, w_in1, w_out)


def solution(mesh):
    n, groups = mesh.shape["fsdp"], mesh.shape["dp"]
    batch_spec = P(("dp", "fsdp"))
    col_spec = P(None, None, "fsdp")
    row_spec = P(None, "fsdp", None)
    gain_spec = P(None, "fsdp")
    in_specs = (batch_spec, batch_spec, gain_spec, col_spec, col_spec, col_spec, row_spec, col_spec, gain_spec,
                col_spec, col_spec, row_spec, P("fsdp"))

    def local_forward(tokens, lengths, attn_gain, w_q, w_k, w_v, w_o, rel_bias, ffn_gain, w_in0, w_in1, w_out, final_gain):
        layers, buckets, heads = rel_bias.shape
        bias_table = jnp.swapaxes(rel_bias, 1, 2).reshape(layers * heads, buckets)
        encoded = encode(n, groups, lengths[None], attn_gain, ffn_gain, final_gain[None], bias_table, tokens, w_q, w_k, w_v, w_o,
                            jnp.swapaxes(w_in0, 1, 2), jnp.swapaxes(w_in1, 1, 2), w_out)
        return encoded[None]

    return jax.shard_map(local_forward, mesh=mesh, in_specs=in_specs, out_specs=batch_spec, check_vma=False)
```

```python
import functools

import jax
import jax.numpy as jnp
from jax import lax
from jax.experimental import pallas as pl
from jax.experimental.pallas import tpu as pltpu
from jax.sharding import PartitionSpec as P

HEAD_DIM = 64
NUM_BUCKETS = 32
NORM_EPS = 1e-6
LANES = 128
MASKED = -1e30
MESH = pl.DeviceIdType.MESH
BF16 = jnp.bfloat16
F32 = jnp.float32

ROW_ATTN, ROW_FFN, ROW_FINAL, ROW_BIAS, ROW_LEN, SMALL_ROWS = 0, 2, 4, 5, 6, 8

OWN, RT, LT, OP = 0, 1, 2, 3
TO_RIGHT = {OWN: LT, RT: OWN, LT: OP, OP: RT}
TO_LEFT = {OWN: RT, RT: OP, LT: OWN, OP: LT}


def bucket_of(rel_pos):
    half_buckets = NUM_BUCKETS // 2
    max_exact = half_buckets // 2
    distance = jnp.abs(rel_pos)
    log_bucket = jnp.full_like(distance, max_exact)
    for step in range(1, half_buckets - max_exact):
        log_bucket += jnp.where(distance * distance >= max_exact * max_exact * 2**step, 1, 0)
    return jnp.where(rel_pos > 0, half_buckets, 0) + jnp.where(distance < max_exact, distance, log_bucket)


def dot(a, b):
    return jnp.dot(a, b, preferred_element_type=F32)


def dot_rows(a, b):
    return lax.dot_general(a, b, (((1,), (1,)), ((), ())), preferred_element_type=F32)


def kernel(n, groups, lengths_in, attn_gain_in, ffn_gain_in, final_gain_in, bias_table_in,
           tok, wq, wk, wv, wo, win0, win1, wout, out,
           lengths, attn_gain, ffn_gain, final_gain, bias_table, smalls, sm_all, gainb, lenb, biasb, tokb, nb, mb, wqkvb, wob, winb, woutb, qb, kb, vb, cb, c1b, hb, pb,
           relay_a, relay_b, recv_l, recv_r, send_sem, recv_sem, load_sem):
    seq, d_model = tok.shape[1], tok.shape[2]
    layers = wq.shape[0]
    half, rows_half = d_model // 2, seq // 2
    share, ff_share = wq.shape[2], wout.shape[1]
    chip_cols = 2 * share

    me, group = lax.axis_index("fsdp"), lax.axis_index("dp")
    right, left = lax.rem(me + 2, n), lax.rem(me + n - 2, n)
    opposite = lax.rem(me + n // 2, n)
    partner = me + 1 - 2 * lax.rem(me, 2)
    counts = {"remote": 0, "local": 0}
    sent, done = [], set()

    def remote(src, dst, device, axis="fsdp"):
        index = counts["remote"]
        counts["remote"] += 1
        copy = pltpu.make_async_remote_copy(
            src_ref=src, dst_ref=dst, send_sem=send_sem.at[index], recv_sem=recv_sem.at[index],
            device_id={axis: device}, device_id_type=MESH)
        sent.append(copy)
        return copy

    def load(src, dst):
        index = counts["local"]
        counts["local"] += 1
        copy = pltpu.make_async_copy(src, dst, load_sem.at[index])
        copy.start()
        return copy

    def rows(slot, count=1):
        return pl.ds(slot * seq, count * seq)

    def part(ref, slot, r, c):
        row = pl.ds(slot * seq, seq) if r is None else pl.ds(slot * seq + r * rows_half, rows_half)
        col = slice(None) if c is None else pl.ds(c * half, half)
        return ref.at[row, col]

    barrier = pltpu.get_barrier_semaphore()
    for k in range(1, n):
        pl.semaphore_signal(barrier, inc=1, device_id={"fsdp": lax.rem(me + k, n)}, device_id_type=MESH)
    for k in range(1, groups):
        pl.semaphore_signal(barrier, inc=1, device_id={"dp": lax.rem(group + k, groups)}, device_id_type=MESH)

    small_loads = [load(src, dst) for src, dst in zip(
        (lengths_in, attn_gain_in, ffn_gain_in, final_gain_in, bias_table_in),
        (lengths, attn_gain, ffn_gain, final_gain, bias_table))]
    tok_load = load(tok.at[0], tokb.at[rows(OWN), :])
    wo_loads = [load(wo.at[layer], wob.at[layer, OWN, pl.ds(0, share), :]) for layer in range(layers)]
    qkv_loads = []
    for layer in range(layers):
        qkv_loads.append([load(w.at[layer], wqkvb.at[layer, :, pl.ds(i * chip_cols, share)])
                          for i, w in enumerate((wq, wk, wv))])
        if layer == 0:
            in_loads = []
            out_loads = []
        in_loads.append([load(w.at[layer], winb.at[layer, i, pl.ds(0, ff_share), :]) for i, w in enumerate((win0, win1))])
        out_loads.append(load(wout.at[layer], woutb.at[layer, pl.ds(0, ff_share), :]))

    for copy in small_loads:
        copy.wait()
    smalls[ROW_ATTN:ROW_ATTN + layers, :] = attn_gain[...].astype(F32)
    smalls[ROW_FFN:ROW_FFN + layers, :] = ffn_gain[...].astype(F32)
    smalls[ROW_FINAL:ROW_FINAL + 1, :] = final_gain[...].astype(F32)
    table = bias_table[...].astype(F32)
    smalls[ROW_BIAS:ROW_BIAS + 1, :] = jnp.concatenate([table[i:i + 1] for i in range(table.shape[0])], axis=1)
    smalls[ROW_LEN:SMALL_ROWS, :] = jnp.broadcast_to(lengths[...].astype(F32), (SMALL_ROWS - ROW_LEN, LANES))

    pl.semaphore_wait(barrier, n - 1 + groups - 1)

    def block_sends(src, dst):
        to_right = [remote(src(c), dst(LT, c), right) for c in range(2)]
        to_left = [remote(src(c), dst(RT, c), left) for c in range(2)]
        return to_right, to_left

    def block_forwards(dst):
        return remote(dst(LT, 0), dst(OP, 0), right), remote(dst(RT, 1), dst(OP, 1), left)

    row_pieces = min(groups, share // 16)
    col_pieces = groups // row_pieces
    piece_rows, piece_cols = share // row_pieces, d_model // col_pieces
    piece_row = pl.multiple_of(group // col_pieces * piece_rows, piece_rows)
    piece_col = pl.multiple_of(lax.rem(group, col_pieces) * piece_cols, piece_cols)

    def wo_copies(layer):
        col = lambda c: pl.ds(pl.multiple_of(piece_col + c * (piece_cols // 2), LANES), piece_cols // 2)
        dst = lambda slot, c: wob.at[layer, slot, pl.ds(piece_row, piece_rows), col(c)]
        fr, fl = block_forwards(dst)
        piece = lambda slot, count: wob.at[layer, pl.ds(slot, count), pl.ds(piece_row, piece_rows), pl.ds(piece_col, piece_cols)]
        to_right = remote(piece(OWN, 1), piece(LT, 1), right)
        to_left = remote(piece(OWN, 1), piece(RT, 1), left)
        spread = [[remote(piece(slot, count), piece(slot, count), lax.rem(group + k, groups), "dp") for k in range(1, groups)]
                  for slot, count in ((RT, 2), (OP, 1))]
        push = {s: remote(wob.at[layer, s, pl.ds(0, share), :], wob.at[layer, s, pl.ds(share, share), :], partner)
                for s in (RT, LT, OP)}
        return to_right, to_left, fr, fl, spread, push

    wo_r, wo_l, wo_fr, wo_fl, wo_spread, wo_share = zip(*[wo_copies(layer) for layer in range(layers)])

    def start_wo(layer):
        wo_r[layer].start()
        wo_l[layer].start()

    def forward_wo(layer):
        wo_r[layer].wait_recv()
        wo_fr[layer].start()
        wo_l[layer].wait_recv()
        wo_fl[layer].start()
        for copy in wo_spread[layer][0]:
            copy.start()

    def spread_far_wo(layer):
        wo_fr[layer].wait_recv()
        wo_fl[layer].wait_recv()
        for copy in wo_spread[layer][1]:
            copy.start()

    def share_wo_near(layer):
        for copy in wo_spread[layer][0]:
            copy.wait_recv()
        wo_share[layer][LT].start()
        wo_share[layer][RT].start()

    def share_wo_far(layer):
        for copy in wo_spread[layer][1]:
            copy.wait_recv()
        wo_share[layer][OP].start()

    small_sends = [remote(smalls, sm_all.at[me], lax.rem(me + k, n)) for k in range(1, n)]
    tok_src = lambda c: part(tokb, OWN, None, c)
    tok_dst = lambda slot, c: part(tokb, slot, None, c)
    tok_r, tok_l = block_sends(tok_src, tok_dst)
    def to_partner(ref):
        return lambda own, other: remote(ref(own), ref(other), partner)

    qkv_push = [[to_partner(lambda o, i=i: wqkvb.at[layer, :, pl.ds(i * chip_cols + o * share, share)])(0, 1)
                 for i in range(3)] for layer in range(layers)]
    in_push = [[to_partner(lambda o, i=i: winb.at[layer, i, pl.ds(o * ff_share, ff_share), :])(0, 1) for i in range(2)]
               for layer in range(layers)]
    out_push = [to_partner(lambda o: woutb.at[layer, pl.ds(o * ff_share, ff_share), :])(0, 1) for layer in range(layers)]
    wo_push = [to_partner(lambda o: wob.at[layer, OWN, pl.ds(o * share, share), :])(0, 1) for layer in range(layers)]

    for copy in small_sends:
        copy.start()
    for copy in wo_loads:
        copy.wait()
    start_wo(0)
    tok_load.wait()
    tok_r[0].start()
    tok_l[1].start()
    for load_copy, copy in zip(qkv_loads[0], qkv_push[0]):
        load_copy.wait()
        copy.start()
    wo_push[0].start()
    for load_copy, copy in zip(in_loads[0], in_push[0]):
        load_copy.wait()
        copy.start()
    out_loads[0].wait()
    out_push[0].start()

    sm_all[me] = smalls[...]
    for copy in small_sends:
        copy.wait_recv()
    for k in range(n):
        gainb[:, k * LANES:(k + 1) * LANES] = sm_all[k]
    for slot, device in ((OWN, me), (RT, right), (LT, left), (OP, opposite)):
        lenb[slot] = jnp.broadcast_to(sm_all[device, ROW_LEN:ROW_LEN + 1, :], (8, LANES))

    def norm_rows(load_row, gain_row, dst, start, count, masked=False):
        step = 32

        def body(i, carry):
            r = pl.multiple_of(start + i * step, step)
            x = load_row(r, step)
            mean_sq = jnp.mean(x * x, axis=-1, keepdims=True)
            normed = x * lax.rsqrt(mean_sq + NORM_EPS) * gainb[gain_row:gain_row + 1, :]
            if masked:
                position = (r + lax.broadcasted_iota(jnp.int32, (step, d_model), 0)).astype(F32)
                normed = jnp.where(position < lenb[OWN, 0:1, 0:1], normed, 0.0)
            dst[pl.ds(r, step), :] = normed.astype(BF16)
            return carry

        lax.fori_loop(0, count // step, body, 0)

    def token_row(r, step):
        return tokb[pl.ds(r, step), :].astype(F32)

    def hidden_row(r, step):
        return hb[pl.ds(r, step), :]

    lane_low = lax.rem(lax.broadcasted_iota(jnp.int32, (1, chip_cols), 1), 2 * HEAD_DIM) < HEAD_DIM

    def project(layer, src, slot, count):
        x = src[rows(slot, count), :]
        q = dot(x, wqkvb[layer, :, 0:chip_cols])
        qb[rows(slot, count), :] = q.astype(BF16)
        for i, ref in ((1, kb), (2, vb)):
            y = dot(x, wqkvb[layer, :, i * chip_cols:(i + 1) * chip_cols])
            ref[0, rows(slot, count), :] = jnp.where(lane_low, y, 0.0).astype(BF16)
            ref[1, rows(slot, count), :] = jnp.where(lane_low, 0.0, y).astype(BF16)

    key_index = lax.broadcasted_iota(jnp.int32, (1, seq), 1).astype(F32)

    def attend(layer, slot, count):
        def body(i, carry):
            s = slot + i
            row = pl.ds(pl.multiple_of(s * seq, seq), seq)
            key_ok = key_index < lenb[s, 0:1, :]
            for pair in range(chip_cols // LANES):
                col = pl.ds(pair * LANES, LANES)
                keys = jnp.concatenate([kb[0, row, col], kb[1, row, col]], axis=0)
                scores = dot_rows(qb[row, col], keys)
                scores = scores + biasb[layer, pair]
                probs = []
                for h in range(2):
                    x = jnp.where(key_ok, scores[:, h * seq:(h + 1) * seq], MASKED)
                    e = jnp.exp(x - jnp.max(x, axis=-1, keepdims=True))
                    probs.append((e / jnp.sum(e, axis=-1, keepdims=True)).astype(BF16))
                values = jnp.concatenate([vb[0, row, col], vb[1, row, col]], axis=0)
                cb[0, row, col] = dot(jnp.concatenate(probs, axis=1), values).astype(BF16)
            return carry

        lax.fori_loop(0, count, body, 0)

    def build_bias():
        rel = lax.broadcasted_iota(jnp.int32, (LANES, 2 * seq), 1)
        rel = jnp.where(rel < seq, rel, rel - 2 * seq)
        lane = lax.broadcasted_iota(jnp.int32, (LANES, 2 * seq), 0)
        one_hot = jnp.where(bucket_of(rel) == lax.rem(lane, NUM_BUCKETS), 1.0, 0.0).astype(BF16)
        table_row = lax.broadcasted_iota(jnp.int32, (8, LANES), 0)
        table_lane = lax.broadcasted_iota(jnp.int32, (8, LANES), 1)
        own_lanes = table_row == table_lane // NUM_BUCKETS
        for pair, device in ((0, me), (1, partner)):
            tables = jnp.where(own_lanes, sm_all[device, ROW_BIAS:ROW_BIAS + 1, :], 0.0)
            lines = dot(tables.astype(BF16), one_hot)
            for layer in range(layers):
                for h in range(2):
                    row = 2 * layer + h
                    line = jnp.broadcast_to(lines[row:row + 1, :], (seq, 2 * seq))
                    shifted = pltpu.roll(line, 0, 1, stride=1, stride_axis=0)
                    biasb[layer, pair, :, h * seq:(h + 1) * seq] = shifted[:, 0:seq]

    norm_rows(token_row, ROW_ATTN, nb, OWN * seq, seq)
    build_bias()
    for copy in qkv_push[0]:
        copy.wait_recv()
    project(0, nb, OWN, 1)
    attend(0, OWN, 1)

    forward_wo(0)
    tok_r[1].start()
    tok_l[0].start()
    tok_fr, tok_fl = block_forwards(tok_dst)
    tok_r[0].wait_recv()
    tok_fr.start()
    tok_l[1].wait_recv()
    tok_fl.start()

    def c_part(src, slot, pair):
        return cb.at[src, rows(slot), pl.ds(pair * LANES, LANES)]

    c_r, c_l = {}, {}

    for slot in (OWN, RT, LT, OP):
        c_r[slot] = remote(cb.at[0, rows(slot), :], cb.at[LT, rows(TO_RIGHT[slot]), :], right)
        c_l[slot] = remote(cb.at[0, rows(slot), :], cb.at[RT, rows(TO_LEFT[slot]), :], left)

    def send_context(to_right, to_left):
        c_r[to_right].start()
        c_l[to_left].start()

    c_fr, c_fl = {}, {}

    def forward_context(slot):
        near, far = TO_RIGHT[slot], TO_RIGHT[TO_RIGHT[slot]]
        c_fr[slot] = remote(c_part(LT, near, 0), c_part(OP, far, 0), right)
        c_r[slot].wait_recv()
        c_fr[slot].start()
        near, far = TO_LEFT[slot], TO_LEFT[TO_LEFT[slot]]
        c_fl[slot] = remote(c_part(RT, near, 1), c_part(OP, far, 1), left)
        c_l[slot].wait_recv()
        c_fl[slot].start()

    send_context(OWN, OWN)

    spread_far_wo(0)
    tok_r[1].wait_recv()
    tok_l[0].wait_recv()
    norm_rows(token_row, ROW_ATTN, nb, RT * seq, 2 * seq)
    project(0, nb, RT, 2)
    attend(0, RT, 2)
    send_context(LT, RT)
    send_context(RT, LT)

    forward_context(OWN)
    tok_fr.wait_recv()
    tok_fl.wait_recv()
    norm_rows(token_row, ROW_ATTN, nb, OP * seq, seq)
    project(0, nb, OP, 1)
    attend(0, OP, 1)
    send_context(OP, OP)
    start_wo(1)

    def add_context(slot, count):
        for j in range(0, d_model, chip_cols):
            col = pl.ds(j, chip_cols)
            y = tokb[rows(slot, count), col].astype(F32)
            for src in (OWN, RT, LT, OP):
                y += dot(cb[src, rows(slot, count), :], wob[0, src, :, col])
            hb[rows(slot, count), col] = y

    forward_context(LT)
    forward_context(RT)
    share_wo_near(0)
    share_wo_far(0)
    wo_push[0].wait_recv()
    for copy in in_push[0]:
        copy.wait_recv()
    out_push[0].wait_recv()

    def feed_forward(layer, slot, count):
        x = mb[layer, rows(slot, count), :]
        gate = dot_rows(x, winb[layer, 0])
        lin = dot_rows(x, winb[layer, 1])
        mixed = (jax.nn.gelu(gate, approximate=True) * lin).astype(BF16)
        for j in range(0, d_model, chip_cols):
            col = pl.ds(j, chip_cols)
            pb[layer, rows(slot, count), col] = dot(mixed, woutb[layer, :, col])

    def scatter_copies(layer):
        p, ra, rb = pb.at[layer], relay_a.at[layer], relay_b.at[layer]
        rl, rr = recv_l.at[layer], recv_r.at[layer]
        row = lambda r: pl.ds(r * rows_half, rows_half)
        copies = {}
        for r in range(2):
            copies["op_r", r] = remote(part(p, OP, r, 0), ra.at[row(r), :], right)
            copies["op_l", r] = remote(part(p, OP, r, 1), rb.at[row(r), :], left)
            copies["plain_r", r] = remote(part(p, RT, r, 1), part(rl, 0, r, 1), right)
            copies["plain_l", r] = remote(part(p, LT, r, 0), part(rr, 0, r, 0), left)
            copies["sum_r", r] = remote(part(p, RT, r, 0), part(rl, 0, r, 0), right)
            copies["sum_l", r] = remote(part(p, LT, r, 1), part(rr, 0, r, 1), left)
        return copies

    def pass_on(layer, copies, r):
        a = pl.ds(RT * seq + r * rows_half, rows_half)
        b = pl.ds(LT * seq + r * rows_half, rows_half)
        row = pl.ds(r * rows_half, rows_half)
        copies["op_r", r].wait_recv()
        pb[layer, a, 0:half] += relay_a[layer, row, :]
        copies["sum_r", r].start()
        copies["op_l", r].wait_recv()
        pb[layer, b, half:d_model] += relay_b[layer, row, :]
        copies["sum_l", r].start()

    def collect(layer, copies, r):
        for name in ("plain_r", "plain_l", "sum_r", "sum_l"):
            copies[name, r].wait_recv()
        row = pl.ds(r * rows_half, rows_half)
        hb[row, :] = hb[row, :] + ((pb[layer, row, :] + recv_l[layer, row, :]) + recv_r[layer, row, :])

    rs = scatter_copies(0)
    c_fr[OWN].wait_recv()
    c_fl[OWN].wait_recv()
    for slot in (RT, LT, OP):
        wo_share[0][slot].wait_recv()
    add_context(OP, 1)
    norm_rows(hidden_row, ROW_FFN, mb.at[0], OP * seq, seq)
    feed_forward(0, OP, 1)
    forward_context(OP)
    for r in range(2):
        rs["op_r", r].start()
        rs["op_l", r].start()
    for slot in (RT, LT):
        c_fr[slot].wait_recv()
        c_fl[slot].wait_recv()
    add_context(RT, 2)
    norm_rows(hidden_row, ROW_FFN, mb.at[0], RT * seq, 2 * seq)
    feed_forward(0, RT, 2)
    rs["plain_r", 0].start()
    rs["plain_l", 0].start()
    forward_wo(1)
    c_fr[OP].wait_recv()
    c_fl[OP].wait_recv()
    add_context(OWN, 1)
    norm_rows(hidden_row, ROW_FFN, mb.at[0], OWN * seq, seq)
    feed_forward(0, OWN, 1)
    pass_on(0, rs, 0)
    rs["plain_r", 1].start()
    rs["plain_l", 1].start()
    pass_on(0, rs, 1)
    spread_far_wo(1)
    for load_copy, copy in zip(qkv_loads[1], qkv_push[1]):
        load_copy.wait()
        copy.start()
    wo_push[1].start()
    for load_copy, copy in zip(in_loads[1], in_push[1]):
        load_copy.wait()
        copy.start()
    out_loads[1].wait()
    out_push[1].start()

    def gather_copies(ref, r):
        to_right = [remote(part(ref, OWN, r, c), part(ref, LT, r, c), right) for c in range(2)]
        to_left = [remote(part(ref, OWN, r, c), part(ref, RT, r, c), left) for c in range(2)]
        fr = remote(part(ref, LT, r, 0), part(ref, OP, r, 0), right)
        fl = remote(part(ref, RT, r, 1), part(ref, OP, r, 1), left)
        return to_right, to_left, fr, fl

    n_gather = [gather_copies(mb.at[2], r) for r in range(2)]
    for r in range(2):
        collect(0, rs, r)
        norm_rows(hidden_row, 1, mb.at[2], r * rows_half, rows_half)
        to_right, to_left, _, _ = n_gather[r]
        to_right[0].start()
        to_left[1].start()
        to_right[1].start()
        to_left[0].start()

    def forward_gather(gather):
        to_right, to_left, fr, fl = gather
        to_right[0].wait_recv()
        fr.start()
        to_left[1].wait_recv()
        fl.start()

    forward_gather(n_gather[0])
    for copy in qkv_push[1]:
        copy.wait_recv()
    for copies in c_r, c_l:
        for slot in (OWN, RT, LT, OP):
            copies[slot].wait_send()
            done.add(id(copies[slot]))
    project(1, mb.at[2], OWN, 1)
    attend(1, OWN, 1)
    forward_gather(n_gather[1])
    share_wo_near(1)
    share_wo_far(1)
    for r in range(2):
        n_gather[r][0][1].wait_recv()
        n_gather[r][1][0].wait_recv()
    project(1, mb.at[2], RT, 2)
    attend(1, RT, 2)
    ctx_r = remote(cb.at[0, rows(RT), :], c1b.at[LT], right)
    ctx_l = remote(cb.at[0, rows(LT), :], c1b.at[RT], left)
    half_rows = lambda r: pl.ds(r * rows_half, rows_half)

    ctx_o = [remote(cb.at[0, pl.ds(OP * seq + r * rows_half, rows_half), :], c1b.at[OP, half_rows(r), :], opposite)
             for r in range(2)]
    ctx_r.start()
    ctx_l.start()
    for r in range(2):
        n_gather[r][2].wait_recv()
        n_gather[r][3].wait_recv()
    project(1, mb.at[2], OP, 1)
    attend(1, OP, 1)
    for copy in ctx_o:
        copy.start()
    wo_push[1].wait_recv()

    def add_second(src, context, r=None):
        row = rows(OWN) if r is None else half_rows(r)
        for j in range(0, d_model, chip_cols):
            col = pl.ds(j, chip_cols)
            hb[row, col] += dot(context, wob[1, src, :, col])

    add_second(OWN, cb[0, rows(OWN), :])
    for slot, copy in ((LT, ctx_r), (RT, ctx_l)):
        wo_share[1][slot].wait_recv()
        copy.wait_recv()
        add_second(slot, c1b[slot])
    wo_share[1][OP].wait_recv()
    m_gather = [gather_copies(mb.at[1], r) for r in range(2)]
    for r in range(2):
        ctx_o[r].wait_recv()
        add_second(OP, c1b[OP, half_rows(r), :], r)
        norm_rows(hidden_row, ROW_FFN + 1, mb.at[1], r * rows_half, rows_half)
        to_right, to_left, _, _ = m_gather[r]
        to_right[0].start()
        to_left[1].start()
        to_right[1].start()
        to_left[0].start()
    for copy in in_push[1]:
        copy.wait_recv()
    out_push[1].wait_recv()
    rs = scatter_copies(1)
    feed_forward(1, OWN, 1)
    for r in range(2):
        forward_gather(m_gather[r])
    for r in range(2):
        m_gather[r][0][1].wait_recv()
        m_gather[r][1][0].wait_recv()
    feed_forward(1, RT, 2)
    rs["plain_r", 0].start()
    rs["plain_l", 0].start()
    for r in range(2):
        m_gather[r][2].wait_recv()
        m_gather[r][3].wait_recv()
    feed_forward(1, OP, 1)
    for r in range(2):
        rs["op_r", r].start()
        rs["op_l", r].start()
    rs["plain_r", 1].start()
    rs["plain_l", 1].start()
    for r in range(2):
        pass_on(1, rs, r)
    for r in range(2):
        collect(1, rs, r)
        norm_rows(hidden_row, ROW_FINAL, out, r * rows_half, rows_half, masked=True)
    for copy in sent:
        if id(copy) not in done:
            copy.wait_send()


def encode(n, groups, lengths, attn_gain, ffn_gain, final_gain, bias_table, tokens, w_q, w_k, w_v, w_o, w_in0, w_in1, w_out):
    _, seq, d_model = tokens.shape
    layers, _, share = w_q.shape
    ff_share = w_out.shape[1]
    chip_cols = 2 * share
    ring = n // 2
    vmem = pl.BlockSpec(memory_space=pltpu.VMEM)
    scratch = [
        pltpu.VMEM(lengths.shape, jnp.int32),
        pltpu.VMEM(attn_gain.shape, BF16),
        pltpu.VMEM(ffn_gain.shape, BF16),
        pltpu.VMEM(final_gain.shape, BF16),
        pltpu.VMEM(bias_table.shape, BF16),
        pltpu.VMEM((SMALL_ROWS, LANES), F32),
        pltpu.VMEM((n, SMALL_ROWS, LANES), F32),
        pltpu.VMEM((8, d_model), F32),
        pltpu.VMEM((ring, 8, LANES), F32),
        pltpu.VMEM((layers, 2, seq, 2 * seq), F32),
        pltpu.VMEM((ring * seq, d_model), BF16),
        pltpu.VMEM((ring * seq, d_model), BF16),
        pltpu.VMEM((layers + 1, ring * seq, d_model), BF16),
        pltpu.VMEM((layers, d_model, 3 * chip_cols), BF16),
        pltpu.VMEM((layers, ring, chip_cols, d_model), BF16),
        pltpu.VMEM((layers, 2, 2 * ff_share, d_model), BF16),
        pltpu.VMEM((layers, 2 * ff_share, d_model), BF16),
        pltpu.VMEM((ring * seq, chip_cols), BF16),
        pltpu.VMEM((2, ring * seq, chip_cols), BF16),
        pltpu.VMEM((2, ring * seq, chip_cols), BF16),
        pltpu.VMEM((ring, ring * seq, chip_cols), BF16),
        pltpu.VMEM((ring, seq, chip_cols), BF16),
        pltpu.VMEM((ring * seq, d_model), F32),
        pltpu.VMEM((layers, ring * seq, d_model), F32),
        pltpu.VMEM((layers, seq, d_model // 2), F32),
        pltpu.VMEM((layers, seq, d_model // 2), F32),
        pltpu.VMEM((layers, seq, d_model), F32),
        pltpu.VMEM((layers, seq, d_model), F32),
        pltpu.SemaphoreType.DMA((160 + 4 * groups,)),
        pltpu.SemaphoreType.DMA((160 + 4 * groups,)),
        pltpu.SemaphoreType.DMA((32,)),
    ]
    return pl.pallas_call(
        functools.partial(kernel, n, groups),
        out_shape=pltpu.VMEM((seq, d_model), BF16),
        in_specs=[pl.BlockSpec(memory_space=pltpu.HBM)] * 13,
        out_specs=vmem,
        scratch_shapes=scratch,
        compiler_params=pltpu.CompilerParams(
            collective_id=0, has_side_effects=True, vmem_limit_bytes=56 * 1024 * 1024),
    )(lengths, attn_gain, ffn_gain, final_gain, bias_table, tokens, w_q, w_k, w_v, w_o, w_in0, w_in1, w_out)


def solution(mesh):
    n, groups = mesh.shape["fsdp"], mesh.shape["dp"]
    batch_spec = P(("dp", "fsdp"))
    col_spec = P(None, None, "fsdp")
    row_spec = P(None, "fsdp", None)
    gain_spec = P(None, "fsdp")
    in_specs = (batch_spec, batch_spec, gain_spec, col_spec, col_spec, col_spec, row_spec, col_spec, gain_spec,
                col_spec, col_spec, row_spec, P("fsdp"))

    def local_forward(tokens, lengths, attn_gain, w_q, w_k, w_v, w_o, rel_bias, ffn_gain, w_in0, w_in1, w_out, final_gain):
        layers, buckets, heads = rel_bias.shape
        bias_table = jnp.swapaxes(rel_bias, 1, 2).reshape(layers * heads, buckets)
        encoded = encode(n, groups, lengths[None], attn_gain, ffn_gain, final_gain[None], bias_table, tokens, w_q, w_k, w_v, w_o,
                            jnp.swapaxes(w_in0, 1, 2), jnp.swapaxes(w_in1, 1, 2), w_out)
        return encoded[None]

    return jax.shard_map(local_forward, mesh=mesh, in_specs=in_specs, out_specs=batch_spec, check_vma=False)
```

```python
import functools

import jax
import jax.numpy as jnp
from jax import lax
from jax.experimental import pallas as pl
from jax.experimental.pallas import tpu as pltpu
from jax.sharding import PartitionSpec as P

HEAD_DIM = 64
NUM_BUCKETS = 32
NORM_EPS = 1e-6
LANES = 128
ROW_PARTS = 4
MASKED = -1e30
MESH = pl.DeviceIdType.MESH
BF16 = jnp.bfloat16
F32 = jnp.float32

ROW_ATTN, ROW_FFN, ROW_FINAL, ROW_BIAS, ROW_LEN, SMALL_ROWS = 0, 2, 4, 5, 6, 8

OWN, RT, LT, OP = 0, 1, 2, 3
TO_RIGHT = {OWN: LT, RT: OWN, LT: OP, OP: RT}
TO_LEFT = {OWN: RT, RT: OP, LT: OWN, OP: LT}


def bucket_of(rel_pos):
    half_buckets = NUM_BUCKETS // 2
    max_exact = half_buckets // 2
    distance = jnp.abs(rel_pos)
    log_bucket = jnp.full_like(distance, max_exact)
    for step in range(1, half_buckets - max_exact):
        log_bucket += jnp.where(distance * distance >= max_exact * max_exact * 2**step, 1, 0)
    return jnp.where(rel_pos > 0, half_buckets, 0) + jnp.where(distance < max_exact, distance, log_bucket)


def dot(a, b):
    return jnp.dot(a, b, preferred_element_type=F32)


def dot_rows(a, b):
    return lax.dot_general(a, b, (((1,), (1,)), ((), ())), preferred_element_type=F32)


def kernel(n, groups, lengths_in, attn_gain_in, ffn_gain_in, final_gain_in, bias_table_in,
           tok, wq, wk, wv, wo, win0, win1, wout, out,
           lengths, attn_gain, ffn_gain, final_gain, bias_table, smalls, sm_all, gainb, lenb, biasb, tokb, nb, mb, wqkvb, wob, winb, woutb, qb, kb, vb, cb, c1b, hb, pb,
           relay_a, relay_b, recv_l, recv_r, send_sem, recv_sem, load_sem):
    seq, d_model = tok.shape[1], tok.shape[2]
    layers = wq.shape[0]
    half, rows_part = d_model // 2, seq // ROW_PARTS
    share, ff_share = wq.shape[2], wout.shape[1]
    chip_cols = 2 * share

    me, group = lax.axis_index("fsdp"), lax.axis_index("dp")
    right, left = lax.rem(me + 2, n), lax.rem(me + n - 2, n)
    opposite = lax.rem(me + n // 2, n)
    partner = me + 1 - 2 * lax.rem(me, 2)
    counts = {"remote": 0, "local": 0}
    sent, done = [], set()

    def remote(src, dst, device, axis="fsdp"):
        index = counts["remote"]
        counts["remote"] += 1
        copy = pltpu.make_async_remote_copy(
            src_ref=src, dst_ref=dst, send_sem=send_sem.at[index], recv_sem=recv_sem.at[index],
            device_id={axis: device}, device_id_type=MESH)
        sent.append(copy)
        return copy

    def load(src, dst):
        index = counts["local"]
        counts["local"] += 1
        copy = pltpu.make_async_copy(src, dst, load_sem.at[index])
        copy.start()
        return copy

    def rows(slot, count=1):
        return pl.ds(slot * seq, count * seq)

    def part(ref, slot, r, c):
        row = pl.ds(slot * seq, seq) if r is None else pl.ds(slot * seq + r * rows_part, rows_part)
        col = slice(None) if c is None else pl.ds(c * half, half)
        return ref.at[row, col]

    barrier = pltpu.get_barrier_semaphore()
    for k in range(1, n):
        pl.semaphore_signal(barrier, inc=1, device_id={"fsdp": lax.rem(me + k, n)}, device_id_type=MESH)
    for k in range(1, groups):
        pl.semaphore_signal(barrier, inc=1, device_id={"dp": lax.rem(group + k, groups)}, device_id_type=MESH)

    small_loads = [load(src, dst) for src, dst in zip(
        (lengths_in, attn_gain_in, ffn_gain_in, final_gain_in, bias_table_in),
        (lengths, attn_gain, ffn_gain, final_gain, bias_table))]
    tok_load = load(tok.at[0], tokb.at[rows(OWN), :])
    wo_loads = [load(wo.at[layer], wob.at[layer, OWN, pl.ds(0, share), :]) for layer in range(layers)]
    qkv_loads = []
    for layer in range(layers):
        qkv_loads.append([load(w.at[layer], wqkvb.at[layer, :, pl.ds(i * chip_cols, share)])
                          for i, w in enumerate((wq, wk, wv))])
        if layer == 0:
            in_loads = []
            out_loads = []
        in_loads.append([load(w.at[layer], winb.at[layer, i, pl.ds(0, ff_share), :]) for i, w in enumerate((win0, win1))])
        out_loads.append(load(wout.at[layer], woutb.at[layer, pl.ds(0, ff_share), :]))

    for copy in small_loads:
        copy.wait()
    smalls[ROW_ATTN:ROW_ATTN + layers, :] = attn_gain[...].astype(F32)
    smalls[ROW_FFN:ROW_FFN + layers, :] = ffn_gain[...].astype(F32)
    smalls[ROW_FINAL:ROW_FINAL + 1, :] = final_gain[...].astype(F32)
    table = bias_table[...].astype(F32)
    smalls[ROW_BIAS:ROW_BIAS + 1, :] = jnp.concatenate([table[i:i + 1] for i in range(table.shape[0])], axis=1)
    smalls[ROW_LEN:SMALL_ROWS, :] = jnp.broadcast_to(lengths[...].astype(F32), (SMALL_ROWS - ROW_LEN, LANES))

    pl.semaphore_wait(barrier, n - 1 + groups - 1)

    def block_sends(src, dst):
        to_right = [remote(src(c), dst(LT, c), right) for c in range(2)]
        to_left = [remote(src(c), dst(RT, c), left) for c in range(2)]
        return to_right, to_left

    def block_forwards(dst):
        return remote(dst(LT, 0), dst(OP, 0), right), remote(dst(RT, 1), dst(OP, 1), left)

    row_pieces = min(groups, share // 16)
    col_pieces = groups // row_pieces
    piece_rows, piece_cols = share // row_pieces, d_model // col_pieces
    piece_row = pl.multiple_of(group // col_pieces * piece_rows, piece_rows)
    piece_col = pl.multiple_of(lax.rem(group, col_pieces) * piece_cols, piece_cols)

    def wo_copies(layer):
        col = lambda c: pl.ds(pl.multiple_of(piece_col + c * (piece_cols // 2), LANES), piece_cols // 2)
        src = lambda c: wob.at[layer, OWN, pl.ds(piece_row, piece_rows), col(c)]
        dst = lambda slot, c: wob.at[layer, slot, pl.ds(piece_row, piece_rows), col(c)]
        to_right, to_left = block_sends(src, dst)
        fr, fl = block_forwards(dst)
        piece = lambda slot, count: wob.at[layer, pl.ds(slot, count), pl.ds(piece_row, piece_rows), pl.ds(piece_col, piece_cols)]
        spread = [[remote(piece(slot, count), piece(slot, count), lax.rem(group + k, groups), "dp") for k in range(1, groups)]
                  for slot, count in ((RT, 2), (OP, 1))]
        push = {s: remote(wob.at[layer, s, pl.ds(0, share), :], wob.at[layer, s, pl.ds(share, share), :], partner)
                for s in (RT, LT, OP)}
        return to_right, to_left, fr, fl, spread, push

    wo_r, wo_l, wo_fr, wo_fl, wo_spread, wo_share = zip(*[wo_copies(layer) for layer in range(layers)])

    def start_wo(layer):
        wo_r[layer][0].start()
        wo_l[layer][1].start()
        wo_r[layer][1].start()
        wo_l[layer][0].start()

    def forward_wo(layer):
        wo_r[layer][0].wait_recv()
        wo_fr[layer].start()
        wo_l[layer][1].wait_recv()
        wo_fl[layer].start()
        wo_r[layer][1].wait_recv()
        wo_l[layer][0].wait_recv()
        for copy in wo_spread[layer][0]:
            copy.start()

    def spread_far_wo(layer):
        wo_fr[layer].wait_recv()
        wo_fl[layer].wait_recv()
        for copy in wo_spread[layer][1]:
            copy.start()

    def share_wo_near(layer):
        for copy in wo_spread[layer][0]:
            copy.wait_recv()
        wo_share[layer][LT].start()
        wo_share[layer][RT].start()

    def share_wo_far(layer):
        for copy in wo_spread[layer][1]:
            copy.wait_recv()
        wo_share[layer][OP].start()

    small_sends = [remote(smalls, sm_all.at[me], lax.rem(me + k, n)) for k in range(1, n)]
    def gather_copies(ref, r):
        to_right = [remote(part(ref, OWN, r, c), part(ref, LT, r, c), right) for c in range(2)]
        to_left = [remote(part(ref, OWN, r, c), part(ref, RT, r, c), left) for c in range(2)]
        fr = remote(part(ref, LT, r, 0), part(ref, OP, r, 0), right)
        fl = remote(part(ref, RT, r, 1), part(ref, OP, r, 1), left)
        return to_right, to_left, fr, fl

    def forward_gather(gather):
        to_right, to_left, fr, fl = gather
        to_right[0].wait_recv()
        fr.start()
        to_left[1].wait_recv()
        fl.start()

    tok_gather = [gather_copies(tokb, r) for r in range(ROW_PARTS)]

    def to_partner(ref):
        return lambda own, other: remote(ref(own), ref(other), partner)

    qkv_push = [[to_partner(lambda o, i=i: wqkvb.at[layer, :, pl.ds(i * chip_cols + o * share, share)])(0, 1)
                 for i in range(3)] for layer in range(layers)]
    in_push = [[to_partner(lambda o, i=i: winb.at[layer, i, pl.ds(o * ff_share, ff_share), :])(0, 1) for i in range(2)]
               for layer in range(layers)]
    out_push = [to_partner(lambda o: woutb.at[layer, pl.ds(o * ff_share, ff_share), :])(0, 1) for layer in range(layers)]
    wo_push = [to_partner(lambda o: wob.at[layer, OWN, pl.ds(o * share, share), :])(0, 1) for layer in range(layers)]

    for copy in small_sends:
        copy.start()
    for copy in wo_loads:
        copy.wait()
    start_wo(0)
    tok_load.wait()
    for to_right, to_left, _, _ in tok_gather:
        to_right[0].start()
        to_left[1].start()
    for load_copy, copy in zip(qkv_loads[0], qkv_push[0]):
        load_copy.wait()
        copy.start()
    wo_push[0].start()
    for load_copy, copy in zip(in_loads[0], in_push[0]):
        load_copy.wait()
        copy.start()
    out_loads[0].wait()
    out_push[0].start()

    sm_all[me] = smalls[...]
    for copy in small_sends:
        copy.wait_recv()
    for k in range(n):
        gainb[:, k * LANES:(k + 1) * LANES] = sm_all[k]
    for slot, device in ((OWN, me), (RT, right), (LT, left), (OP, opposite)):
        lenb[slot] = jnp.broadcast_to(sm_all[device, ROW_LEN:ROW_LEN + 1, :], (8, LANES))

    def norm_rows(load_row, gain_row, dst, start, count, masked=False):
        step = 32

        def body(i, carry):
            r = pl.multiple_of(start + i * step, step)
            x = load_row(r, step)
            mean_sq = jnp.mean(x * x, axis=-1, keepdims=True)
            normed = x * lax.rsqrt(mean_sq + NORM_EPS) * gainb[gain_row:gain_row + 1, :]
            if masked:
                position = (r + lax.broadcasted_iota(jnp.int32, (step, d_model), 0)).astype(F32)
                normed = jnp.where(position < lenb[OWN, 0:1, 0:1], normed, 0.0)
            dst[pl.ds(r, step), :] = normed.astype(BF16)
            return carry

        lax.fori_loop(0, count // step, body, 0)

    def token_row(r, step):
        return tokb[pl.ds(r, step), :].astype(F32)

    def hidden_row(r, step):
        return hb[pl.ds(r, step), :]

    lane_low = lax.rem(lax.broadcasted_iota(jnp.int32, (1, chip_cols), 1), 2 * HEAD_DIM) < HEAD_DIM

    def project(layer, src, slot, count):
        x = src[rows(slot, count), :]
        q = dot(x, wqkvb[layer, :, 0:chip_cols])
        qb[rows(slot, count), :] = q.astype(BF16)
        for i, ref in ((1, kb), (2, vb)):
            y = dot(x, wqkvb[layer, :, i * chip_cols:(i + 1) * chip_cols])
            ref[0, rows(slot, count), :] = jnp.where(lane_low, y, 0.0).astype(BF16)
            ref[1, rows(slot, count), :] = jnp.where(lane_low, 0.0, y).astype(BF16)

    key_index = lax.broadcasted_iota(jnp.int32, (1, seq), 1).astype(F32)

    def attend(layer, slot, count):
        def body(i, carry):
            s = slot + i
            row = pl.ds(pl.multiple_of(s * seq, seq), seq)
            key_ok = key_index < lenb[s, 0:1, :]
            for pair in range(chip_cols // LANES):
                col = pl.ds(pair * LANES, LANES)
                keys = jnp.concatenate([kb[0, row, col], kb[1, row, col]], axis=0)
                scores = dot_rows(qb[row, col], keys)
                scores = scores + biasb[layer, pair]
                probs = []
                for h in range(2):
                    x = jnp.where(key_ok, scores[:, h * seq:(h + 1) * seq], MASKED)
                    e = jnp.exp(x - jnp.max(x, axis=-1, keepdims=True))
                    probs.append((e / jnp.sum(e, axis=-1, keepdims=True)).astype(BF16))
                values = jnp.concatenate([vb[0, row, col], vb[1, row, col]], axis=0)
                cb[0, row, col] = dot(jnp.concatenate(probs, axis=1), values).astype(BF16)
            return carry

        lax.fori_loop(0, count, body, 0)

    def build_bias():
        rel = lax.broadcasted_iota(jnp.int32, (LANES, 2 * seq), 1)
        rel = jnp.where(rel < seq, rel, rel - 2 * seq)
        lane = lax.broadcasted_iota(jnp.int32, (LANES, 2 * seq), 0)
        one_hot = jnp.where(bucket_of(rel) == lax.rem(lane, NUM_BUCKETS), 1.0, 0.0).astype(BF16)
        table_row = lax.broadcasted_iota(jnp.int32, (8, LANES), 0)
        table_lane = lax.broadcasted_iota(jnp.int32, (8, LANES), 1)
        own_lanes = table_row == table_lane // NUM_BUCKETS
        for pair, device in ((0, me), (1, partner)):
            tables = jnp.where(own_lanes, sm_all[device, ROW_BIAS:ROW_BIAS + 1, :], 0.0)
            lines = dot(tables.astype(BF16), one_hot)
            for layer in range(layers):
                for h in range(2):
                    row = 2 * layer + h
                    line = jnp.broadcast_to(lines[row:row + 1, :], (seq, 2 * seq))
                    shifted = pltpu.roll(line, 0, 1, stride=1, stride_axis=0)
                    biasb[layer, pair, :, h * seq:(h + 1) * seq] = shifted[:, 0:seq]

    norm_rows(token_row, ROW_ATTN, nb, OWN * seq, seq)
    build_bias()
    for copy in qkv_push[0]:
        copy.wait_recv()
    project(0, nb, OWN, 1)
    attend(0, OWN, 1)

    forward_wo(0)
    for to_right, to_left, _, _ in tok_gather:
        to_right[1].start()
        to_left[0].start()
    for gather in tok_gather:
        forward_gather(gather)

    def c_part(src, slot, pair):
        return cb.at[src, rows(slot), pl.ds(pair * LANES, LANES)]

    c_r, c_l = {}, {}

    for slot in (OWN, RT, LT, OP):
        c_r[slot] = [remote(c_part(0, slot, p), c_part(LT, TO_RIGHT[slot], p), right) for p in range(2)]
        c_l[slot] = [remote(c_part(0, slot, p), c_part(RT, TO_LEFT[slot], p), left) for p in range(2)]

    def send_context(to_right, to_left):
        c_r[to_right][0].start()
        c_l[to_left][1].start()
        c_r[to_right][1].start()
        c_l[to_left][0].start()

    c_fr, c_fl = {}, {}

    def forward_context(slot):
        near, far = TO_RIGHT[slot], TO_RIGHT[TO_RIGHT[slot]]
        c_fr[slot] = remote(c_part(LT, near, 0), c_part(OP, far, 0), right)
        c_r[slot][0].wait_recv()
        c_fr[slot].start()
        near, far = TO_LEFT[slot], TO_LEFT[TO_LEFT[slot]]
        c_fl[slot] = remote(c_part(RT, near, 1), c_part(OP, far, 1), left)
        c_l[slot][1].wait_recv()
        c_fl[slot].start()

    send_context(OWN, OWN)

    spread_far_wo(0)
    for to_right, to_left, _, _ in tok_gather:
        to_right[1].wait_recv()
        to_left[0].wait_recv()
    norm_rows(token_row, ROW_ATTN, nb, RT * seq, 2 * seq)
    project(0, nb, RT, 2)
    attend(0, RT, 2)
    send_context(LT, RT)
    send_context(RT, LT)

    forward_context(OWN)
    for _, _, fr, fl in tok_gather:
        fr.wait_recv()
        fl.wait_recv()
    norm_rows(token_row, ROW_ATTN, nb, OP * seq, seq)
    project(0, nb, OP, 1)
    attend(0, OP, 1)
    send_context(OP, OP)
    start_wo(1)

    def add_context(slot, count):
        for j in range(0, d_model, chip_cols):
            col = pl.ds(j, chip_cols)
            y = tokb[rows(slot, count), col].astype(F32)
            for src in (OWN, RT, LT, OP):
                y += dot(cb[src, rows(slot, count), :], wob[0, src, :, col])
            hb[rows(slot, count), col] = y

    forward_context(LT)
    forward_context(RT)
    share_wo_near(0)
    share_wo_far(0)
    wo_push[0].wait_recv()
    for copy in in_push[0]:
        copy.wait_recv()
    out_push[0].wait_recv()

    def feed_forward(layer, slot, count):
        x = mb[layer, rows(slot, count), :]
        gate = dot_rows(x, winb[layer, 0])
        lin = dot_rows(x, winb[layer, 1])
        mixed = (jax.nn.gelu(gate, approximate=True) * lin).astype(BF16)
        for j in range(0, d_model, chip_cols):
            col = pl.ds(j, chip_cols)
            pb[layer, rows(slot, count), col] = dot(mixed, woutb[layer, :, col])

    def scatter_copies(layer):
        p, ra, rb = pb.at[layer], relay_a.at[layer], relay_b.at[layer]
        rl, rr = recv_l.at[layer], recv_r.at[layer]
        row = lambda r: pl.ds(r * rows_part, rows_part)
        copies = {}
        for r in range(ROW_PARTS):
            copies["op_r", r] = remote(part(p, OP, r, 0), ra.at[row(r), :], right)
            copies["op_l", r] = remote(part(p, OP, r, 1), rb.at[row(r), :], left)
            copies["plain_r", r] = remote(part(p, RT, r, 1), part(rl, 0, r, 1), right)
            copies["plain_l", r] = remote(part(p, LT, r, 0), part(rr, 0, r, 0), left)
            copies["sum_r", r] = remote(part(p, RT, r, 0), part(rl, 0, r, 0), right)
            copies["sum_l", r] = remote(part(p, LT, r, 1), part(rr, 0, r, 1), left)
        return copies

    def pass_on(layer, copies, r):
        a = pl.ds(RT * seq + r * rows_part, rows_part)
        b = pl.ds(LT * seq + r * rows_part, rows_part)
        row = pl.ds(r * rows_part, rows_part)
        copies["op_r", r].wait_recv()
        pb[layer, a, 0:half] += relay_a[layer, row, :]
        copies["sum_r", r].start()
        copies["op_l", r].wait_recv()
        pb[layer, b, half:d_model] += relay_b[layer, row, :]
        copies["sum_l", r].start()

    def collect(layer, copies, r):
        for name in ("plain_r", "plain_l", "sum_r", "sum_l"):
            copies[name, r].wait_recv()
        row = pl.ds(r * rows_part, rows_part)
        hb[row, :] = hb[row, :] + ((pb[layer, row, :] + recv_l[layer, row, :]) + recv_r[layer, row, :])

    rs = scatter_copies(0)
    c_r[LT][1].wait_recv()
    c_l[RT][0].wait_recv()
    c_fr[OWN].wait_recv()
    c_fl[OWN].wait_recv()
    for slot in (RT, LT, OP):
        wo_share[0][slot].wait_recv()
    add_context(OP, 1)
    norm_rows(hidden_row, ROW_FFN, mb.at[0], OP * seq, seq)
    feed_forward(0, OP, 1)
    forward_context(OP)
    for r in range(ROW_PARTS):
        rs["op_r", r].start()
        rs["op_l", r].start()
    for slot in (OWN, OP):
        c_r[slot][1].wait_recv()
        c_l[slot][0].wait_recv()
    for slot in (RT, LT):
        c_fr[slot].wait_recv()
        c_fl[slot].wait_recv()
    add_context(RT, 2)
    norm_rows(hidden_row, ROW_FFN, mb.at[0], RT * seq, 2 * seq)
    feed_forward(0, RT, 2)
    for r in range(ROW_PARTS // 2):
        rs["plain_r", r].start()
        rs["plain_l", r].start()
    forward_wo(1)
    c_r[RT][1].wait_recv()
    c_l[LT][0].wait_recv()
    c_fr[OP].wait_recv()
    c_fl[OP].wait_recv()
    add_context(OWN, 1)
    norm_rows(hidden_row, ROW_FFN, mb.at[0], OWN * seq, seq)
    feed_forward(0, OWN, 1)
    for r in range(ROW_PARTS):
        pass_on(0, rs, r)
        if r < ROW_PARTS // 2:
            rs["plain_r", ROW_PARTS // 2 + r].start()
            rs["plain_l", ROW_PARTS // 2 + r].start()
    spread_far_wo(1)
    for load_copy, copy in zip(qkv_loads[1], qkv_push[1]):
        load_copy.wait()
        copy.start()
    wo_push[1].start()
    for load_copy, copy in zip(in_loads[1], in_push[1]):
        load_copy.wait()
        copy.start()
    out_loads[1].wait()
    out_push[1].start()

    n_gather = [gather_copies(mb.at[2], r) for r in range(ROW_PARTS)]
    for r in range(ROW_PARTS):
        collect(0, rs, r)
        norm_rows(hidden_row, 1, mb.at[2], r * rows_part, rows_part)
        to_right, to_left, _, _ = n_gather[r]
        to_right[0].start()
        to_left[1].start()
        to_right[1].start()
        to_left[0].start()

        if r >= 2:
            forward_gather(n_gather[r - 2])

    forward_gather(n_gather[ROW_PARTS - 2])
    for copy in qkv_push[1]:
        copy.wait_recv()
    for copies in c_r, c_l:
        for slot in (OWN, RT, LT, OP):
            for copy in copies[slot]:
                copy.wait_send()
                done.add(id(copy))
    project(1, mb.at[2], OWN, 1)
    attend(1, OWN, 1)
    forward_gather(n_gather[ROW_PARTS - 1])
    share_wo_near(1)
    share_wo_far(1)
    for r in range(ROW_PARTS):
        n_gather[r][0][1].wait_recv()
        n_gather[r][1][0].wait_recv()
    project(1, mb.at[2], RT, 2)
    attend(1, RT, 2)
    ctx_r = remote(cb.at[0, rows(RT), :], c1b.at[LT], right)
    ctx_l = remote(cb.at[0, rows(LT), :], c1b.at[RT], left)
    part_rows = lambda r: pl.ds(r * rows_part, rows_part)

    ctx_o = [remote(cb.at[0, pl.ds(OP * seq + r * rows_part, rows_part), :], c1b.at[OP, part_rows(r), :], opposite)
             for r in range(ROW_PARTS)]
    ctx_r.start()
    ctx_l.start()
    for r in range(ROW_PARTS):
        n_gather[r][2].wait_recv()
        n_gather[r][3].wait_recv()
    project(1, mb.at[2], OP, 1)
    attend(1, OP, 1)
    for copy in ctx_o:
        copy.start()
    wo_push[1].wait_recv()

    def add_second(src, context, r=None):
        row = rows(OWN) if r is None else part_rows(r)
        for j in range(0, d_model, chip_cols):
            col = pl.ds(j, chip_cols)
            hb[row, col] += dot(context, wob[1, src, :, col])

    add_second(OWN, cb[0, rows(OWN), :])
    for slot, copy in ((LT, ctx_r), (RT, ctx_l)):
        wo_share[1][slot].wait_recv()
        copy.wait_recv()
        add_second(slot, c1b[slot])
    wo_share[1][OP].wait_recv()
    m_gather = [gather_copies(mb.at[1], r) for r in range(ROW_PARTS)]
    for r in range(ROW_PARTS):
        ctx_o[r].wait_recv()
        add_second(OP, c1b[OP, part_rows(r), :], r)
        norm_rows(hidden_row, ROW_FFN + 1, mb.at[1], r * rows_part, rows_part)
        to_right, to_left, _, _ = m_gather[r]
        to_right[0].start()
        to_left[1].start()
        to_right[1].start()
        to_left[0].start()
    for copy in in_push[1]:
        copy.wait_recv()
    out_push[1].wait_recv()
    rs = scatter_copies(1)
    for r in range(ROW_PARTS // 2):
        forward_gather(m_gather[r])
    feed_forward(1, OWN, 1)
    for r in range(ROW_PARTS // 2, ROW_PARTS):
        forward_gather(m_gather[r])
    for r in range(ROW_PARTS):
        m_gather[r][0][1].wait_recv()
        m_gather[r][1][0].wait_recv()
    feed_forward(1, RT, 2)
    for r in range(ROW_PARTS // 2):
        rs["plain_r", r].start()
        rs["plain_l", r].start()
    for r in range(ROW_PARTS):
        m_gather[r][2].wait_recv()
        m_gather[r][3].wait_recv()
    feed_forward(1, OP, 1)
    for r in range(ROW_PARTS):
        rs["op_r", r].start()
        rs["op_l", r].start()
    for r in range(ROW_PARTS // 2, ROW_PARTS):
        rs["plain_r", r].start()
        rs["plain_l", r].start()
    for r in range(ROW_PARTS):
        pass_on(1, rs, r)
    for r in range(ROW_PARTS):
        collect(1, rs, r)
        norm_rows(hidden_row, ROW_FINAL, out, r * rows_part, rows_part, masked=True)
    for copy in sent:
        if id(copy) not in done:
            copy.wait_send()


def encode(n, groups, lengths, attn_gain, ffn_gain, final_gain, bias_table, tokens, w_q, w_k, w_v, w_o, w_in0, w_in1, w_out):
    _, seq, d_model = tokens.shape
    layers, _, share = w_q.shape
    ff_share = w_out.shape[1]
    chip_cols = 2 * share
    ring = n // 2
    vmem = pl.BlockSpec(memory_space=pltpu.VMEM)
    scratch = [
        pltpu.VMEM(lengths.shape, jnp.int32),
        pltpu.VMEM(attn_gain.shape, BF16),
        pltpu.VMEM(ffn_gain.shape, BF16),
        pltpu.VMEM(final_gain.shape, BF16),
        pltpu.VMEM(bias_table.shape, BF16),
        pltpu.VMEM((SMALL_ROWS, LANES), F32),
        pltpu.VMEM((n, SMALL_ROWS, LANES), F32),
        pltpu.VMEM((8, d_model), F32),
        pltpu.VMEM((ring, 8, LANES), F32),
        pltpu.VMEM((layers, 2, seq, 2 * seq), F32),
        pltpu.VMEM((ring * seq, d_model), BF16),
        pltpu.VMEM((ring * seq, d_model), BF16),
        pltpu.VMEM((layers + 1, ring * seq, d_model), BF16),
        pltpu.VMEM((layers, d_model, 3 * chip_cols), BF16),
        pltpu.VMEM((layers, ring, chip_cols, d_model), BF16),
        pltpu.VMEM((layers, 2, 2 * ff_share, d_model), BF16),
        pltpu.VMEM((layers, 2 * ff_share, d_model), BF16),
        pltpu.VMEM((ring * seq, chip_cols), BF16),
        pltpu.VMEM((2, ring * seq, chip_cols), BF16),
        pltpu.VMEM((2, ring * seq, chip_cols), BF16),
        pltpu.VMEM((ring, ring * seq, chip_cols), BF16),
        pltpu.VMEM((ring, seq, chip_cols), BF16),
        pltpu.VMEM((ring * seq, d_model), F32),
        pltpu.VMEM((layers, ring * seq, d_model), F32),
        pltpu.VMEM((layers, seq, d_model // 2), F32),
        pltpu.VMEM((layers, seq, d_model // 2), F32),
        pltpu.VMEM((layers, seq, d_model), F32),
        pltpu.VMEM((layers, seq, d_model), F32),
        pltpu.SemaphoreType.DMA((240 + 4 * groups,)),
        pltpu.SemaphoreType.DMA((240 + 4 * groups,)),
        pltpu.SemaphoreType.DMA((32,)),
    ]
    return pl.pallas_call(
        functools.partial(kernel, n, groups),
        out_shape=pltpu.VMEM((seq, d_model), BF16),
        in_specs=[pl.BlockSpec(memory_space=pltpu.HBM)] * 13,
        out_specs=vmem,
        scratch_shapes=scratch,
        compiler_params=pltpu.CompilerParams(
            collective_id=0, has_side_effects=True, vmem_limit_bytes=56 * 1024 * 1024),
    )(lengths, attn_gain, ffn_gain, final_gain, bias_table, tokens, w_q, w_k, w_v, w_o, w_in0, w_in1, w_out)


def solution(mesh):
    n, groups = mesh.shape["fsdp"], mesh.shape["dp"]
    batch_spec = P(("dp", "fsdp"))
    col_spec = P(None, None, "fsdp")
    row_spec = P(None, "fsdp", None)
    gain_spec = P(None, "fsdp")
    in_specs = (batch_spec, batch_spec, gain_spec, col_spec, col_spec, col_spec, row_spec, col_spec, gain_spec,
                col_spec, col_spec, row_spec, P("fsdp"))

    def local_forward(tokens, lengths, attn_gain, w_q, w_k, w_v, w_o, rel_bias, ffn_gain, w_in0, w_in1, w_out, final_gain):
        layers, buckets, heads = rel_bias.shape
        bias_table = jnp.swapaxes(rel_bias, 1, 2).reshape(layers * heads, buckets)
        encoded = encode(n, groups, lengths[None], attn_gain, ffn_gain, final_gain[None], bias_table, tokens, w_q, w_k, w_v, w_o,
                            jnp.swapaxes(w_in0, 1, 2), jnp.swapaxes(w_in1, 1, 2), w_out)
        return encoded[None]

    return jax.shard_map(local_forward, mesh=mesh, in_specs=in_specs, out_specs=batch_spec, check_vma=False)
```

```python
import functools

import jax
import jax.numpy as jnp
from jax import lax
from jax.experimental import pallas as pl
from jax.experimental.pallas import tpu as pltpu
from jax.sharding import PartitionSpec as P

HEAD_DIM = 64
NUM_BUCKETS = 32
NORM_EPS = 1e-6
LANES = 128
MASKED = -1e30
MESH = pl.DeviceIdType.MESH
BF16 = jnp.bfloat16
F32 = jnp.float32

ROW_ATTN, ROW_FFN, ROW_FINAL, ROW_BIAS, ROW_LEN, SMALL_ROWS = 0, 2, 4, 5, 6, 8

OWN, RT, LT, OP = 0, 1, 2, 3
TO_RIGHT = {OWN: LT, RT: OWN, LT: OP, OP: RT}
TO_LEFT = {OWN: RT, RT: OP, LT: OWN, OP: LT}


def bucket_of(rel_pos):
    half_buckets = NUM_BUCKETS // 2
    max_exact = half_buckets // 2
    distance = jnp.abs(rel_pos)
    log_bucket = jnp.full_like(distance, max_exact)
    for step in range(1, half_buckets - max_exact):
        log_bucket += jnp.where(distance * distance >= max_exact * max_exact * 2**step, 1, 0)
    return jnp.where(rel_pos > 0, half_buckets, 0) + jnp.where(distance < max_exact, distance, log_bucket)


def dot(a, b):
    return jnp.dot(a, b, preferred_element_type=F32)


def dot_rows(a, b):
    return lax.dot_general(a, b, (((1,), (1,)), ((), ())), preferred_element_type=F32)


def kernel(n, groups, lengths_in, attn_gain_in, ffn_gain_in, final_gain_in, bias_table_in,
           tok, wq, wk, wv, wo, win0, win1, wout, out,
           lengths, attn_gain, ffn_gain, final_gain, bias_table, smalls, sm_all, gainb, lenb, biasb, tokb, nb, mb, wqkvb, wob, winb, woutb, qb, kb, vb, cb, c1b, hb, pb,
           relay_a, relay_b, recv_l, recv_r, send_sem, recv_sem, load_sem):
    seq, d_model = tok.shape[1], tok.shape[2]
    layers = wq.shape[0]
    half, rows_half = d_model // 2, seq // 2
    share, ff_share = wq.shape[2], wout.shape[1]
    chip_cols = 2 * share

    me, group = lax.axis_index("fsdp"), lax.axis_index("dp")
    right, left = lax.rem(me + 2, n), lax.rem(me + n - 2, n)
    opposite = lax.rem(me + n // 2, n)
    partner = me + 1 - 2 * lax.rem(me, 2)
    counts = {"remote": 0, "local": 0}
    sent, done = [], set()

    def remote(src, dst, device, axis="fsdp"):
        index = counts["remote"]
        counts["remote"] += 1
        copy = pltpu.make_async_remote_copy(
            src_ref=src, dst_ref=dst, send_sem=send_sem.at[index], recv_sem=recv_sem.at[index],
            device_id={axis: device}, device_id_type=MESH)
        sent.append(copy)
        return copy

    def load(src, dst):
        index = counts["local"]
        counts["local"] += 1
        copy = pltpu.make_async_copy(src, dst, load_sem.at[index])
        copy.start()
        return copy

    def rows(slot, count=1):
        return pl.ds(slot * seq, count * seq)

    def part(ref, slot, r, c):
        row = pl.ds(slot * seq, seq) if r is None else pl.ds(slot * seq + r * rows_half, rows_half)
        col = slice(None) if c is None else pl.ds(c * half, half)
        return ref.at[row, col]

    barrier = pltpu.get_barrier_semaphore()
    for device in (right, left, opposite, partner):
        pl.semaphore_signal(barrier, inc=1, device_id={"fsdp": device}, device_id_type=MESH)
    for k in range(1, groups):
        pl.semaphore_signal(barrier, inc=1, device_id={"dp": lax.rem(group + k, groups)}, device_id_type=MESH)

    small_loads = [load(src, dst) for src, dst in zip(
        (lengths_in, attn_gain_in, ffn_gain_in, final_gain_in, bias_table_in),
        (lengths, attn_gain, ffn_gain, final_gain, bias_table))]
    tok_load = load(tok.at[0], tokb.at[rows(OWN), :])
    wo_loads = [load(wo.at[layer], wob.at[layer, OWN, pl.ds(0, share), :]) for layer in range(layers)]
    qkv_loads = []
    for layer in range(layers):
        qkv_loads.append([load(w.at[layer], wqkvb.at[layer, :, pl.ds(i * chip_cols, share)])
                          for i, w in enumerate((wq, wk, wv))])
        if layer == 0:
            in_loads = []
            out_loads = []
        in_loads.append([load(w.at[layer], winb.at[layer, i, pl.ds(0, ff_share), :]) for i, w in enumerate((win0, win1))])
        out_loads.append(load(wout.at[layer], woutb.at[layer, pl.ds(0, ff_share), :]))

    for copy in small_loads:
        copy.wait()
    smalls[ROW_ATTN:ROW_ATTN + layers, :] = attn_gain[...].astype(F32)
    smalls[ROW_FFN:ROW_FFN + layers, :] = ffn_gain[...].astype(F32)
    smalls[ROW_FINAL:ROW_FINAL + 1, :] = final_gain[...].astype(F32)
    table = bias_table[...].astype(F32)
    smalls[ROW_BIAS:ROW_BIAS + 1, :] = jnp.concatenate([table[i:i + 1] for i in range(table.shape[0])], axis=1)
    smalls[ROW_LEN:SMALL_ROWS, :] = jnp.broadcast_to(lengths[...].astype(F32), (SMALL_ROWS - ROW_LEN, LANES))

    pl.semaphore_wait(barrier, 4 + groups - 1)

    def block_sends(src, dst):
        to_right = [remote(src(c), dst(LT, c), right) for c in range(2)]
        to_left = [remote(src(c), dst(RT, c), left) for c in range(2)]
        return to_right, to_left

    def block_forwards(dst):
        return remote(dst(LT, 0), dst(OP, 0), right), remote(dst(RT, 1), dst(OP, 1), left)

    row_pieces = min(groups, share // 16)
    col_pieces = groups // row_pieces
    piece_rows, piece_cols = share // row_pieces, d_model // col_pieces
    piece_row = pl.multiple_of(group // col_pieces * piece_rows, piece_rows)
    piece_col = pl.multiple_of(lax.rem(group, col_pieces) * piece_cols, piece_cols)

    def wo_copies(layer):
        col = lambda c: pl.ds(pl.multiple_of(piece_col + c * (piece_cols // 2), LANES), piece_cols // 2)
        src = lambda c: wob.at[layer, OWN, pl.ds(piece_row, piece_rows), col(c)]
        dst = lambda slot, c: wob.at[layer, slot, pl.ds(piece_row, piece_rows), col(c)]
        fr, fl = block_forwards(dst)
        piece = lambda slot, count: wob.at[layer, pl.ds(slot, count), pl.ds(piece_row, piece_rows), pl.ds(piece_col, piece_cols)]
        if layer == 0:
            to_right, to_left = block_sends(src, dst)
            to_left = to_left[::-1]
        else:
            to_right = [remote(piece(OWN, 1), piece(LT, 1), right)]
            to_left = [remote(piece(OWN, 1), piece(RT, 1), left)]
        spread = [[remote(piece(slot, count), piece(slot, count), lax.rem(group + k, groups), "dp") for k in range(1, groups)]
                  for slot, count in ((RT, 2), (OP, 1))]
        push = {s: remote(wob.at[layer, s, pl.ds(0, share), :], wob.at[layer, s, pl.ds(share, share), :], partner)
                for s in (RT, LT, OP)}
        return to_right, to_left, fr, fl, spread, push

    wo_r, wo_l, wo_fr, wo_fl, wo_spread, wo_share = zip(*[wo_copies(layer) for layer in range(layers)])

    def start_wo(layer):
        for copy_right, copy_left in zip(wo_r[layer], wo_l[layer]):
            copy_right.start()
            copy_left.start()

    def forward_wo(layer):
        wo_r[layer][0].wait_recv()
        wo_fr[layer].start()
        wo_l[layer][0].wait_recv()
        wo_fl[layer].start()
        for copies in wo_r[layer], wo_l[layer]:
            for copy in copies[1:]:
                copy.wait_recv()
        for copy in wo_spread[layer][0]:
            copy.start()

    def spread_far_wo(layer):
        wo_fr[layer].wait_recv()
        wo_fl[layer].wait_recv()
        for copy in wo_spread[layer][1]:
            copy.start()

    def share_wo_near(layer):
        for copy in wo_spread[layer][0]:
            copy.wait_recv()
        wo_share[layer][LT].start()
        wo_share[layer][RT].start()

    def share_wo_far(layer):
        for copy in wo_spread[layer][1]:
            copy.wait_recv()
        wo_share[layer][OP].start()

    core, chip = lax.rem(me, 2), me // 2
    small_sends = [remote(smalls, sm_all.at[core, chip], device) for device in (right, left, opposite)]
    small_push = remote(sm_all.at[core], sm_all.at[core], partner)
    small_of = lambda device: (lax.rem(device, 2), device // 2)
    tok_src = lambda c: part(tokb, OWN, None, c)
    tok_dst = lambda slot, c: part(tokb, slot, None, c)
    tok_r, tok_l = block_sends(tok_src, tok_dst)
    def to_partner(ref):
        return lambda own, other: remote(ref(own), ref(other), partner)

    qkv_push = [[to_partner(lambda o, i=i: wqkvb.at[layer, :, pl.ds(i * chip_cols + o * share, share)])(0, 1)
                 for i in range(3)] for layer in range(layers)]
    in_push = [[to_partner(lambda o, i=i: winb.at[layer, i, pl.ds(o * ff_share, ff_share), :])(0, 1) for i in range(2)]
               for layer in range(layers)]
    out_push = [to_partner(lambda o: woutb.at[layer, pl.ds(o * ff_share, ff_share), :])(0, 1) for layer in range(layers)]
    wo_push = [to_partner(lambda o: wob.at[layer, OWN, pl.ds(o * share, share), :])(0, 1) for layer in range(layers)]

    for copy in small_sends:
        copy.start()
    for copy in wo_loads:
        copy.wait()
    start_wo(0)
    tok_load.wait()
    tok_r[0].start()
    tok_l[1].start()
    for load_copy, copy in zip(qkv_loads[0], qkv_push[0]):
        load_copy.wait()
        copy.start()
    wo_push[0].start()
    for load_copy, copy in zip(in_loads[0], in_push[0]):
        load_copy.wait()
        copy.start()
    out_loads[0].wait()
    out_push[0].start()

    sm_all[core, chip] = smalls[...]
    for copy in small_sends:
        copy.wait_recv()
    small_push.start()
    small_push.wait_recv()
    for k in range(n):
        gainb[:, k * LANES:(k + 1) * LANES] = sm_all[k % 2, k // 2]
    for slot, device in ((OWN, me), (RT, right), (LT, left), (OP, opposite)):
        at_core, at_chip = small_of(device)
        lenb[slot] = jnp.broadcast_to(sm_all[at_core, at_chip, ROW_LEN:ROW_LEN + 1, :], (8, LANES))

    def norm_rows(load_row, gain_row, dst, start, count, masked=False):
        step = 32

        def body(i, carry):
            r = pl.multiple_of(start + i * step, step)
            x = load_row(r, step)
            mean_sq = jnp.mean(x * x, axis=-1, keepdims=True)
            normed = x * lax.rsqrt(mean_sq + NORM_EPS) * gainb[gain_row:gain_row + 1, :]
            if masked:
                position = (r + lax.broadcasted_iota(jnp.int32, (step, d_model), 0)).astype(F32)
                normed = jnp.where(position < lenb[OWN, 0:1, 0:1], normed, 0.0)
            dst[pl.ds(r, step), :] = normed.astype(BF16)
            return carry

        lax.fori_loop(0, count // step, body, 0)

    def token_row(r, step):
        return tokb[pl.ds(r, step), :].astype(F32)

    def hidden_row(r, step):
        return hb[pl.ds(r, step), :]

    lane_low = lax.rem(lax.broadcasted_iota(jnp.int32, (1, chip_cols), 1), 2 * HEAD_DIM) < HEAD_DIM

    def project(layer, src, slot, count):
        x = src[rows(slot, count), :]
        q = dot(x, wqkvb[layer, :, 0:chip_cols])
        qb[rows(slot, count), :] = q.astype(BF16)
        for i, ref in ((1, kb), (2, vb)):
            y = dot(x, wqkvb[layer, :, i * chip_cols:(i + 1) * chip_cols])
            ref[0, rows(slot, count), :] = jnp.where(lane_low, y, 0.0).astype(BF16)
            ref[1, rows(slot, count), :] = jnp.where(lane_low, 0.0, y).astype(BF16)

    key_index = lax.broadcasted_iota(jnp.int32, (1, seq), 1).astype(F32)

    def attend(layer, slot, count):
        def body(i, carry):
            s = slot + i
            row = pl.ds(pl.multiple_of(s * seq, seq), seq)
            key_ok = key_index < lenb[s, 0:1, :]
            for pair in range(chip_cols // LANES):
                col = pl.ds(pair * LANES, LANES)
                keys = jnp.concatenate([kb[0, row, col], kb[1, row, col]], axis=0)
                scores = dot_rows(qb[row, col], keys)
                scores = scores + biasb[layer, pair]
                probs = []
                for h in range(2):
                    x = jnp.where(key_ok, scores[:, h * seq:(h + 1) * seq], MASKED)
                    e = jnp.exp(x - jnp.max(x, axis=-1, keepdims=True))
                    probs.append((e / jnp.sum(e, axis=-1, keepdims=True)).astype(BF16))
                values = jnp.concatenate([vb[0, row, col], vb[1, row, col]], axis=0)
                cb[0, row, col] = dot(jnp.concatenate(probs, axis=1), values).astype(BF16)
            return carry

        lax.fori_loop(0, count, body, 0)

    def build_bias():
        rel = lax.broadcasted_iota(jnp.int32, (LANES, 2 * seq), 1)
        rel = jnp.where(rel < seq, rel, rel - 2 * seq)
        lane = lax.broadcasted_iota(jnp.int32, (LANES, 2 * seq), 0)
        one_hot = jnp.where(bucket_of(rel) == lax.rem(lane, NUM_BUCKETS), 1.0, 0.0).astype(BF16)
        table_row = lax.broadcasted_iota(jnp.int32, (8, LANES), 0)
        table_lane = lax.broadcasted_iota(jnp.int32, (8, LANES), 1)
        own_lanes = table_row == table_lane // NUM_BUCKETS
        for pair, device in ((0, me), (1, partner)):
            at_core, at_chip = small_of(device)
            tables = jnp.where(own_lanes, sm_all[at_core, at_chip, ROW_BIAS:ROW_BIAS + 1, :], 0.0)
            lines = dot(tables.astype(BF16), one_hot)
            for layer in range(layers):
                for h in range(2):
                    row = 2 * layer + h
                    line = jnp.broadcast_to(lines[row:row + 1, :], (seq, 2 * seq))
                    shifted = pltpu.roll(line, 0, 1, stride=1, stride_axis=0)
                    biasb[layer, pair, :, h * seq:(h + 1) * seq] = shifted[:, 0:seq]

    norm_rows(token_row, ROW_ATTN, nb, OWN * seq, seq)
    build_bias()
    for copy in qkv_push[0]:
        copy.wait_recv()
    project(0, nb, OWN, 1)
    attend(0, OWN, 1)

    forward_wo(0)
    tok_r[1].start()
    tok_l[0].start()
    tok_fr, tok_fl = block_forwards(tok_dst)
    tok_r[0].wait_recv()
    tok_fr.start()
    tok_l[1].wait_recv()
    tok_fl.start()

    def c_part(src, slot, pair):
        return cb.at[src, rows(slot), pl.ds(pair * LANES, LANES)]

    c_r, c_l = {}, {}

    for slot in (OWN, RT, LT, OP):
        c_r[slot] = [remote(c_part(0, slot, p), c_part(LT, TO_RIGHT[slot], p), right) for p in range(2)]
        c_l[slot] = [remote(c_part(0, slot, p), c_part(RT, TO_LEFT[slot], p), left) for p in range(2)]

    def send_context(to_right, to_left):
        c_r[to_right][0].start()
        c_l[to_left][1].start()
        c_r[to_right][1].start()
        c_l[to_left][0].start()

    c_fr, c_fl = {}, {}

    def forward_context(slot):
        near, far = TO_RIGHT[slot], TO_RIGHT[TO_RIGHT[slot]]
        c_fr[slot] = remote(c_part(LT, near, 0), c_part(OP, far, 0), right)
        c_r[slot][0].wait_recv()
        c_fr[slot].start()
        near, far = TO_LEFT[slot], TO_LEFT[TO_LEFT[slot]]
        c_fl[slot] = remote(c_part(RT, near, 1), c_part(OP, far, 1), left)
        c_l[slot][1].wait_recv()
        c_fl[slot].start()

    send_context(OWN, OWN)

    spread_far_wo(0)
    tok_r[1].wait_recv()
    tok_l[0].wait_recv()
    norm_rows(token_row, ROW_ATTN, nb, RT * seq, 2 * seq)
    project(0, nb, RT, 2)
    attend(0, RT, 2)
    send_context(LT, RT)
    send_context(RT, LT)

    forward_context(OWN)
    tok_fr.wait_recv()
    tok_fl.wait_recv()
    norm_rows(token_row, ROW_ATTN, nb, OP * seq, seq)
    project(0, nb, OP, 1)
    attend(0, OP, 1)
    send_context(OP, OP)
    start_wo(1)

    def add_context(slot, count):
        for j in range(0, d_model, chip_cols):
            col = pl.ds(j, chip_cols)
            y = tokb[rows(slot, count), col].astype(F32)
            for src in (OWN, RT, LT, OP):
                y += dot(cb[src, rows(slot, count), :], wob[0, src, :, col])
            hb[rows(slot, count), col] = y

    forward_context(LT)
    forward_context(RT)
    share_wo_near(0)
    share_wo_far(0)
    wo_push[0].wait_recv()
    for copy in in_push[0]:
        copy.wait_recv()
    out_push[0].wait_recv()

    def feed_forward(layer, slot, count):
        x = mb[layer, rows(slot, count), :]
        gate = dot_rows(x, winb[layer, 0])
        lin = dot_rows(x, winb[layer, 1])
        mixed = (jax.nn.gelu(gate, approximate=True) * lin).astype(BF16)
        for j in range(0, d_model, chip_cols):
            col = pl.ds(j, chip_cols)
            pb[layer, rows(slot, count), col] = dot(mixed, woutb[layer, :, col])

    def scatter_copies(layer):
        p, ra, rb = pb.at[layer], relay_a.at[layer], relay_b.at[layer]
        rl, rr = recv_l.at[layer], recv_r.at[layer]
        row = lambda r: pl.ds(r * rows_half, rows_half)
        copies = {}
        for r in range(2):
            copies["op_r", r] = remote(part(p, OP, r, 0), ra.at[row(r), :], right)
            copies["op_l", r] = remote(part(p, OP, r, 1), rb.at[row(r), :], left)
            copies["plain_r", r] = remote(part(p, RT, r, 1), part(rl, 0, r, 1), right)
            copies["plain_l", r] = remote(part(p, LT, r, 0), part(rr, 0, r, 0), left)
            copies["sum_r", r] = remote(part(p, RT, r, 0), part(rl, 0, r, 0), right)
            copies["sum_l", r] = remote(part(p, LT, r, 1), part(rr, 0, r, 1), left)
        return copies

    def pass_on(layer, copies, r):
        a = pl.ds(RT * seq + r * rows_half, rows_half)
        b = pl.ds(LT * seq + r * rows_half, rows_half)
        row = pl.ds(r * rows_half, rows_half)
        copies["op_r", r].wait_recv()
        pb[layer, a, 0:half] += relay_a[layer, row, :]
        copies["sum_r", r].start()
        copies["op_l", r].wait_recv()
        pb[layer, b, half:d_model] += relay_b[layer, row, :]
        copies["sum_l", r].start()

    def collect(layer, copies, r):
        for name in ("plain_r", "plain_l", "sum_r", "sum_l"):
            copies[name, r].wait_recv()
        row = pl.ds(r * rows_half, rows_half)
        hb[row, :] = hb[row, :] + ((pb[layer, row, :] + recv_l[layer, row, :]) + recv_r[layer, row, :])

    rs = scatter_copies(0)
    c_r[LT][1].wait_recv()
    c_l[RT][0].wait_recv()
    c_fr[OWN].wait_recv()
    c_fl[OWN].wait_recv()
    for slot in (RT, LT, OP):
        wo_share[0][slot].wait_recv()
    add_context(OP, 1)
    norm_rows(hidden_row, ROW_FFN, mb.at[0], OP * seq, seq)
    feed_forward(0, OP, 1)
    forward_context(OP)
    for r in range(2):
        rs["op_r", r].start()
        rs["op_l", r].start()
    for slot in (OWN, OP):
        c_r[slot][1].wait_recv()
        c_l[slot][0].wait_recv()
    for slot in (RT, LT):
        c_fr[slot].wait_recv()
        c_fl[slot].wait_recv()
    add_context(RT, 2)
    norm_rows(hidden_row, ROW_FFN, mb.at[0], RT * seq, 2 * seq)
    feed_forward(0, RT, 2)
    rs["plain_r", 0].start()
    rs["plain_l", 0].start()
    forward_wo(1)
    c_r[RT][1].wait_recv()
    c_l[LT][0].wait_recv()
    c_fr[OP].wait_recv()
    c_fl[OP].wait_recv()
    add_context(OWN, 1)
    norm_rows(hidden_row, ROW_FFN, mb.at[0], OWN * seq, seq)
    feed_forward(0, OWN, 1)
    pass_on(0, rs, 0)
    rs["plain_r", 1].start()
    rs["plain_l", 1].start()
    pass_on(0, rs, 1)
    spread_far_wo(1)
    for load_copy, copy in zip(qkv_loads[1], qkv_push[1]):
        load_copy.wait()
        copy.start()
    wo_push[1].start()
    for load_copy, copy in zip(in_loads[1], in_push[1]):
        load_copy.wait()
        copy.start()
    out_loads[1].wait()
    out_push[1].start()

    def gather_copies(ref, r):
        split = (None,) if r == 0 else (0, 1)
        to_right = [remote(part(ref, OWN, r, c), part(ref, LT, r, c), right) for c in split]
        to_left = [remote(part(ref, OWN, r, c), part(ref, RT, r, c), left) for c in reversed(split)]
        fr = remote(part(ref, LT, r, 0), part(ref, OP, r, 0), right)
        fl = remote(part(ref, RT, r, 1), part(ref, OP, r, 1), left)
        return to_right, to_left, fr, fl

    def start_gather(gather):
        for copy_right, copy_left in zip(gather[0], gather[1]):
            copy_right.start()
            copy_left.start()

    def wait_near(gather):
        for copies in gather[0], gather[1]:
            for copy in copies[1:]:
                copy.wait_recv()

    n_gather = [gather_copies(mb.at[2], r) for r in range(2)]
    for r in range(2):
        collect(0, rs, r)
        norm_rows(hidden_row, 1, mb.at[2], r * rows_half, rows_half)
        start_gather(n_gather[r])

    def forward_gather(gather):
        to_right, to_left, fr, fl = gather
        to_right[0].wait_recv()
        fr.start()
        to_left[0].wait_recv()
        fl.start()

    forward_gather(n_gather[0])
    for copy in qkv_push[1]:
        copy.wait_recv()
    for copies in c_r, c_l:
        for slot in (OWN, RT, LT, OP):
            for copy in copies[slot]:
                copy.wait_send()
                done.add(id(copy))
    project(1, mb.at[2], OWN, 1)
    attend(1, OWN, 1)
    forward_gather(n_gather[1])
    share_wo_near(1)
    share_wo_far(1)
    for r in range(2):
        wait_near(n_gather[r])
    project(1, mb.at[2], RT, 2)
    attend(1, RT, 2)
    ctx_r = remote(cb.at[0, rows(RT), :], c1b.at[LT], right)
    ctx_l = remote(cb.at[0, rows(LT), :], c1b.at[RT], left)
    half_rows = lambda r: pl.ds(r * rows_half, rows_half)

    ctx_o = [remote(cb.at[0, pl.ds(OP * seq + r * rows_half, rows_half), :], c1b.at[OP, half_rows(r), :], opposite)
             for r in range(2)]
    ctx_r.start()
    ctx_l.start()
    for r in range(2):
        n_gather[r][2].wait_recv()
        n_gather[r][3].wait_recv()
    project(1, mb.at[2], OP, 1)
    attend(1, OP, 1)
    for copy in ctx_o:
        copy.start()
    wo_push[1].wait_recv()

    def add_second(src, context, r=None):
        row = rows(OWN) if r is None else half_rows(r)
        for j in range(0, d_model, chip_cols):
            col = pl.ds(j, chip_cols)
            hb[row, col] += dot(context, wob[1, src, :, col])

    add_second(OWN, cb[0, rows(OWN), :])
    for slot, copy in ((LT, ctx_r), (RT, ctx_l)):
        wo_share[1][slot].wait_recv()
        copy.wait_recv()
        add_second(slot, c1b[slot])
    wo_share[1][OP].wait_recv()
    m_gather = [gather_copies(mb.at[1], r) for r in range(2)]
    for r in range(2):
        ctx_o[r].wait_recv()
        add_second(OP, c1b[OP, half_rows(r), :], r)
        norm_rows(hidden_row, ROW_FFN + 1, mb.at[1], r * rows_half, rows_half)
        start_gather(m_gather[r])
    for copy in in_push[1]:
        copy.wait_recv()
    out_push[1].wait_recv()
    rs = scatter_copies(1)
    feed_forward(1, OWN, 1)
    for r in range(2):
        forward_gather(m_gather[r])
    for r in range(2):
        wait_near(m_gather[r])
    feed_forward(1, RT, 2)
    rs["plain_r", 0].start()
    rs["plain_l", 0].start()
    for r in range(2):
        m_gather[r][2].wait_recv()
        m_gather[r][3].wait_recv()
    feed_forward(1, OP, 1)
    for r in range(2):
        rs["op_r", r].start()
        rs["op_l", r].start()
    rs["plain_r", 1].start()
    rs["plain_l", 1].start()
    for r in range(2):
        pass_on(1, rs, r)
    for r in range(2):
        collect(1, rs, r)
        norm_rows(hidden_row, ROW_FINAL, out, r * rows_half, rows_half, masked=True)
    for copy in sent:
        if id(copy) not in done:
            copy.wait_send()


def encode(n, groups, lengths, attn_gain, ffn_gain, final_gain, bias_table, tokens, w_q, w_k, w_v, w_o, w_in0, w_in1, w_out):
    _, seq, d_model = tokens.shape
    layers, _, share = w_q.shape
    ff_share = w_out.shape[1]
    chip_cols = 2 * share
    ring = n // 2
    vmem = pl.BlockSpec(memory_space=pltpu.VMEM)
    scratch = [
        pltpu.VMEM(lengths.shape, jnp.int32),
        pltpu.VMEM(attn_gain.shape, BF16),
        pltpu.VMEM(ffn_gain.shape, BF16),
        pltpu.VMEM(final_gain.shape, BF16),
        pltpu.VMEM(bias_table.shape, BF16),
        pltpu.VMEM((SMALL_ROWS, LANES), F32),
        pltpu.VMEM((2, ring, SMALL_ROWS, LANES), F32),
        pltpu.VMEM((8, d_model), F32),
        pltpu.VMEM((ring, 8, LANES), F32),
        pltpu.VMEM((layers, 2, seq, 2 * seq), F32),
        pltpu.VMEM((ring * seq, d_model), BF16),
        pltpu.VMEM((ring * seq, d_model), BF16),
        pltpu.VMEM((layers + 1, ring * seq, d_model), BF16),
        pltpu.VMEM((layers, d_model, 3 * chip_cols), BF16),
        pltpu.VMEM((layers, ring, chip_cols, d_model), BF16),
        pltpu.VMEM((layers, 2, 2 * ff_share, d_model), BF16),
        pltpu.VMEM((layers, 2 * ff_share, d_model), BF16),
        pltpu.VMEM((ring * seq, chip_cols), BF16),
        pltpu.VMEM((2, ring * seq, chip_cols), BF16),
        pltpu.VMEM((2, ring * seq, chip_cols), BF16),
        pltpu.VMEM((ring, ring * seq, chip_cols), BF16),
        pltpu.VMEM((ring, seq, chip_cols), BF16),
        pltpu.VMEM((ring * seq, d_model), F32),
        pltpu.VMEM((layers, ring * seq, d_model), F32),
        pltpu.VMEM((layers, seq, d_model // 2), F32),
        pltpu.VMEM((layers, seq, d_model // 2), F32),
        pltpu.VMEM((layers, seq, d_model), F32),
        pltpu.VMEM((layers, seq, d_model), F32),
        pltpu.SemaphoreType.DMA((160 + 4 * groups,)),
        pltpu.SemaphoreType.DMA((160 + 4 * groups,)),
        pltpu.SemaphoreType.DMA((32,)),
    ]
    return pl.pallas_call(
        functools.partial(kernel, n, groups),
        out_shape=pltpu.VMEM((seq, d_model), BF16),
        in_specs=[pl.BlockSpec(memory_space=pltpu.HBM)] * 13,
        out_specs=vmem,
        scratch_shapes=scratch,
        compiler_params=pltpu.CompilerParams(
            collective_id=0, has_side_effects=True, vmem_limit_bytes=56 * 1024 * 1024),
    )(lengths, attn_gain, ffn_gain, final_gain, bias_table, tokens, w_q, w_k, w_v, w_o, w_in0, w_in1, w_out)


def solution(mesh):
    n, groups = mesh.shape["fsdp"], mesh.shape["dp"]
    batch_spec = P(("dp", "fsdp"))
    col_spec = P(None, None, "fsdp")
    row_spec = P(None, "fsdp", None)
    gain_spec = P(None, "fsdp")
    in_specs = (batch_spec, batch_spec, gain_spec, col_spec, col_spec, col_spec, row_spec, col_spec, gain_spec,
                col_spec, col_spec, row_spec, P("fsdp"))

    def local_forward(tokens, lengths, attn_gain, w_q, w_k, w_v, w_o, rel_bias, ffn_gain, w_in0, w_in1, w_out, final_gain):
        layers, buckets, heads = rel_bias.shape
        bias_table = jnp.swapaxes(rel_bias, 1, 2).reshape(layers * heads, buckets)
        encoded = encode(n, groups, lengths[None], attn_gain, ffn_gain, final_gain[None], bias_table, tokens, w_q, w_k, w_v, w_o,
                            jnp.swapaxes(w_in0, 1, 2), jnp.swapaxes(w_in1, 1, 2), w_out)
        return encoded[None]

    return jax.shard_map(local_forward, mesh=mesh, in_specs=in_specs, out_specs=batch_spec, check_vma=False)
```

```python
import functools

import jax
import jax.numpy as jnp
from jax import lax
from jax.experimental import pallas as pl
from jax.experimental.pallas import tpu as pltpu
from jax.sharding import PartitionSpec as P

HEAD_DIM = 64
NUM_BUCKETS = 32
NORM_EPS = 1e-6
LANES = 128
MASKED = -1e30
MESH = pl.DeviceIdType.MESH
BF16 = jnp.bfloat16
F32 = jnp.float32

ROW_ATTN, ROW_FFN, ROW_FINAL, ROW_BIAS, ROW_LEN, SMALL_ROWS = 0, 2, 4, 5, 6, 8

OWN, RT, LT, OP = 0, 1, 2, 3
TO_RIGHT = {OWN: LT, RT: OWN, LT: OP, OP: RT}
TO_LEFT = {OWN: RT, RT: OP, LT: OWN, OP: LT}


def bucket_of(rel_pos):
    half_buckets = NUM_BUCKETS // 2
    max_exact = half_buckets // 2
    distance = jnp.abs(rel_pos)
    log_bucket = jnp.full_like(distance, max_exact)
    for step in range(1, half_buckets - max_exact):
        log_bucket += jnp.where(distance * distance >= max_exact * max_exact * 2**step, 1, 0)
    return jnp.where(rel_pos > 0, half_buckets, 0) + jnp.where(distance < max_exact, distance, log_bucket)


def dot(a, b):
    return jnp.dot(a, b, preferred_element_type=F32)


def dot_rows(a, b):
    return lax.dot_general(a, b, (((1,), (1,)), ((), ())), preferred_element_type=F32)


def kernel(n, groups, lengths_in, attn_gain_in, ffn_gain_in, final_gain_in, bias_table_in,
           tok, wq, wk, wv, wo, win0, win1, wout, out,
           lengths, attn_gain, ffn_gain, final_gain, bias_table, smalls, sm_all, gainb, lenb, biasb, tokb, nb, mb, wqkvb, wob, winb, woutb, qb, kb, vb, cb, c1b, hb, pb,
           relay_a, relay_b, recv_l, recv_r, send_sem, recv_sem, load_sem):
    seq, d_model = tok.shape[1], tok.shape[2]
    layers = wq.shape[0]
    half, rows_half = d_model // 2, seq // 2
    share, ff_share = wq.shape[2], wout.shape[1]
    chip_cols = 2 * share

    me, group = lax.axis_index("fsdp"), lax.axis_index("dp")
    right, left = lax.rem(me + 2, n), lax.rem(me + n - 2, n)
    opposite = lax.rem(me + n // 2, n)
    partner = me + 1 - 2 * lax.rem(me, 2)
    counts = {"remote": 0, "local": 0}
    sent, done = [], set()

    def remote(src, dst, device, axis="fsdp"):
        index = counts["remote"]
        counts["remote"] += 1
        copy = pltpu.make_async_remote_copy(
            src_ref=src, dst_ref=dst, send_sem=send_sem.at[index], recv_sem=recv_sem.at[index],
            device_id={axis: device}, device_id_type=MESH)
        sent.append(copy)
        return copy

    def load(src, dst):
        index = counts["local"]
        counts["local"] += 1
        copy = pltpu.make_async_copy(src, dst, load_sem.at[index])
        copy.start()
        return copy

    def rows(slot, count=1):
        return pl.ds(slot * seq, count * seq)

    def part(ref, slot, r, c):
        row = pl.ds(slot * seq, seq) if r is None else pl.ds(slot * seq + r * rows_half, rows_half)
        col = slice(None) if c is None else pl.ds(c * half, half)
        return ref.at[row, col]

    barrier = pltpu.get_barrier_semaphore()
    for k in range(1, n):
        pl.semaphore_signal(barrier, inc=1, device_id={"fsdp": lax.rem(me + k, n)}, device_id_type=MESH)
    for k in range(1, groups):
        pl.semaphore_signal(barrier, inc=1, device_id={"dp": lax.rem(group + k, groups)}, device_id_type=MESH)

    small_loads = [load(src, dst) for src, dst in zip(
        (lengths_in, attn_gain_in, ffn_gain_in, final_gain_in, bias_table_in),
        (lengths, attn_gain, ffn_gain, final_gain, bias_table))]
    tok_load = load(tok.at[0], tokb.at[rows(OWN), :])
    wo_loads = [load(wo.at[layer], wob.at[layer, OWN, pl.ds(0, share), :]) for layer in range(layers)]
    qkv_loads = []
    for layer in range(layers):
        qkv_loads.append([load(w.at[layer], wqkvb.at[layer, :, pl.ds(i * chip_cols, share)])
                          for i, w in enumerate((wq, wk, wv))])
        if layer == 0:
            in_loads = []
            out_loads = []
        in_loads.append([load(w.at[layer], winb.at[layer, i, pl.ds(0, ff_share), :]) for i, w in enumerate((win0, win1))])
        out_loads.append(load(wout.at[layer], woutb.at[layer, pl.ds(0, ff_share), :]))

    for copy in small_loads:
        copy.wait()
    smalls[ROW_ATTN:ROW_ATTN + layers, :] = attn_gain[...].astype(F32)
    smalls[ROW_FFN:ROW_FFN + layers, :] = ffn_gain[...].astype(F32)
    smalls[ROW_FINAL:ROW_FINAL + 1, :] = final_gain[...].astype(F32)
    table = bias_table[...].astype(F32)
    smalls[ROW_BIAS:ROW_BIAS + 1, :] = jnp.concatenate([table[i:i + 1] for i in range(table.shape[0])], axis=1)
    smalls[ROW_LEN:SMALL_ROWS, :] = jnp.broadcast_to(lengths[...].astype(F32), (SMALL_ROWS - ROW_LEN, LANES))

    pl.semaphore_wait(barrier, n - 1 + groups - 1)

    def block_sends(src, dst):
        to_right = [remote(src(c), dst(LT, c), right) for c in range(2)]
        to_left = [remote(src(c), dst(RT, c), left) for c in range(2)]
        return to_right, to_left

    def block_forwards(dst):
        return remote(dst(LT, 0), dst(OP, 0), right), remote(dst(RT, 1), dst(OP, 1), left)

    row_pieces = min(groups, share // 16)
    col_pieces = groups // row_pieces
    piece_rows, piece_cols = share // row_pieces, d_model // col_pieces
    piece_row = pl.multiple_of(group // col_pieces * piece_rows, piece_rows)
    piece_col = pl.multiple_of(lax.rem(group, col_pieces) * piece_cols, piece_cols)

    def wo_copies(layer):
        col = lambda c: pl.ds(pl.multiple_of(piece_col + c * (piece_cols // 2), LANES), piece_cols // 2)
        src = lambda c: wob.at[layer, OWN, pl.ds(piece_row, piece_rows), col(c)]
        dst = lambda slot, c: wob.at[layer, slot, pl.ds(piece_row, piece_rows), col(c)]
        to_right, to_left = block_sends(src, dst)
        fr, fl = block_forwards(dst)
        piece = lambda slot, count: wob.at[layer, pl.ds(slot, count), pl.ds(piece_row, piece_rows), pl.ds(piece_col, piece_cols)]
        spread = [[remote(piece(slot, count), piece(slot, count), lax.rem(group + k, groups), "dp") for k in range(1, groups)]
                  for slot, count in ((RT, 2), (OP, 1))]
        push = {s: remote(wob.at[layer, s, pl.ds(0, share), :], wob.at[layer, s, pl.ds(share, share), :], partner)
                for s in (RT, LT, OP)}
        return to_right, to_left, fr, fl, spread, push

    wo_r, wo_l, wo_fr, wo_fl, wo_spread, wo_share = zip(*[wo_copies(layer) for layer in range(layers)])

    def start_wo(layer):
        wo_r[layer][0].start()
        wo_l[layer][1].start()
        wo_r[layer][1].start()
        wo_l[layer][0].start()

    def forward_wo(layer):
        wo_r[layer][0].wait_recv()
        wo_fr[layer].start()
        wo_l[layer][1].wait_recv()
        wo_fl[layer].start()
        wo_r[layer][1].wait_recv()
        wo_l[layer][0].wait_recv()
        for copy in wo_spread[layer][0]:
            copy.start()

    def spread_far_wo(layer):
        wo_fr[layer].wait_recv()
        wo_fl[layer].wait_recv()
        for copy in wo_spread[layer][1]:
            copy.start()

    def share_wo_near(layer):
        for copy in wo_spread[layer][0]:
            copy.wait_recv()
        wo_share[layer][LT].start()
        wo_share[layer][RT].start()

    def share_wo_far(layer):
        for copy in wo_spread[layer][1]:
            copy.wait_recv()
        wo_share[layer][OP].start()

    small_sends = [remote(smalls, sm_all.at[me], lax.rem(me + k, n)) for k in range(1, n)]
    tok_src = lambda c: part(tokb, OWN, None, c)
    tok_dst = lambda slot, c: part(tokb, slot, None, c)
    tok_r, tok_l = block_sends(tok_src, tok_dst)
    def to_partner(ref):
        return lambda own, other: remote(ref(own), ref(other), partner)

    qkv_push = [[to_partner(lambda o, i=i: wqkvb.at[layer, :, pl.ds(i * chip_cols + o * share, share)])(0, 1)
                 for i in range(3)] for layer in range(layers)]
    in_push = [[to_partner(lambda o, i=i: winb.at[layer, i, pl.ds(o * ff_share, ff_share), :])(0, 1) for i in range(2)]
               for layer in range(layers)]
    out_push = [to_partner(lambda o: woutb.at[layer, pl.ds(o * ff_share, ff_share), :])(0, 1) for layer in range(layers)]
    wo_push = [to_partner(lambda o: wob.at[layer, OWN, pl.ds(o * share, share), :])(0, 1) for layer in range(layers)]

    for copy in small_sends:
        copy.start()
    for copy in wo_loads:
        copy.wait()
    start_wo(0)
    tok_load.wait()
    tok_r[0].start()
    tok_l[1].start()
    for load_copy, copy in zip(qkv_loads[0], qkv_push[0]):
        load_copy.wait()
        copy.start()
    wo_push[0].start()
    for load_copy, copy in zip(in_loads[0], in_push[0]):
        load_copy.wait()
        copy.start()
    out_loads[0].wait()
    out_push[0].start()

    sm_all[me] = smalls[...]
    forward_wo(0)
    tok_r[1].start()
    tok_l[0].start()
    for copy in small_sends:
        copy.wait_recv()
    for k in range(n):
        gainb[:, k * LANES:(k + 1) * LANES] = sm_all[k]
    for slot, device in ((OWN, me), (RT, right), (LT, left), (OP, opposite)):
        lenb[slot] = jnp.broadcast_to(sm_all[device, ROW_LEN:ROW_LEN + 1, :], (8, LANES))

    def norm_rows(load_row, gain_row, dst, start, count, masked=False):
        step = 32

        def body(i, carry):
            r = pl.multiple_of(start + i * step, step)
            x = load_row(r, step)
            mean_sq = jnp.mean(x * x, axis=-1, keepdims=True)
            normed = x * lax.rsqrt(mean_sq + NORM_EPS) * gainb[gain_row:gain_row + 1, :]
            if masked:
                position = (r + lax.broadcasted_iota(jnp.int32, (step, d_model), 0)).astype(F32)
                normed = jnp.where(position < lenb[OWN, 0:1, 0:1], normed, 0.0)
            dst[pl.ds(r, step), :] = normed.astype(BF16)
            return carry

        lax.fori_loop(0, count // step, body, 0)

    def token_row(r, step):
        return tokb[pl.ds(r, step), :].astype(F32)

    def hidden_row(r, step):
        return hb[pl.ds(r, step), :]

    lane_low = lax.rem(lax.broadcasted_iota(jnp.int32, (1, chip_cols), 1), 2 * HEAD_DIM) < HEAD_DIM

    def project(layer, src, slot, count):
        x = src[rows(slot, count), :]
        q = dot(x, wqkvb[layer, :, 0:chip_cols])
        qb[rows(slot, count), :] = q.astype(BF16)
        for i, ref in ((1, kb), (2, vb)):
            y = dot(x, wqkvb[layer, :, i * chip_cols:(i + 1) * chip_cols])
            ref[0, rows(slot, count), :] = jnp.where(lane_low, y, 0.0).astype(BF16)
            ref[1, rows(slot, count), :] = jnp.where(lane_low, 0.0, y).astype(BF16)

    key_index = lax.broadcasted_iota(jnp.int32, (1, seq), 1).astype(F32)

    def attend(layer, slot, count):
        def body(i, carry):
            s = slot + i
            row = pl.ds(pl.multiple_of(s * seq, seq), seq)
            key_ok = key_index < lenb[s, 0:1, :]
            for pair in range(chip_cols // LANES):
                col = pl.ds(pair * LANES, LANES)
                keys = jnp.concatenate([kb[0, row, col], kb[1, row, col]], axis=0)
                scores = dot_rows(qb[row, col], keys)
                scores = scores + biasb[layer, pair]
                probs = []
                for h in range(2):
                    x = jnp.where(key_ok, scores[:, h * seq:(h + 1) * seq], MASKED)
                    e = jnp.exp(x - jnp.max(x, axis=-1, keepdims=True))
                    probs.append((e / jnp.sum(e, axis=-1, keepdims=True)).astype(BF16))
                values = jnp.concatenate([vb[0, row, col], vb[1, row, col]], axis=0)
                cb[0, row, col] = dot(jnp.concatenate(probs, axis=1), values).astype(BF16)
            return carry

        lax.fori_loop(0, count, body, 0)

    def build_bias():
        rel = lax.broadcasted_iota(jnp.int32, (LANES, 2 * seq), 1)
        rel = jnp.where(rel < seq, rel, rel - 2 * seq)
        lane = lax.broadcasted_iota(jnp.int32, (LANES, 2 * seq), 0)
        one_hot = jnp.where(bucket_of(rel) == lax.rem(lane, NUM_BUCKETS), 1.0, 0.0).astype(BF16)
        table_row = lax.broadcasted_iota(jnp.int32, (8, LANES), 0)
        table_lane = lax.broadcasted_iota(jnp.int32, (8, LANES), 1)
        own_lanes = table_row == table_lane // NUM_BUCKETS
        for pair, device in ((0, me), (1, partner)):
            tables = jnp.where(own_lanes, sm_all[device, ROW_BIAS:ROW_BIAS + 1, :], 0.0)
            lines = dot(tables.astype(BF16), one_hot)
            for layer in range(layers):
                for h in range(2):
                    row = 2 * layer + h
                    line = jnp.broadcast_to(lines[row:row + 1, :], (seq, 2 * seq))
                    shifted = pltpu.roll(line, 0, 1, stride=1, stride_axis=0)
                    biasb[layer, pair, :, h * seq:(h + 1) * seq] = shifted[:, 0:seq]

    norm_rows(token_row, ROW_ATTN, nb, OWN * seq, seq)
    build_bias()
    for copy in qkv_push[0]:
        copy.wait_recv()
    project(0, nb, OWN, 1)
    attend(0, OWN, 1)

    tok_fr, tok_fl = block_forwards(tok_dst)
    tok_r[0].wait_recv()
    tok_fr.start()
    tok_l[1].wait_recv()
    tok_fl.start()

    def c_part(src, slot, pair):
        return cb.at[src, rows(slot), pl.ds(pair * LANES, LANES)]

    c_r, c_l = {}, {}

    for slot in (OWN, RT, LT, OP):
        c_r[slot] = [remote(c_part(0, slot, p), c_part(LT, TO_RIGHT[slot], p), right) for p in range(2)]
        c_l[slot] = [remote(c_part(0, slot, p), c_part(RT, TO_LEFT[slot], p), left) for p in range(2)]

    def send_context(to_right, to_left):
        c_r[to_right][0].start()
        c_l[to_left][1].start()
        c_r[to_right][1].start()
        c_l[to_left][0].start()

    c_fr, c_fl = {}, {}

    def forward_context(slot):
        near, far = TO_RIGHT[slot], TO_RIGHT[TO_RIGHT[slot]]
        c_fr[slot] = remote(c_part(LT, near, 0), c_part(OP, far, 0), right)
        c_r[slot][0].wait_recv()
        c_fr[slot].start()
        near, far = TO_LEFT[slot], TO_LEFT[TO_LEFT[slot]]
        c_fl[slot] = remote(c_part(RT, near, 1), c_part(OP, far, 1), left)
        c_l[slot][1].wait_recv()
        c_fl[slot].start()

    send_context(OWN, OWN)

    spread_far_wo(0)
    tok_r[1].wait_recv()
    tok_l[0].wait_recv()
    norm_rows(token_row, ROW_ATTN, nb, RT * seq, 2 * seq)
    project(0, nb, RT, 2)
    attend(0, RT, 2)
    send_context(LT, RT)
    send_context(RT, LT)

    forward_context(OWN)
    tok_fr.wait_recv()
    tok_fl.wait_recv()
    norm_rows(token_row, ROW_ATTN, nb, OP * seq, seq)
    project(0, nb, OP, 1)
    attend(0, OP, 1)
    send_context(OP, OP)
    start_wo(1)

    def add_context(slot, count):
        for j in range(0, d_model, chip_cols):
            col = pl.ds(j, chip_cols)
            y = tokb[rows(slot, count), col].astype(F32)
            for src in (OWN, RT, LT, OP):
                y += dot(cb[src, rows(slot, count), :], wob[0, src, :, col])
            hb[rows(slot, count), col] = y

    forward_context(LT)
    forward_context(RT)
    share_wo_near(0)
    share_wo_far(0)
    wo_push[0].wait_recv()
    for copy in in_push[0]:
        copy.wait_recv()
    out_push[0].wait_recv()

    def feed_forward(layer, slot, count):
        x = mb[layer, rows(slot, count), :]
        gate = dot_rows(x, winb[layer, 0])
        lin = dot_rows(x, winb[layer, 1])
        mixed = (jax.nn.gelu(gate, approximate=True) * lin).astype(BF16)
        for j in range(0, d_model, chip_cols):
            col = pl.ds(j, chip_cols)
            pb[layer, rows(slot, count), col] = dot(mixed, woutb[layer, :, col])

    def scatter_copies(layer):
        p, ra, rb = pb.at[layer], relay_a.at[layer], relay_b.at[layer]
        rl, rr = recv_l.at[layer], recv_r.at[layer]
        row = lambda r: pl.ds(r * rows_half, rows_half)
        copies = {}
        for r in range(2):
            copies["op_r", r] = remote(part(p, OP, r, 0), ra.at[row(r), :], right)
            copies["op_l", r] = remote(part(p, OP, r, 1), rb.at[row(r), :], left)
            copies["plain_r", r] = remote(part(p, RT, r, 1), part(rl, 0, r, 1), right)
            copies["plain_l", r] = remote(part(p, LT, r, 0), part(rr, 0, r, 0), left)
            copies["sum_r", r] = remote(part(p, RT, r, 0), part(rl, 0, r, 0), right)
            copies["sum_l", r] = remote(part(p, LT, r, 1), part(rr, 0, r, 1), left)
        return copies

    def pass_on(layer, copies, r):
        a = pl.ds(RT * seq + r * rows_half, rows_half)
        b = pl.ds(LT * seq + r * rows_half, rows_half)
        row = pl.ds(r * rows_half, rows_half)
        copies["op_r", r].wait_recv()
        pb[layer, a, 0:half] += relay_a[layer, row, :]
        copies["sum_r", r].start()
        copies["op_l", r].wait_recv()
        pb[layer, b, half:d_model] += relay_b[layer, row, :]
        copies["sum_l", r].start()

    def collect(layer, copies, r):
        for name in ("plain_r", "plain_l", "sum_r", "sum_l"):
            copies[name, r].wait_recv()
        row = pl.ds(r * rows_half, rows_half)
        hb[row, :] = hb[row, :] + ((pb[layer, row, :] + recv_l[layer, row, :]) + recv_r[layer, row, :])

    rs = scatter_copies(0)
    c_r[LT][1].wait_recv()
    c_l[RT][0].wait_recv()
    c_fr[OWN].wait_recv()
    c_fl[OWN].wait_recv()
    for slot in (RT, LT, OP):
        wo_share[0][slot].wait_recv()
    add_context(OP, 1)
    norm_rows(hidden_row, ROW_FFN, mb.at[0], OP * seq, seq)
    feed_forward(0, OP, 1)
    forward_context(OP)
    for r in range(2):
        rs["op_r", r].start()
        rs["op_l", r].start()
    for slot in (OWN, OP):
        c_r[slot][1].wait_recv()
        c_l[slot][0].wait_recv()
    for slot in (RT, LT):
        c_fr[slot].wait_recv()
        c_fl[slot].wait_recv()
    add_context(RT, 2)
    norm_rows(hidden_row, ROW_FFN, mb.at[0], RT * seq, 2 * seq)
    feed_forward(0, RT, 2)
    rs["plain_r", 0].start()
    rs["plain_l", 0].start()
    forward_wo(1)
    c_r[RT][1].wait_recv()
    c_l[LT][0].wait_recv()
    c_fr[OP].wait_recv()
    c_fl[OP].wait_recv()
    add_context(OWN, 1)
    norm_rows(hidden_row, ROW_FFN, mb.at[0], OWN * seq, seq)
    feed_forward(0, OWN, 1)
    pass_on(0, rs, 0)
    rs["plain_r", 1].start()
    rs["plain_l", 1].start()
    pass_on(0, rs, 1)
    spread_far_wo(1)
    for load_copy, copy in zip(qkv_loads[1], qkv_push[1]):
        load_copy.wait()
        copy.start()
    wo_push[1].start()
    for load_copy, copy in zip(in_loads[1], in_push[1]):
        load_copy.wait()
        copy.start()
    out_loads[1].wait()
    out_push[1].start()

    def gather_copies(ref, r):
        to_right = [remote(part(ref, OWN, r, c), part(ref, LT, r, c), right) for c in range(2)]
        to_left = [remote(part(ref, OWN, r, c), part(ref, RT, r, c), left) for c in range(2)]
        fr = remote(part(ref, LT, r, 0), part(ref, OP, r, 0), right)
        fl = remote(part(ref, RT, r, 1), part(ref, OP, r, 1), left)
        return to_right, to_left, fr, fl

    n_gather = [gather_copies(mb.at[2], r) for r in range(2)]
    for r in range(2):
        collect(0, rs, r)
        norm_rows(hidden_row, 1, mb.at[2], r * rows_half, rows_half)
        to_right, to_left, _, _ = n_gather[r]
        to_right[0].start()
        to_left[1].start()
        to_right[1].start()
        to_left[0].start()

    def forward_gather(gather):
        to_right, to_left, fr, fl = gather
        to_right[0].wait_recv()
        fr.start()
        to_left[1].wait_recv()
        fl.start()

    forward_gather(n_gather[0])
    for copy in qkv_push[1]:
        copy.wait_recv()
    for copies in c_r, c_l:
        for slot in (OWN, RT, LT, OP):
            for copy in copies[slot]:
                copy.wait_send()
                done.add(id(copy))
    project(1, mb.at[2], OWN, 1)
    attend(1, OWN, 1)
    forward_gather(n_gather[1])
    share_wo_near(1)
    share_wo_far(1)
    for r in range(2):
        n_gather[r][0][1].wait_recv()
        n_gather[r][1][0].wait_recv()
    project(1, mb.at[2], RT, 2)
    attend(1, RT, 2)
    ctx_r = remote(cb.at[0, rows(RT), :], c1b.at[LT], right)
    ctx_l = remote(cb.at[0, rows(LT), :], c1b.at[RT], left)
    half_rows = lambda r: pl.ds(r * rows_half, rows_half)

    ctx_o = [remote(cb.at[0, pl.ds(OP * seq + r * rows_half, rows_half), :], c1b.at[OP, half_rows(r), :], opposite)
             for r in range(2)]
    ctx_r.start()
    ctx_l.start()
    for r in range(2):
        n_gather[r][2].wait_recv()
        n_gather[r][3].wait_recv()
    project(1, mb.at[2], OP, 1)
    attend(1, OP, 1)
    for copy in ctx_o:
        copy.start()
    wo_push[1].wait_recv()

    def add_second(src, context, r=None):
        row = rows(OWN) if r is None else half_rows(r)
        for j in range(0, d_model, chip_cols):
            col = pl.ds(j, chip_cols)
            hb[row, col] += dot(context, wob[1, src, :, col])

    add_second(OWN, cb[0, rows(OWN), :])
    for slot, copy in ((LT, ctx_r), (RT, ctx_l)):
        wo_share[1][slot].wait_recv()
        copy.wait_recv()
        add_second(slot, c1b[slot])
    wo_share[1][OP].wait_recv()
    m_gather = [gather_copies(mb.at[1], r) for r in range(2)]
    for r in range(2):
        ctx_o[r].wait_recv()
        add_second(OP, c1b[OP, half_rows(r), :], r)
        norm_rows(hidden_row, ROW_FFN + 1, mb.at[1], r * rows_half, rows_half)
        to_right, to_left, _, _ = m_gather[r]
        to_right[0].start()
        to_left[1].start()
        to_right[1].start()
        to_left[0].start()
    for copy in in_push[1]:
        copy.wait_recv()
    out_push[1].wait_recv()
    rs = scatter_copies(1)
    feed_forward(1, OWN, 1)
    for r in range(2):
        forward_gather(m_gather[r])
    for r in range(2):
        m_gather[r][0][1].wait_recv()
        m_gather[r][1][0].wait_recv()
    feed_forward(1, RT, 2)
    rs["plain_r", 0].start()
    rs["plain_l", 0].start()
    for r in range(2):
        m_gather[r][2].wait_recv()
        m_gather[r][3].wait_recv()
    feed_forward(1, OP, 1)
    for r in range(2):
        rs["op_r", r].start()
        rs["op_l", r].start()
    rs["plain_r", 1].start()
    rs["plain_l", 1].start()
    for r in range(2):
        pass_on(1, rs, r)
    for r in range(2):
        collect(1, rs, r)
        norm_rows(hidden_row, ROW_FINAL, out, r * rows_half, rows_half, masked=True)
    for copy in sent:
        if id(copy) not in done:
            copy.wait_send()


def encode(n, groups, lengths, attn_gain, ffn_gain, final_gain, bias_table, tokens, w_q, w_k, w_v, w_o, w_in0, w_in1, w_out):
    _, seq, d_model = tokens.shape
    layers, _, share = w_q.shape
    ff_share = w_out.shape[1]
    chip_cols = 2 * share
    ring = n // 2
    vmem = pl.BlockSpec(memory_space=pltpu.VMEM)
    scratch = [
        pltpu.VMEM(lengths.shape, jnp.int32),
        pltpu.VMEM(attn_gain.shape, BF16),
        pltpu.VMEM(ffn_gain.shape, BF16),
        pltpu.VMEM(final_gain.shape, BF16),
        pltpu.VMEM(bias_table.shape, BF16),
        pltpu.VMEM((SMALL_ROWS, LANES), F32),
        pltpu.VMEM((n, SMALL_ROWS, LANES), F32),
        pltpu.VMEM((8, d_model), F32),
        pltpu.VMEM((ring, 8, LANES), F32),
        pltpu.VMEM((layers, 2, seq, 2 * seq), F32),
        pltpu.VMEM((ring * seq, d_model), BF16),
        pltpu.VMEM((ring * seq, d_model), BF16),
        pltpu.VMEM((layers + 1, ring * seq, d_model), BF16),
        pltpu.VMEM((layers, d_model, 3 * chip_cols), BF16),
        pltpu.VMEM((layers, ring, chip_cols, d_model), BF16),
        pltpu.VMEM((layers, 2, 2 * ff_share, d_model), BF16),
        pltpu.VMEM((layers, 2 * ff_share, d_model), BF16),
        pltpu.VMEM((ring * seq, chip_cols), BF16),
        pltpu.VMEM((2, ring * seq, chip_cols), BF16),
        pltpu.VMEM((2, ring * seq, chip_cols), BF16),
        pltpu.VMEM((ring, ring * seq, chip_cols), BF16),
        pltpu.VMEM((ring, seq, chip_cols), BF16),
        pltpu.VMEM((ring * seq, d_model), F32),
        pltpu.VMEM((layers, ring * seq, d_model), F32),
        pltpu.VMEM((layers, seq, d_model // 2), F32),
        pltpu.VMEM((layers, seq, d_model // 2), F32),
        pltpu.VMEM((layers, seq, d_model), F32),
        pltpu.VMEM((layers, seq, d_model), F32),
        pltpu.SemaphoreType.DMA((160 + 4 * groups,)),
        pltpu.SemaphoreType.DMA((160 + 4 * groups,)),
        pltpu.SemaphoreType.DMA((32,)),
    ]
    return pl.pallas_call(
        functools.partial(kernel, n, groups),
        out_shape=pltpu.VMEM((seq, d_model), BF16),
        in_specs=[pl.BlockSpec(memory_space=pltpu.HBM)] * 13,
        out_specs=vmem,
        scratch_shapes=scratch,
        compiler_params=pltpu.CompilerParams(
            collective_id=0, has_side_effects=True, vmem_limit_bytes=56 * 1024 * 1024),
    )(lengths, attn_gain, ffn_gain, final_gain, bias_table, tokens, w_q, w_k, w_v, w_o, w_in0, w_in1, w_out)


def solution(mesh):
    n, groups = mesh.shape["fsdp"], mesh.shape["dp"]
    batch_spec = P(("dp", "fsdp"))
    col_spec = P(None, None, "fsdp")
    row_spec = P(None, "fsdp", None)
    gain_spec = P(None, "fsdp")
    in_specs = (batch_spec, batch_spec, gain_spec, col_spec, col_spec, col_spec, row_spec, col_spec, gain_spec,
                col_spec, col_spec, row_spec, P("fsdp"))

    def local_forward(tokens, lengths, attn_gain, w_q, w_k, w_v, w_o, rel_bias, ffn_gain, w_in0, w_in1, w_out, final_gain):
        layers, buckets, heads = rel_bias.shape
        bias_table = jnp.swapaxes(rel_bias, 1, 2).reshape(layers * heads, buckets)
        encoded = encode(n, groups, lengths[None], attn_gain, ffn_gain, final_gain[None], bias_table, tokens, w_q, w_k, w_v, w_o,
                            jnp.swapaxes(w_in0, 1, 2), jnp.swapaxes(w_in1, 1, 2), w_out)
        return encoded[None]

    return jax.shard_map(local_forward, mesh=mesh, in_specs=in_specs, out_specs=batch_spec, check_vma=False)
```

```python
import functools

import jax
import jax.numpy as jnp
from jax import lax
from jax.experimental import pallas as pl
from jax.experimental.pallas import tpu as pltpu
from jax.sharding import PartitionSpec as P

HEAD_DIM = 64
NUM_BUCKETS = 32
NORM_EPS = 1e-6
LANES = 128
MASKED = -1e30
MESH = pl.DeviceIdType.MESH
BF16 = jnp.bfloat16
F32 = jnp.float32

ROW_ATTN, ROW_FFN, ROW_FINAL, ROW_BIAS, ROW_LEN, SMALL_ROWS = 0, 2, 4, 5, 6, 8

OWN, RT, LT, OP = 0, 1, 2, 3
TO_RIGHT = {OWN: LT, RT: OWN, LT: OP, OP: RT}
TO_LEFT = {OWN: RT, RT: OP, LT: OWN, OP: LT}


def bucket_of(rel_pos):
    half_buckets = NUM_BUCKETS // 2
    max_exact = half_buckets // 2
    distance = jnp.abs(rel_pos)
    log_bucket = jnp.full_like(distance, max_exact)
    for step in range(1, half_buckets - max_exact):
        log_bucket += jnp.where(distance * distance >= max_exact * max_exact * 2**step, 1, 0)
    return jnp.where(rel_pos > 0, half_buckets, 0) + jnp.where(distance < max_exact, distance, log_bucket)


def dot(a, b):
    return jnp.dot(a, b, preferred_element_type=F32)


def dot_rows(a, b):
    return lax.dot_general(a, b, (((1,), (1,)), ((), ())), preferred_element_type=F32)


def kernel(n, groups, lengths_in, attn_gain_in, ffn_gain_in, final_gain_in, bias_table_in,
           tok, wq, wk, wv, wo, win0, win1, wout, out,
           lengths, attn_gain, ffn_gain, final_gain, bias_table, smalls, sm_all, gainb, lenb, biasb, tokb, nb, mb, wqkvb, wob, winb, woutb, qb, kb, vb, cb, c1b, hb, pb,
           relay_a, relay_b, recv_l, recv_r, send_sem, recv_sem, load_sem):
    seq, d_model = tok.shape[1], tok.shape[2]
    layers = wq.shape[0]
    half, rows_half = d_model // 2, seq // 2
    share, ff_share = wq.shape[2], wout.shape[1]
    chip_cols = 2 * share

    me, group = lax.axis_index("fsdp"), lax.axis_index("dp")
    right, left = lax.rem(me + 2, n), lax.rem(me + n - 2, n)
    opposite = lax.rem(me + n // 2, n)
    partner = me + 1 - 2 * lax.rem(me, 2)
    counts = {"remote": 0, "local": 0}
    sent, done = [], set()

    def remote(src, dst, device, axis="fsdp"):
        index = counts["remote"]
        counts["remote"] += 1
        copy = pltpu.make_async_remote_copy(
            src_ref=src, dst_ref=dst, send_sem=send_sem.at[index], recv_sem=recv_sem.at[index],
            device_id={axis: device}, device_id_type=MESH)
        sent.append(copy)
        return copy

    def load(src, dst):
        index = counts["local"]
        counts["local"] += 1
        copy = pltpu.make_async_copy(src, dst, load_sem.at[index])
        copy.start()
        return copy

    def rows(slot, count=1):
        return pl.ds(slot * seq, count * seq)

    def part(ref, slot, r, c):
        row = pl.ds(slot * seq, seq) if r is None else pl.ds(slot * seq + r * rows_half, rows_half)
        col = slice(None) if c is None else pl.ds(c * half, half)
        return ref.at[row, col]

    barrier = pltpu.get_barrier_semaphore()
    for k in range(1, n):
        pl.semaphore_signal(barrier, inc=1, device_id={"fsdp": lax.rem(me + k, n)}, device_id_type=MESH)
    for k in range(1, groups):
        pl.semaphore_signal(barrier, inc=1, device_id={"dp": lax.rem(group + k, groups)}, device_id_type=MESH)

    small_loads = [load(src, dst) for src, dst in zip(
        (lengths_in, attn_gain_in, ffn_gain_in, final_gain_in, bias_table_in),
        (lengths, attn_gain, ffn_gain, final_gain, bias_table))]
    tok_load = load(tok.at[0], tokb.at[rows(OWN), :])
    wo_loads = [load(wo.at[layer], wob.at[layer, OWN, pl.ds(0, share), :]) for layer in range(layers)]
    qkv_loads = []
    for layer in range(layers):
        qkv_loads.append([load(w.at[layer], wqkvb.at[layer, :, pl.ds(i * chip_cols, share)])
                          for i, w in enumerate((wq, wk, wv))])
        if layer == 0:
            in_loads = []
            out_loads = []
        in_loads.append([load(w.at[layer], winb.at[layer, i, pl.ds(0, ff_share), :]) for i, w in enumerate((win0, win1))])
        out_loads.append(load(wout.at[layer], woutb.at[layer, pl.ds(0, ff_share), :]))

    for copy in small_loads:
        copy.wait()
    smalls[ROW_ATTN:ROW_ATTN + layers, :] = attn_gain[...].astype(F32)
    smalls[ROW_FFN:ROW_FFN + layers, :] = ffn_gain[...].astype(F32)
    smalls[ROW_FINAL:ROW_FINAL + 1, :] = final_gain[...].astype(F32)
    table = bias_table[...].astype(F32)
    smalls[ROW_BIAS:ROW_BIAS + 1, :] = jnp.concatenate([table[i:i + 1] for i in range(table.shape[0])], axis=1)
    smalls[ROW_LEN:SMALL_ROWS, :] = jnp.broadcast_to(lengths[...].astype(F32), (SMALL_ROWS - ROW_LEN, LANES))

    pl.semaphore_wait(barrier, n - 1 + groups - 1)

    def block_sends(src, dst):
        to_right = [remote(src(c), dst(LT, c), right) for c in range(2)]
        to_left = [remote(src(c), dst(RT, c), left) for c in range(2)]
        return to_right, to_left

    def block_forwards(dst):
        return remote(dst(LT, 0), dst(OP, 0), right), remote(dst(RT, 1), dst(OP, 1), left)

    row_pieces = min(groups, share // 16)
    col_pieces = groups // row_pieces
    piece_rows, piece_cols = share // row_pieces, d_model // col_pieces
    piece_row = pl.multiple_of(group // col_pieces * piece_rows, piece_rows)
    piece_col = pl.multiple_of(lax.rem(group, col_pieces) * piece_cols, piece_cols)

    def wo_copies(layer):
        col = lambda c: pl.ds(pl.multiple_of(piece_col + c * (piece_cols // 2), LANES), piece_cols // 2)
        src = lambda c: wob.at[layer, OWN, pl.ds(piece_row, piece_rows), col(c)]
        dst = lambda slot, c: wob.at[layer, slot, pl.ds(piece_row, piece_rows), col(c)]
        fr, fl = block_forwards(dst)
        piece = lambda slot, count: wob.at[layer, pl.ds(slot, count), pl.ds(piece_row, piece_rows), pl.ds(piece_col, piece_cols)]
        if layer == 0:
            to_right, to_left = block_sends(src, dst)
            to_left = to_left[::-1]
        else:
            to_right = [remote(piece(OWN, 1), piece(LT, 1), right)]
            to_left = [remote(piece(OWN, 1), piece(RT, 1), left)]
        spread = [[remote(piece(slot, count), piece(slot, count), lax.rem(group + k, groups), "dp") for k in range(1, groups)]
                  for slot, count in ((RT, 2), (OP, 1))]
        push = {s: remote(wob.at[layer, s, pl.ds(0, share), :], wob.at[layer, s, pl.ds(share, share), :], partner)
                for s in (RT, LT, OP)}
        return to_right, to_left, fr, fl, spread, push

    wo_r, wo_l, wo_fr, wo_fl, wo_spread, wo_share = zip(*[wo_copies(layer) for layer in range(layers)])

    def start_wo(layer):
        for copy_right, copy_left in zip(wo_r[layer], wo_l[layer]):
            copy_right.start()
            copy_left.start()

    def forward_wo(layer):
        wo_r[layer][0].wait_recv()
        wo_fr[layer].start()
        wo_l[layer][0].wait_recv()
        wo_fl[layer].start()
        for copies in wo_r[layer], wo_l[layer]:
            for copy in copies[1:]:
                copy.wait_recv()
        for copy in wo_spread[layer][0]:
            copy.start()

    def spread_far_wo(layer):
        wo_fr[layer].wait_recv()
        wo_fl[layer].wait_recv()
        for copy in wo_spread[layer][1]:
            copy.start()

    def share_wo_near(layer):
        for copy in wo_spread[layer][0]:
            copy.wait_recv()
        wo_share[layer][LT].start()
        wo_share[layer][RT].start()

    def share_wo_far(layer):
        for copy in wo_spread[layer][1]:
            copy.wait_recv()
        wo_share[layer][OP].start()

    small_sends = [remote(smalls, sm_all.at[me], lax.rem(me + k, n)) for k in range(1, n)]
    tok_src = lambda c: part(tokb, OWN, None, c)
    tok_dst = lambda slot, c: part(tokb, slot, None, c)
    tok_r, tok_l = block_sends(tok_src, tok_dst)
    def to_partner(ref):
        return lambda own, other: remote(ref(own), ref(other), partner)

    qkv_push = [[to_partner(lambda o, i=i: wqkvb.at[layer, :, pl.ds(i * chip_cols + o * share, share)])(0, 1)
                 for i in range(3)] for layer in range(layers)]
    in_push = [[to_partner(lambda o, i=i: winb.at[layer, i, pl.ds(o * ff_share, ff_share), :])(0, 1) for i in range(2)]
               for layer in range(layers)]
    out_push = [to_partner(lambda o: woutb.at[layer, pl.ds(o * ff_share, ff_share), :])(0, 1) for layer in range(layers)]
    wo_push = [to_partner(lambda o: wob.at[layer, OWN, pl.ds(o * share, share), :])(0, 1) for layer in range(layers)]

    for copy in small_sends:
        copy.start()
    for copy in wo_loads:
        copy.wait()
    start_wo(0)
    tok_load.wait()
    tok_r[0].start()
    tok_l[1].start()
    for load_copy, copy in zip(qkv_loads[0], qkv_push[0]):
        load_copy.wait()
        copy.start()
    wo_push[0].start()
    for load_copy, copy in zip(in_loads[0], in_push[0]):
        load_copy.wait()
        copy.start()
    out_loads[0].wait()
    out_push[0].start()

    sm_all[me] = smalls[...]
    for copy in small_sends:
        copy.wait_recv()
    for k in range(n):
        gainb[:, k * LANES:(k + 1) * LANES] = sm_all[k]
    for slot, device in ((OWN, me), (RT, right), (LT, left), (OP, opposite)):
        lenb[slot] = jnp.broadcast_to(sm_all[device, ROW_LEN:ROW_LEN + 1, :], (8, LANES))

    def norm_rows(load_row, gain_row, dst, start, count, masked=False):
        step = 32

        def body(i, carry):
            r = pl.multiple_of(start + i * step, step)
            x = load_row(r, step)
            mean_sq = jnp.mean(x * x, axis=-1, keepdims=True)
            normed = x * lax.rsqrt(mean_sq + NORM_EPS) * gainb[gain_row:gain_row + 1, :]
            if masked:
                position = (r + lax.broadcasted_iota(jnp.int32, (step, d_model), 0)).astype(F32)
                normed = jnp.where(position < lenb[OWN, 0:1, 0:1], normed, 0.0)
            dst[pl.ds(r, step), :] = normed.astype(BF16)
            return carry

        lax.fori_loop(0, count // step, body, 0)

    def token_row(r, step):
        return tokb[pl.ds(r, step), :].astype(F32)

    def hidden_row(r, step):
        return hb[pl.ds(r, step), :]

    lane_low = lax.rem(lax.broadcasted_iota(jnp.int32, (1, chip_cols), 1), 2 * HEAD_DIM) < HEAD_DIM

    def project(layer, src, slot, count):
        x = src[rows(slot, count), :]
        q = dot(x, wqkvb[layer, :, 0:chip_cols])
        qb[rows(slot, count), :] = q.astype(BF16)
        for i, ref in ((1, kb), (2, vb)):
            y = dot(x, wqkvb[layer, :, i * chip_cols:(i + 1) * chip_cols])
            ref[0, rows(slot, count), :] = jnp.where(lane_low, y, 0.0).astype(BF16)
            ref[1, rows(slot, count), :] = jnp.where(lane_low, 0.0, y).astype(BF16)

    key_index = lax.broadcasted_iota(jnp.int32, (1, seq), 1).astype(F32)

    def attend(layer, slot, count):
        def body(i, carry):
            s = slot + i
            row = pl.ds(pl.multiple_of(s * seq, seq), seq)
            key_ok = key_index < lenb[s, 0:1, :]
            for pair in range(chip_cols // LANES):
                col = pl.ds(pair * LANES, LANES)
                keys = jnp.concatenate([kb[0, row, col], kb[1, row, col]], axis=0)
                scores = dot_rows(qb[row, col], keys)
                scores = scores + biasb[layer, pair]
                probs = []
                for h in range(2):
                    x = jnp.where(key_ok, scores[:, h * seq:(h + 1) * seq], MASKED)
                    e = jnp.exp(x - jnp.max(x, axis=-1, keepdims=True))
                    probs.append((e / jnp.sum(e, axis=-1, keepdims=True)).astype(BF16))
                values = jnp.concatenate([vb[0, row, col], vb[1, row, col]], axis=0)
                cb[0, row, col] = dot(jnp.concatenate(probs, axis=1), values).astype(BF16)
            return carry

        lax.fori_loop(0, count, body, 0)

    def build_bias():
        rel = lax.broadcasted_iota(jnp.int32, (LANES, 2 * seq), 1)
        rel = jnp.where(rel < seq, rel, rel - 2 * seq)
        lane = lax.broadcasted_iota(jnp.int32, (LANES, 2 * seq), 0)
        one_hot = jnp.where(bucket_of(rel) == lax.rem(lane, NUM_BUCKETS), 1.0, 0.0).astype(BF16)
        table_row = lax.broadcasted_iota(jnp.int32, (8, LANES), 0)
        table_lane = lax.broadcasted_iota(jnp.int32, (8, LANES), 1)
        own_lanes = table_row == table_lane // NUM_BUCKETS
        for pair, device in ((0, me), (1, partner)):
            tables = jnp.where(own_lanes, sm_all[device, ROW_BIAS:ROW_BIAS + 1, :], 0.0)
            lines = dot(tables.astype(BF16), one_hot)
            for layer in range(layers):
                for h in range(2):
                    row = 2 * layer + h
                    line = jnp.broadcast_to(lines[row:row + 1, :], (seq, 2 * seq))
                    shifted = pltpu.roll(line, 0, 1, stride=1, stride_axis=0)
                    biasb[layer, pair, :, h * seq:(h + 1) * seq] = shifted[:, 0:seq]

    norm_rows(token_row, ROW_ATTN, nb, OWN * seq, seq)
    build_bias()
    for copy in qkv_push[0]:
        copy.wait_recv()
    project(0, nb, OWN, 1)
    attend(0, OWN, 1)

    forward_wo(0)
    tok_r[1].start()
    tok_l[0].start()
    tok_fr, tok_fl = block_forwards(tok_dst)
    tok_r[0].wait_recv()
    tok_fr.start()
    tok_l[1].wait_recv()
    tok_fl.start()

    def c_part(src, slot, pair):
        return cb.at[src, rows(slot), pl.ds(pair * LANES, LANES)]

    c_r, c_l = {}, {}

    for slot in (OWN, RT, LT, OP):
        c_r[slot] = [remote(c_part(0, slot, p), c_part(LT, TO_RIGHT[slot], p), right) for p in range(2)]
        c_l[slot] = [remote(c_part(0, slot, p), c_part(RT, TO_LEFT[slot], p), left) for p in range(2)]

    def send_context(to_right, to_left):
        c_r[to_right][0].start()
        c_l[to_left][1].start()
        c_r[to_right][1].start()
        c_l[to_left][0].start()

    c_fr, c_fl = {}, {}

    def forward_context(slot):
        near, far = TO_RIGHT[slot], TO_RIGHT[TO_RIGHT[slot]]
        c_fr[slot] = remote(c_part(LT, near, 0), c_part(OP, far, 0), right)
        c_r[slot][0].wait_recv()
        c_fr[slot].start()
        near, far = TO_LEFT[slot], TO_LEFT[TO_LEFT[slot]]
        c_fl[slot] = remote(c_part(RT, near, 1), c_part(OP, far, 1), left)
        c_l[slot][1].wait_recv()
        c_fl[slot].start()

    send_context(OWN, OWN)

    spread_far_wo(0)
    tok_r[1].wait_recv()
    tok_l[0].wait_recv()
    norm_rows(token_row, ROW_ATTN, nb, RT * seq, 2 * seq)
    project(0, nb, RT, 2)
    attend(0, RT, 2)
    send_context(LT, RT)
    send_context(RT, LT)

    forward_context(OWN)
    tok_fr.wait_recv()
    tok_fl.wait_recv()
    norm_rows(token_row, ROW_ATTN, nb, OP * seq, seq)
    project(0, nb, OP, 1)
    attend(0, OP, 1)
    send_context(OP, OP)
    start_wo(1)

    def add_context(slot, count):
        for j in range(0, d_model, chip_cols):
            col = pl.ds(j, chip_cols)
            y = tokb[rows(slot, count), col].astype(F32)
            for src in (OWN, RT, LT, OP):
                y += dot(cb[src, rows(slot, count), :], wob[0, src, :, col])
            hb[rows(slot, count), col] = y

    forward_context(LT)
    forward_context(RT)
    share_wo_near(0)
    share_wo_far(0)
    wo_push[0].wait_recv()
    for copy in in_push[0]:
        copy.wait_recv()
    out_push[0].wait_recv()

    def feed_forward(layer, slot, count):
        x = mb[layer, rows(slot, count), :]
        gate = dot_rows(x, winb[layer, 0])
        lin = dot_rows(x, winb[layer, 1])
        mixed = (jax.nn.gelu(gate, approximate=True) * lin).astype(BF16)
        for j in range(0, d_model, chip_cols):
            col = pl.ds(j, chip_cols)
            pb[layer, rows(slot, count), col] = dot(mixed, woutb[layer, :, col])

    def scatter_copies(layer):
        p, ra, rb = pb.at[layer], relay_a.at[layer], relay_b.at[layer]
        rl, rr = recv_l.at[layer], recv_r.at[layer]
        row = lambda r: pl.ds(r * rows_half, rows_half)
        copies = {}
        for r in range(2):
            copies["op_r", r] = remote(part(p, OP, r, 0), ra.at[row(r), :], right)
            copies["op_l", r] = remote(part(p, OP, r, 1), rb.at[row(r), :], left)
            copies["plain_r", r] = remote(part(p, RT, r, 1), part(rl, 0, r, 1), right)
            copies["plain_l", r] = remote(part(p, LT, r, 0), part(rr, 0, r, 0), left)
            copies["sum_r", r] = remote(part(p, RT, r, 0), part(rl, 0, r, 0), right)
            copies["sum_l", r] = remote(part(p, LT, r, 1), part(rr, 0, r, 1), left)
        return copies

    def pass_on(layer, copies, r):
        a = pl.ds(RT * seq + r * rows_half, rows_half)
        b = pl.ds(LT * seq + r * rows_half, rows_half)
        row = pl.ds(r * rows_half, rows_half)
        copies["op_r", r].wait_recv()
        pb[layer, a, 0:half] += relay_a[layer, row, :]
        copies["sum_r", r].start()
        copies["op_l", r].wait_recv()
        pb[layer, b, half:d_model] += relay_b[layer, row, :]
        copies["sum_l", r].start()

    def collect(layer, copies, r):
        for name in ("plain_r", "plain_l", "sum_r", "sum_l"):
            copies[name, r].wait_recv()
        row = pl.ds(r * rows_half, rows_half)
        hb[row, :] = hb[row, :] + ((pb[layer, row, :] + recv_l[layer, row, :]) + recv_r[layer, row, :])

    rs = scatter_copies(0)
    c_r[LT][1].wait_recv()
    c_l[RT][0].wait_recv()
    c_fr[OWN].wait_recv()
    c_fl[OWN].wait_recv()
    for slot in (RT, LT, OP):
        wo_share[0][slot].wait_recv()
    add_context(OP, 1)
    norm_rows(hidden_row, ROW_FFN, mb.at[0], OP * seq, seq)
    feed_forward(0, OP, 1)
    forward_context(OP)
    for r in range(2):
        rs["op_r", r].start()
        rs["op_l", r].start()
    for slot in (OWN, OP):
        c_r[slot][1].wait_recv()
        c_l[slot][0].wait_recv()
    for slot in (RT, LT):
        c_fr[slot].wait_recv()
        c_fl[slot].wait_recv()
    add_context(RT, 2)
    norm_rows(hidden_row, ROW_FFN, mb.at[0], RT * seq, 2 * seq)
    feed_forward(0, RT, 2)
    rs["plain_r", 0].start()
    rs["plain_l", 0].start()
    forward_wo(1)
    c_r[RT][1].wait_recv()
    c_l[LT][0].wait_recv()
    c_fr[OP].wait_recv()
    c_fl[OP].wait_recv()
    add_context(OWN, 1)
    norm_rows(hidden_row, ROW_FFN, mb.at[0], OWN * seq, seq)
    feed_forward(0, OWN, 1)
    pass_on(0, rs, 0)
    rs["plain_r", 1].start()
    rs["plain_l", 1].start()
    pass_on(0, rs, 1)
    spread_far_wo(1)
    for load_copy, copy in zip(qkv_loads[1], qkv_push[1]):
        load_copy.wait()
        copy.start()
    wo_push[1].start()
    for load_copy, copy in zip(in_loads[1], in_push[1]):
        load_copy.wait()
        copy.start()
    out_loads[1].wait()
    out_push[1].start()

    def gather_copies(ref, r):
        split = (None,) if r == 0 else (0, 1)
        to_right = [remote(part(ref, OWN, r, c), part(ref, LT, r, c), right) for c in split]
        to_left = [remote(part(ref, OWN, r, c), part(ref, RT, r, c), left) for c in reversed(split)]
        fr = remote(part(ref, LT, r, 0), part(ref, OP, r, 0), right)
        fl = remote(part(ref, RT, r, 1), part(ref, OP, r, 1), left)
        return to_right, to_left, fr, fl

    def start_gather(gather):
        for copy_right, copy_left in zip(gather[0], gather[1]):
            copy_right.start()
            copy_left.start()

    def wait_near(gather):
        for copies in gather[0], gather[1]:
            for copy in copies[1:]:
                copy.wait_recv()

    n_gather = [gather_copies(mb.at[2], r) for r in range(2)]
    for r in range(2):
        collect(0, rs, r)
        norm_rows(hidden_row, 1, mb.at[2], r * rows_half, rows_half)
        start_gather(n_gather[r])

    def forward_gather(gather):
        to_right, to_left, fr, fl = gather
        to_right[0].wait_recv()
        fr.start()
        to_left[0].wait_recv()
        fl.start()

    forward_gather(n_gather[0])
    for copy in qkv_push[1]:
        copy.wait_recv()
    for copies in c_r, c_l:
        for slot in (OWN, RT, LT, OP):
            for copy in copies[slot]:
                copy.wait_send()
                done.add(id(copy))
    project(1, mb.at[2], OWN, 1)
    attend(1, OWN, 1)
    forward_gather(n_gather[1])
    share_wo_near(1)
    share_wo_far(1)
    for r in range(2):
        wait_near(n_gather[r])
    project(1, mb.at[2], RT, 2)
    attend(1, RT, 2)
    ctx_r = remote(cb.at[0, rows(RT), :], c1b.at[LT], right)
    ctx_l = remote(cb.at[0, rows(LT), :], c1b.at[RT], left)
    half_rows = lambda r: pl.ds(r * rows_half, rows_half)

    ctx_o = [remote(cb.at[0, pl.ds(OP * seq + r * rows_half, rows_half), :], c1b.at[OP, half_rows(r), :], opposite)
             for r in range(2)]
    ctx_r.start()
    ctx_l.start()
    for r in range(2):
        n_gather[r][2].wait_recv()
        n_gather[r][3].wait_recv()
    project(1, mb.at[2], OP, 1)
    attend(1, OP, 1)
    for copy in ctx_o:
        copy.start()
    wo_push[1].wait_recv()

    def add_second(src, context, r=None):
        row = rows(OWN) if r is None else half_rows(r)
        for j in range(0, d_model, chip_cols):
            col = pl.ds(j, chip_cols)
            hb[row, col] += dot(context, wob[1, src, :, col])

    add_second(OWN, cb[0, rows(OWN), :])
    for slot, copy in ((LT, ctx_r), (RT, ctx_l)):
        wo_share[1][slot].wait_recv()
        copy.wait_recv()
        add_second(slot, c1b[slot])
    wo_share[1][OP].wait_recv()
    m_gather = [gather_copies(mb.at[1], r) for r in range(2)]
    for r in range(2):
        ctx_o[r].wait_recv()
        add_second(OP, c1b[OP, half_rows(r), :], r)
        norm_rows(hidden_row, ROW_FFN + 1, mb.at[1], r * rows_half, rows_half)
        start_gather(m_gather[r])
    for copy in in_push[1]:
        copy.wait_recv()
    out_push[1].wait_recv()
    rs = scatter_copies(1)
    feed_forward(1, OWN, 1)
    for r in range(2):
        forward_gather(m_gather[r])
    for r in range(2):
        wait_near(m_gather[r])
    feed_forward(1, RT, 2)
    rs["plain_r", 0].start()
    rs["plain_l", 0].start()
    for r in range(2):
        m_gather[r][2].wait_recv()
        m_gather[r][3].wait_recv()
    feed_forward(1, OP, 1)
    for r in range(2):
        rs["op_r", r].start()
        rs["op_l", r].start()
    rs["plain_r", 1].start()
    rs["plain_l", 1].start()
    for r in range(2):
        pass_on(1, rs, r)
    for r in range(2):
        collect(1, rs, r)
        norm_rows(hidden_row, ROW_FINAL, out, r * rows_half, rows_half, masked=True)
    for copy in sent:
        if id(copy) not in done:
            copy.wait_send()


def encode(n, groups, lengths, attn_gain, ffn_gain, final_gain, bias_table, tokens, w_q, w_k, w_v, w_o, w_in0, w_in1, w_out):
    _, seq, d_model = tokens.shape
    layers, _, share = w_q.shape
    ff_share = w_out.shape[1]
    chip_cols = 2 * share
    ring = n // 2
    vmem = pl.BlockSpec(memory_space=pltpu.VMEM)
    scratch = [
        pltpu.VMEM(lengths.shape, jnp.int32),
        pltpu.VMEM(attn_gain.shape, BF16),
        pltpu.VMEM(ffn_gain.shape, BF16),
        pltpu.VMEM(final_gain.shape, BF16),
        pltpu.VMEM(bias_table.shape, BF16),
        pltpu.VMEM((SMALL_ROWS, LANES), F32),
        pltpu.VMEM((n, SMALL_ROWS, LANES), F32),
        pltpu.VMEM((8, d_model), F32),
        pltpu.VMEM((ring, 8, LANES), F32),
        pltpu.VMEM((layers, 2, seq, 2 * seq), F32),
        pltpu.VMEM((ring * seq, d_model), BF16),
        pltpu.VMEM((ring * seq, d_model), BF16),
        pltpu.VMEM((layers + 1, ring * seq, d_model), BF16),
        pltpu.VMEM((layers, d_model, 3 * chip_cols), BF16),
        pltpu.VMEM((layers, ring, chip_cols, d_model), BF16),
        pltpu.VMEM((layers, 2, 2 * ff_share, d_model), BF16),
        pltpu.VMEM((layers, 2 * ff_share, d_model), BF16),
        pltpu.VMEM((ring * seq, chip_cols), BF16),
        pltpu.VMEM((2, ring * seq, chip_cols), BF16),
        pltpu.VMEM((2, ring * seq, chip_cols), BF16),
        pltpu.VMEM((ring, ring * seq, chip_cols), BF16),
        pltpu.VMEM((ring, seq, chip_cols), BF16),
        pltpu.VMEM((ring * seq, d_model), F32),
        pltpu.VMEM((layers, ring * seq, d_model), F32),
        pltpu.VMEM((layers, seq, d_model // 2), F32),
        pltpu.VMEM((layers, seq, d_model // 2), F32),
        pltpu.VMEM((layers, seq, d_model), F32),
        pltpu.VMEM((layers, seq, d_model), F32),
        pltpu.SemaphoreType.DMA((160 + 4 * groups,)),
        pltpu.SemaphoreType.DMA((160 + 4 * groups,)),
        pltpu.SemaphoreType.DMA((32,)),
    ]
    return pl.pallas_call(
        functools.partial(kernel, n, groups),
        out_shape=pltpu.VMEM((seq, d_model), BF16),
        in_specs=[pl.BlockSpec(memory_space=pltpu.HBM)] * 13,
        out_specs=vmem,
        scratch_shapes=scratch,
        compiler_params=pltpu.CompilerParams(
            collective_id=0, has_side_effects=True, vmem_limit_bytes=56 * 1024 * 1024),
    )(lengths, attn_gain, ffn_gain, final_gain, bias_table, tokens, w_q, w_k, w_v, w_o, w_in0, w_in1, w_out)


def solution(mesh):
    n, groups = mesh.shape["fsdp"], mesh.shape["dp"]
    batch_spec = P(("dp", "fsdp"))
    col_spec = P(None, None, "fsdp")
    row_spec = P(None, "fsdp", None)
    gain_spec = P(None, "fsdp")
    in_specs = (batch_spec, batch_spec, gain_spec, col_spec, col_spec, col_spec, row_spec, col_spec, gain_spec,
                col_spec, col_spec, row_spec, P("fsdp"))

    def local_forward(tokens, lengths, attn_gain, w_q, w_k, w_v, w_o, rel_bias, ffn_gain, w_in0, w_in1, w_out, final_gain):
        layers, buckets, heads = rel_bias.shape
        bias_table = jnp.swapaxes(rel_bias, 1, 2).reshape(layers * heads, buckets)
        encoded = encode(n, groups, lengths[None], attn_gain, ffn_gain, final_gain[None], bias_table, tokens, w_q, w_k, w_v, w_o,
                            jnp.swapaxes(w_in0, 1, 2), jnp.swapaxes(w_in1, 1, 2), w_out)
        return encoded[None]

    return jax.shard_map(local_forward, mesh=mesh, in_specs=in_specs, out_specs=batch_spec, check_vma=False)
```
